32 devices in a mesh: row: 4 (over y, x), col: 8 (over z, core).
Axes of the slice: x: 2, y: 2, z: 4, core: 2. Of those that a mesh axis runs over, the one named last changes fastest.
Arguments:
- docs: bfloat16 [4096, 4, 896], P(('row', 'col')), may hold values from -6 to 6
- routes: int32 [4096, 1], P(('row', 'col')), may hold values from 0 to 31; in each aligned block of 128 rows (0 to 127, 128 to 255, ...) at most 8 rows name the same one
- level_one: float32 [4, 896, 896], P('row', 'col'), may hold values from -6 to 6
- level_two: float32 [8, 896, 896], P('col', 'row'), may hold values from -6 to 6
- moment_one: float32 [4, 896, 896], P('row', 'col'), may hold values from -18 to 18
- moment_two: float32 [8, 896, 896], P('col', 'row'), may hold values from -18 to 18
Outputs:
- new_one: float32 [4, 896, 896], P('row', 'col')
- new_two: float32 [8, 896, 896], P('col', 'row')
- next_moment_one: float32 [4, 896, 896], P('row', 'col')
- next_moment_two: float32 [8, 896, 896], P('col', 'row')
The draws below stay inside these ranges and needn't reach their ends.
Inputs may be any that keep to these rules, and one draw needn't show every extreme that they name: `routes`: each block names one path; among the 128 blocks of one device no path is named more than 8 times, and every path is named by some block.
All inputs are finite; a program needn't handle non-finite values.
Results may differ from the reference program's by a relative error of at most 0.017.
Values may be sent and summed in bfloat16 or wider, within the bound.
A program may use at most 128 MiB of HBM per device.

```python
import math
import jax
import jax.numpy as jnp
import numpy as np
from jax import lax

D = 896
BLOCK = 4
STEPS = 3
DOCS = 128
PATHS = 32
CAP = 8
TOTAL_DOCS = 4096
N_ROW = 4
N_COL = 8


def block_scale(stream_key, dims, shards, smallest, high):
    level, own = 1.0, jax.random.fold_in(stream_key, 6)
    for axis_at, parts in shards:
        heights = jnp.exp(jax.random.uniform(jax.random.fold_in(own, axis_at), (parts,), jnp.float32, smallest / len(shards), high / len(shards)))
        level = level * jnp.repeat(heights, dims[axis_at] // parts).reshape([-1 if axis == axis_at else 1 for axis in range(len(dims))])
    return level


def assign_block(rng, own, number, rows, number_of, top, limit, slope):
    ranking = jax.random.permutation(rng, number_of)
    heavy_load, common = portions_of(number_of, rows * top, limit, slope, True), portions_of(number_of, rows * top, limit, slope, False)
    places = jnp.arange(number_of)

    def named(tallies, rotation):
        used = int((tallies > 0).sum())
        fixed = max(1, used // 4)
        shifted = fixed + (places - fixed + rotation * (used - fixed)) % max(1, number_of - fixed)
        return jnp.zeros((number_of,), jnp.int32).at[ranking[jnp.where(places < fixed, places, shifted)]].set(jnp.asarray(tallies, jnp.int32))

    tallies = jnp.where(number % 4 == 0, named(heavy_load, number // 4), named(common, number - number // 4 - 1))
    mixed = jax.random.permutation(jax.random.fold_in(own, 3), number_of)
    donor, taker = mixed[0:number_of // 2 * 2:2], mixed[1:number_of // 2 * 2:2]
    margin = jnp.minimum(tallies[donor] - 1, limit - tallies[taker]) // 2
    margin = jnp.where((donor == ranking[0]) | (taker == ranking[0]) | (tallies[taker] == 0), 0, jnp.maximum(margin, 0))
    shifted = jax.random.randint(jax.random.fold_in(own, 4), (number_of // 2,), 0, 1 << 20) % (margin + 1)
    tallies = tallies.at[donor].add(-shifted).at[taker].add(shifted)
    items = jnp.searchsorted(jnp.cumsum(tallies), jnp.arange(rows * top), side="right").astype(jnp.int32)
    table = items.reshape(top, rows).T
    table = table[jax.random.permutation(jax.random.fold_in(own, 1), rows)]
    rotation = jax.random.randint(jax.random.fold_in(own, 2), (rows, 1), 0, top)
    return jnp.take_along_axis(table, (jnp.arange(top)[None, :] + rotation) % top, axis=1)


def portions_of(count, total, limit, lean, full):
    portions = [(1 << 20) // math.isqrt(grade ** lean) + 1 for grade in range(1, count + 1)]
    largest = limit if full else min(limit, max(-(-total // count), total * portions[0] // sum(portions)))
    least = 1 if total - largest >= count - 1 else 0
    counts, spare = [largest] + [least] * (count - 1), total - largest - least * (count - 1)
    while spare > 0:
        candidates = [i for i in range(1, count) if counts[i] < largest] or [i for i in range(1, count) if counts[i] < limit]
        whole, remaining = sum([portions[i] for i in candidates]), spare
        for i in candidates:
            more = min(limit - counts[i], max(1, remaining * portions[i] // whole), spare)
            counts[i] = counts[i] + more
            spare = spare - more
    return np.array(counts)


def scatter_about(own_key, extent, scale, bound, shards=(), kind=jnp.bfloat16):
    level = block_scale(own_key, extent, shards, -0.22, 0.18) if shards else 1.0
    entries = jax.random.normal(own_key, extent, jnp.float32) * scale * level
    return jnp.minimum(jnp.maximum(entries, -bound), bound).astype(kind)


def setup_inputs(seed: int = 0) -> dict:
    key_list = jax.random.split(jax.random.key(seed), 7)
    docs = scatter_about(key_list[0], (TOTAL_DOCS, BLOCK, D), 1.0, 6.0, ((0, 32),))
    routes_keys = jax.random.split(jax.random.fold_in(key_list[1], 1), TOTAL_DOCS // DOCS)
    routes_turns = jax.random.permutation(jax.random.fold_in(key_list[1], 3), TOTAL_DOCS // DOCS)
    routes = jax.vmap(lambda own, number: assign_block(jax.random.fold_in(key_list[1], 2), own, number, DOCS, PATHS, 1, CAP, 2))(routes_keys, routes_turns).reshape((TOTAL_DOCS, 1))
    level_one = scatter_about(key_list[2], (N_ROW, D, D), 1.0, 6.0, ((0, 4), (1, 8)), jnp.float32)
    level_two = scatter_about(key_list[3], (N_COL, D, D), 1.0, 6.0, ((0, 8), (1, 4)), jnp.float32)
    moment_one = scatter_about(key_list[4], (N_ROW, D, D), 3.0, 18.0, ((0, 4), (1, 8)), jnp.float32)
    moment_two = scatter_about(key_list[5], (N_COL, D, D), 3.0, 18.0, ((0, 8), (1, 4)), jnp.float32)
    return {"docs": docs, "routes": routes, "level_one": level_one, "level_two": level_two, "moment_one": moment_one, "moment_two": moment_two}


inner_rate = 64.0
outer_rate = 0.7
momentum_decay = 0.9

def normalize(values):
    return values * lax.rsqrt(lax.optimization_barrier(jnp.mean(values * values, axis=-1, keepdims=True)) + 1e-06)

def path_loss(weights, inputs, targets, row_weights):
    first, second = weights
    factor = inputs.shape[-1] ** (-0.5)
    hidden_in = jnp.dot(normalize(inputs).astype(jnp.bfloat16), first.astype(jnp.bfloat16), preferred_element_type=jnp.float32) * factor
    hidden = inputs + jax.nn.silu(hidden_in)
    output = hidden + jnp.dot(normalize(hidden).astype(jnp.bfloat16), second.astype(jnp.bfloat16), preferred_element_type=jnp.float32) * factor
    error = output - targets
    return 0.5 * jnp.sum(row_weights[:, None] * error * error) / jnp.sum(row_weights)

def train_path(first, second, rows, valid):
    width = rows.shape[-1]
    length = rows.shape[-2]
    blocks = rows.reshape(-1, length, width).astype(jnp.float32)
    inputs = blocks[:, :-1].reshape(-1, width)
    targets = blocks[:, 1:].reshape(-1, width)
    row_weights = jnp.repeat(valid.reshape(-1).astype(jnp.float32), length - 1)
    for turn in range(STEPS):
        grads = jax.grad(path_loss)((first, second), inputs, targets, row_weights)
        first = first - inner_rate * grads[0]
        second = second - inner_rate * grads[1]
    return (first, second)

def reference(docs, routes, level_one, level_two, moment_one, moment_two):
    paths = N_ROW * N_COL
    dest = routes[:, 0]
    source_routes = dest.reshape(paths, DOCS)
    onehot = (source_routes[:, :, None] == jnp.arange(paths, dtype=jnp.int32)[None, None, :]).astype(jnp.int32)
    rank = lax.optimization_barrier(jnp.sum(jnp.cumsum(onehot, axis=1) * onehot, axis=2)) - 1
    slot_all = (jnp.arange(paths, dtype=jnp.int32)[:, None] * CAP + rank).reshape(-1).astype(jnp.int32)

    def one_path(carry, path):
        sum_one, sum_two = carry
        place = jnp.where(dest == path, slot_all, paths * CAP).astype(jnp.int32)
        buffer = jnp.zeros((paths * CAP + 1, BLOCK, D), jnp.bfloat16).at[place].add(docs)[:-1]
        valid = jnp.zeros((paths * CAP + 1,), jnp.float32).at[place].add(1.0)[:-1]
        index_one = path // N_COL
        index_two = path % N_COL
        start_one = level_one[index_one]
        start_two = level_two[index_two]
        end_one, end_two = train_path(start_one, start_two, buffer, valid)
        sum_one = sum_one.at[index_one].add(start_one - end_one)
        sum_two = sum_two.at[index_two].add(start_two - end_two)
        return ((sum_one, sum_two), None)
    init = (jnp.zeros((N_ROW, D, D), jnp.float32), jnp.zeros((N_COL, D, D), jnp.float32))
    (sum_one, sum_two), unused = lax.scan(one_path, init, jnp.arange(paths, dtype=jnp.int32))
    delta_one = sum_one / N_COL
    delta_two = sum_two / N_ROW
    next_moment_one = momentum_decay * moment_one + delta_one
    next_moment_two = momentum_decay * moment_two + delta_two
    new_one = level_one - outer_rate * (delta_one + momentum_decay * next_moment_one)
    new_two = level_two - outer_rate * (delta_two + momentum_decay * next_moment_two)
    return (new_one, new_two, next_moment_one, next_moment_two)
```

```python
import functools

import jax
import jax.numpy as jnp
from jax import lax
from jax.experimental import pallas as pl
from jax.experimental.pallas import tpu as pltpu
from jax.sharding import PartitionSpec as P

STEPS = 3
BLOCK_COLS = 256
EARLY = 4

inner_rate = 64.0
outer_rate = 0.7
momentum_decay = 0.9

MESH = pl.DeviceIdType.MESH
f32 = jnp.float32
bf16 = jnp.bfloat16


def product(a, b, i, j):
    return lax.dot_general(a, b, (((i,), (j,)), ((), ())), preferred_element_type=f32)


def column_blocks(width):
    return [(at, min(BLOCK_COLS, width - at)) for at in range(0, width, BLOCK_COLS)]


def fold(values):
    return sum(values[:, at : at + 128] for at in range(0, values.shape[1], 128))


def spread(values, width):
    return jnp.concatenate([values] * (width // 128), axis=1) if width > 128 else values


def round_kernel(
    n_row, n_col, cap, kept,
    route_ref, docs_hbm, one_hbm, two_hbm,
    share_one, share_two,
    docs_v, one_v, two_v, out_ref, cnt_ref, arrived, counts, whole_one, whole_two,
    z, h, g, e, ds, t, xb, hb, eb, db, gram, w2, dw, rx, rr, mm,
    one_out, two_out, pair_buf, part_buf, one_buf, two_buf,
    load_sem, doc_send, doc_recv, cnt_send, cnt_recv,
    up_send, down_send, one_recv, pair_send, pair_recv, two_send, two_recv,
    spair_send, spair_recv, sone_send, sone_recv, stwo_send, stwo_recv,
):
    row, col = lax.axis_index("row"), lax.axis_index("col")
    n = n_row * n_col
    me = row * n_col + col
    chips = n_col // 2
    place, core = col // 2, col % 2
    partner = place * 2 + 1 - core
    lines, width = arrived.shape[1:]
    rows = z.shape[0]
    per = rows // n
    group = 2 * n_row
    chunk = group * per
    half = rows // 2
    count = docs_v.shape[0]
    length = docs_v.shape[1]
    scale = width ** (-0.5)
    blocks = column_blocks(width)
    barrier = pltpu.get_barrier_semaphore()

    loads = [
        pltpu.make_async_copy(one_hbm, one_v, load_sem.at[0]),
        pltpu.make_async_copy(two_hbm, two_v, load_sem.at[1]),
        pltpu.make_async_copy(docs_hbm, docs_v, load_sem.at[2]),
    ]
    for copy in loads:
        copy.start()

    def greet(k, carry):
        to = (me + k) % n
        pl.semaphore_signal(
            barrier, inc=1, device_id={"row": to // n_col, "col": to % n_col}, device_id_type=MESH
        )
        return carry

    lax.fori_loop(1, n, greet, 0)
    loads[0].wait()
    whole_one[col] = one_v[...].astype(bf16)
    loads[1].wait()
    whole_two[row] = two_v[...].astype(bf16)

    target = route_ref[...]
    named = jnp.broadcast_to(target.astype(f32), (count, count))
    earlier = lax.broadcasted_iota(jnp.int32, (count, count), 0) < lax.broadcasted_iota(
        jnp.int32, (count, count), 1
    )
    rank = jnp.sum(jnp.where((named.T == named) & earlier, 1.0, 0.0), axis=0, keepdims=True)
    slot = target * cap + rank.astype(jnp.int32)
    slots = lax.broadcasted_iota(jnp.int32, (n * cap, count), 0)
    dispatch = jnp.where(slots == slot, 1.0, 0.0).astype(bf16)
    path = lax.broadcasted_iota(jnp.int32, (n, 1, count), 0)
    mine = jnp.where(jnp.broadcast_to(target[None], (n, 1, count)) == path, 1.0, 0.0)
    cnt_ref[...] = jnp.broadcast_to(jnp.sum(mine, axis=-1, keepdims=True), cnt_ref.shape)

    pl.semaphore_wait(barrier, n - 1)

    def along(block, to, send):
        return pltpu.make_async_remote_copy(
            src_ref=whole_one.at[block],
            dst_ref=whole_one.at[block],
            send_sem=send.at[block],
            recv_sem=one_recv.at[block],
            device_id={"row": row, "col": to},
            device_id_type=MESH,
        )

    def across(block):
        return pltpu.make_async_remote_copy(
            src_ref=whole_one.at[block],
            dst_ref=whole_one.at[block],
            send_sem=pair_send.at[block],
            recv_sem=pair_recv.at[block],
            device_id={"row": row, "col": partner},
            device_id_type=MESH,
        )

    def two_copy(k):
        return pltpu.make_async_remote_copy(
            src_ref=whole_two.at[row],
            dst_ref=whole_two.at[row],
            send_sem=two_send.at[k],
            recv_sem=two_recv.at[k],
            device_id={"row": (row + k) % n_row, "col": col},
            device_id_type=MESH,
        )

    def two_wait(k):
        from_row = (row - k + n_row) % n_row
        return pltpu.make_async_remote_copy(
            src_ref=whole_two.at[row],
            dst_ref=whole_two.at[from_row],
            send_sem=two_send.at[k],
            recv_sem=two_recv.at[k],
            device_id={"row": (row + k) % n_row, "col": col},
            device_id_type=MESH,
        )

    @pl.when(place < chips - 1)
    def _():
        along(col, col + 2, up_send).start()

    @pl.when(place > 0)
    def _():
        along(col, col - 2, down_send).start()

    across(col).start()
    for k in range(1, n_row):
        two_copy(k).start()

    loads[2].wait()
    docs = jnp.swapaxes(docs_v[...], 0, 1)
    for step in range(length):
        sent = jnp.dot(dispatch, docs[step], preferred_element_type=f32)
        out_ref[:, step * cap : (step + 1) * cap, :] = sent.reshape(n, cap, width).astype(bf16)

    def pair_of(u):
        to_row = (row + u % n_row) % n_row
        apart = u // group * 2 % chips + u // group // (chips // 2)
        to_col = (place + apart) % chips * 2 + (core + u // n_row) % 2
        to = to_row * n_col + to_col
        peer = {"row": to_row, "col": to_col}
        return (
            pltpu.make_async_remote_copy(
                src_ref=out_ref.at[to],
                dst_ref=arrived.at[u],
                send_sem=doc_send.at[u],
                recv_sem=doc_recv.at[u],
                device_id=peer,
                device_id_type=MESH,
            ),
            pltpu.make_async_remote_copy(
                src_ref=cnt_ref.at[to],
                dst_ref=counts.at[u],
                send_sem=cnt_send.at[u],
                recv_sem=cnt_recv.at[u],
                device_id=peer,
                device_id_type=MESH,
            ),
        )

    def send_docs(first, last):
        def body(u, carry):
            for copy in pair_of(u):
                copy.start()
            return carry

        lax.fori_loop(first, last, body, 0)

    arrived[0] = out_ref[me]
    counts[0] = cnt_ref[me]
    send_docs(1, group)
    pieces = [(at, min(at + EARLY, n)) for at in range(group, n, EARLY)]

    for step in range(1, chips):
        if pieces:
            send_docs(*pieces.pop(0))
        low, high = col - 2 * step, col + 2 * step

        @pl.when(place >= step)
        def _():
            along(low, col, up_send).wait_recv()
            across(low).start()

        @pl.when((place >= step) & (place < chips - 1))
        def _():
            along(low, col + 2, up_send).start()

        @pl.when(place < chips - step)
        def _():
            along(high, col, down_send).wait_recv()
            across(high).start()

        @pl.when((place < chips - step) & (place > 0))
        def _():
            along(high, col - 2, down_send).start()

    if pieces:
        send_docs(pieces[0][0], n)

    for q in range(chips):
        across(2 * q + 1 - core).wait_recv()
    for k in range(1, n_row):
        two_wait(k).wait_recv()

    def arrive(first, last):
        def body(u, carry):
            for copy in pair_of(u):
                copy.wait_recv()
            return carry

        lax.fori_loop(first, last, body, 0)

    def unpack(k, at):
        block = arrived[pl.ds(k * group, group)].astype(f32)
        if per == kept:
            first, last = block[:, :kept], block[:, lines - kept :]
        else:
            live = lax.broadcasted_iota(jnp.int32, block.shape, 1) < kept
            first = jnp.where(live, block, 0.0)[:, :per]
            last = jnp.where(live, pltpu.roll(block, kept, 1), 0.0)[:, :per]
        first = first.reshape(chunk, width)
        xb[at, :] = first.astype(bf16)
        t[at, :] = last.reshape(chunk, width).astype(bf16)
        size = jnp.sum(fold(first * first), axis=-1, keepdims=True) * (1.0 / width)
        rx[at, :] = jnp.broadcast_to(lax.rsqrt(size + 1e-06), (chunk, 128))

    def hidden(at, start):
        size = jnp.zeros((at.size, 128), f32)
        for n0, nn in blocks:
            cols = pl.ds(n0, nn)
            zz = start(cols, nn)
            z[at, cols] = zz
            gate = 1.0 / (1.0 + jnp.exp(-zz))
            act = zz * gate
            hh = xb[at, cols].astype(f32) + act
            h[at, cols] = hh
            hb[at, cols] = hh.astype(bf16)
            g[at, cols] = gate + act * (1.0 - gate)
            size = size + fold(hh * hh)
        size = jnp.sum(size, axis=-1, keepdims=True) * (1.0 / width)
        rr[at, :] = jnp.broadcast_to(lax.rsqrt(size + 1e-06), (at.size, 128))

    def errors(at, weights):
        r = rr[at, :]
        both = jnp.zeros((at.size, 128), f32)
        for n0, nn in blocks:
            cols = pl.ds(n0, nn)
            pp = product(hb[at, :], weights(cols), 1, 0)
            rw = spread(r, nn)
            ee = h[at, cols] + scale * rw * pp - t[at, cols].astype(f32)
            er = ee * rw
            e[at, cols] = ee
            eb[at, cols] = er.astype(bf16)
            both = both + fold(er * pp)
        both = jnp.sum(both, axis=-1, keepdims=True) * (1.0 / width)
        mm[at, :] = jnp.broadcast_to(both, (at.size, 128)) * r * r

    def slopes(at, weights, turn):
        m, rw = mm[at, :], rx[at, :]
        for n0, nn in blocks:
            cols = pl.ds(n0, nn)
            qq = product(eb[at, :], weights(cols), 1, 1)
            dd = (e[at, cols] + scale * (qq - h[at, cols] * spread(m, nn))) * g[at, cols]
            dd = dd * spread(rw, nn)
            if turn is None:
                ds[at, cols] = dd
                db[at, cols] = dd.astype(bf16)
            else:
                total = ds[at, cols] + dd
                ds[at, cols] = total
                db[at, cols] = jnp.where(turn == STEPS - 1, total, dd).astype(bf16)


    def two_cols(cols):
        return whole_two[:, :, cols].reshape(width, cols.size)

    def two_rows(cols):
        return whole_two[...].reshape(width, width)[cols.start : cols.start + cols.size]

    arrive(1, group)
    low, high = pl.ds(0, half), pl.ds(half, half)

    def first_turn(k, carry):
        at = pl.ds(pl.multiple_of(k * chunk, chunk), chunk)
        unpack(k, at)

        def start(cols, nn):
            zz = product(xb[at, :], whole_one[:, :, cols].reshape(width, nn), 1, 0)
            return scale * spread(rx[at, :], nn) * zz

        hidden(at, start)
        errors(at, two_cols)
        slopes(at, two_rows, None)

        @pl.when(k == chips // 2 - 1)
        def _():
            gram[low, low] = product(xb[low, :], xb[low, :], 1, 1).astype(bf16)
            for n0, nn in blocks:
                cols = pl.ds(n0, nn)
                dw[:, cols] = product(hb[low, :], eb[low, cols], 0, 0)

        @pl.when(k < chips - 1)
        def _():
            arrive((k + 1) * group, (k + 2) * group)

        return carry

    lax.fori_loop(0, chips, first_turn, 0)
    gram[high, :] = product(xb[high, :], xb[...], 1, 1).astype(bf16)
    gram[low, high] = product(xb[low, :], xb[high, :], 1, 1).astype(bf16)

    filled = jnp.sum(counts[...].reshape(n, 128), axis=0, keepdims=True)[:, :1]
    rate = inner_rate * scale / (filled * (length - 1))

    for n0, nn in blocks:
        cols = pl.ds(n0, nn)
        change = dw[:, cols] + product(hb[high, :], eb[high, cols], 0, 0)
        dw[:, cols] = change
        w2[1, :, cols] = (two_cols(cols).astype(f32) - rate * change).astype(bf16)

    everything = pl.ds(0, rows)

    def stwo_copy(k):
        to = (row + k) % n_row
        return pltpu.make_async_remote_copy(
            src_ref=two_out.at[to],
            dst_ref=two_buf.at[k],
            send_sem=stwo_send.at[k],
            recv_sem=stwo_recv.at[k],
            device_id={"row": to, "col": col},
            device_id_type=MESH,
        )

    def later_turn(turn, carry):
        now, later = turn % 2, (turn + 1) % 2

        def start(cols, nn):
            step = product(gram[...], db[:, cols], 1, 0)
            return z[:, cols] - (rate * scale) * spread(rx[...], nn) * step

        hidden(everything, start)
        errors(everything, lambda cols: w2[now, :, cols])
        for n0, nn in blocks:
            cols = pl.ds(n0, nn)
            change = dw[:, cols] + product(hb[...], eb[:, cols], 0, 0)
            dw[:, cols] = change
            change = rate * change
            w2[later, :, cols] = (two_cols(cols).astype(f32) - change).astype(bf16)
            two_out[:, :, cols] = change.astype(bf16).reshape(n_row, width // n_row, nn)

        @pl.when(turn == STEPS - 1)
        def _():
            for k in range(1, n_row):
                stwo_copy(k).start()

        slopes(everything, lambda cols: w2[now, cols, :], turn)
        return carry

    lax.fori_loop(1, STEPS, later_turn, 0)

    for n0, nn in blocks:
        cols = pl.ds(n0, nn)
        change = rate * product(xb[...], db[:, cols], 0, 0)
        one_out[:, :, cols] = change.astype(bf16).reshape(n_col, width // n_col, nn)

    def spair_copy(q):
        return pltpu.make_async_remote_copy(
            src_ref=one_out.at[2 * q + 1 - core],
            dst_ref=pair_buf.at[q],
            send_sem=spair_send.at[q],
            recv_sem=spair_recv.at[q],
            device_id={"row": row, "col": partner},
            device_id_type=MESH,
        )

    def sone_copy(k):
        return pltpu.make_async_remote_copy(
            src_ref=part_buf.at[k],
            dst_ref=one_buf.at[k],
            send_sem=sone_send.at[k],
            recv_sem=sone_recv.at[k],
            device_id={"row": row, "col": (col + 2 * k) % n_col},
            device_id_type=MESH,
        )

    for k in range(1, chips):
        spair_copy((place + k) % chips).start()
    spair_copy(place).start()
    for k in range(1, chips):
        q = (place + k) % chips
        spair_copy(q).wait_recv()
        part_buf[k] = (one_out[2 * q + core].astype(f32) + pair_buf[q].astype(f32)).astype(bf16)
        sone_copy(k).start()
    spair_copy(place).wait_recv()
    share_one[...] = one_out[col].astype(f32) + pair_buf[place].astype(f32)
    share_two[...] = two_out[row].astype(f32)
    for k in range(1, n_row):
        stwo_copy(k).wait_recv()
        share_two[...] += two_buf[k].astype(f32)
    for k in range(1, chips):
        sone_copy(k).wait_recv()
        share_one[...] += one_buf[k].astype(f32)

    def sent(u, carry):
        for copy in pair_of(u):
            copy.wait_send()
        return carry

    lax.fori_loop(1, n, sent, 0)
    for q in range(chips):
        block = 2 * q + core
        across(block).wait_send()

        @pl.when((place >= q) & (place < chips - 1))
        def _():
            along(block, col + 2, up_send).wait_send()

        @pl.when((place <= q) & (place > 0))
        def _():
            along(block, col - 2, down_send).wait_send()

        spair_copy(q).wait_send()
    for k in range(1, n_row):
        two_copy(k).wait_send()
        stwo_copy(k).wait_send()
    for k in range(1, chips):
        sone_copy(k).wait_send()


def shards(docs, routes, level_one, level_two, moment_one, moment_two):
    n_row = lax.axis_size("row")
    n_col = lax.axis_size("col")
    paths = n_row * n_col
    count, length, width = docs.shape
    cap = max(2, (2 * count + paths - 1) // paths)
    lines = length * cap
    kept = (length - 1) * cap
    per = (kept + 7) // 8 * 8
    rows = paths * per
    chips = n_col // 2
    one_rows, two_rows = width // n_col, width // n_row
    vmem = pl.BlockSpec(memory_space=pltpu.VMEM)
    hbm = pl.BlockSpec(memory_space=pl.ANY)
    dma = pltpu.SemaphoreType.DMA
    full = pltpu.VMEM((rows, width), f32)
    thin = pltpu.VMEM((rows, width), bf16)
    side = pltpu.VMEM((rows, 128), f32)
    share_one, share_two = pl.pallas_call(
        functools.partial(round_kernel, n_row, n_col, cap, kept),
        out_shape=(
            jax.ShapeDtypeStruct((one_rows, width), f32),
            jax.ShapeDtypeStruct((two_rows, width), f32),
        ),
        in_specs=[vmem, hbm, hbm, hbm],
        out_specs=(vmem,) * 2,
        scratch_shapes=[
            pltpu.VMEM((count, length, width), bf16),
            pltpu.VMEM((one_rows, width), f32),
            pltpu.VMEM((two_rows, width), f32),
            pltpu.VMEM((paths, lines, width), bf16),
            pltpu.VMEM((paths, 1, 128), f32),
            pltpu.VMEM((paths, lines, width), bf16),
            pltpu.VMEM((paths, 1, 128), f32),
            pltpu.VMEM((n_col, one_rows, width), bf16),
            pltpu.VMEM((n_row, two_rows, width), bf16),
            full, full, full, full, full, thin, thin, thin, thin, thin,
            pltpu.VMEM((rows, rows), bf16),
            pltpu.VMEM((2, width, width), bf16),
            pltpu.VMEM((width, width), f32),
            side, side, side,
            pltpu.VMEM((n_col, one_rows, width), bf16),
            pltpu.VMEM((n_row, two_rows, width), bf16),
            pltpu.VMEM((chips, one_rows, width), bf16),
            pltpu.VMEM((chips, one_rows, width), bf16),
            pltpu.VMEM((chips, one_rows, width), bf16),
            pltpu.VMEM((n_row, two_rows, width), bf16),
            dma((3,)), dma((paths,)), dma((paths,)), dma((paths,)), dma((paths,)),
            dma((n_col,)), dma((n_col,)), dma((n_col,)), dma((n_col,)), dma((n_col,)),
            dma((n_row,)), dma((n_row,)),
            dma((chips,)), dma((chips,)), dma((chips,)), dma((chips,)),
            dma((n_row,)), dma((n_row,)),
        ],
        compiler_params=pltpu.CompilerParams(
            collective_id=0, has_side_effects=True, vmem_limit_bytes=67043328
        ),
    )(routes.reshape(1, count), docs, level_one[0], level_two[0])
    delta_one = (share_one / n_col)[None]
    delta_two = (share_two / n_row)[None]
    next_moment_one = momentum_decay * moment_one + delta_one
    next_moment_two = momentum_decay * moment_two + delta_two
    new_one = level_one - outer_rate * (delta_one + momentum_decay * next_moment_one)
    new_two = level_two - outer_rate * (delta_two + momentum_decay * next_moment_two)
    return (new_one, new_two, next_moment_one, next_moment_two)


def solution(mesh):
    placed = (
        P(("row", "col"), None, None),
        P(("row", "col"), None),
        P("row", "col", None),
        P("col", "row", None),
        P("row", "col", None),
        P("col", "row", None),
    )
    return jax.shard_map(
        shards,
        mesh=mesh,
        in_specs=placed,
        out_specs=(
            P("row", "col", None),
            P("col", "row", None),
            P("row", "col", None),
            P("col", "row", None),
        ),
        check_vma=False,
    )
```

```python
import functools

import jax
import jax.numpy as jnp
from jax import lax
from jax.experimental import pallas as pl
from jax.experimental.pallas import tpu as pltpu
from jax.sharding import PartitionSpec as P

STEPS = 3
BLOCK_COLS = 256

inner_rate = 64.0
outer_rate = 0.7
momentum_decay = 0.9

MESH = pl.DeviceIdType.MESH
f32 = jnp.float32
bf16 = jnp.bfloat16


def product(a, b, i, j):
    return lax.dot_general(a, b, (((i,), (j,)), ((), ())), preferred_element_type=f32)


def column_blocks(width):
    return [(at, min(BLOCK_COLS, width - at)) for at in range(0, width, BLOCK_COLS)]


def fold(values):
    return sum(values[:, at : at + 128] for at in range(0, values.shape[1], 128))


def spread(values, width):
    return jnp.concatenate([values] * (width // 128), axis=1) if width > 128 else values


def round_kernel(
    n_row, n_col, cap, kept,
    route_ref, docs_hbm, one_hbm, two_hbm, moment_one_hbm, moment_two_hbm,
    new_one, new_two, next_one, next_two,
    docs_v, one_v, two_v, moment_one, moment_two, out_ref, cnt_ref, arrived, counts, whole_one, whole_two,
    z, h, g, e, ds, t, xb, hb, eb, db, gram, w2, dw, rx, rr,
    one_out, two_out, pair_buf, one_buf, two_buf,
    load_sem, doc_send, doc_recv, cnt_send, cnt_recv,
    own_send, relay_send, one_recv, pair_send, pair_recv, two_send, two_recv,
    spair_send, spair_recv, sone_send, sone_recv, stwo_send, stwo_recv,
):
    row, col = lax.axis_index("row"), lax.axis_index("col")
    n = n_row * n_col
    me = row * n_col + col
    chips = n_col // 2
    place, core = col // 2, col % 2
    partner = place * 2 + 1 - core
    side = chips // 2
    upper = place // side
    base = upper * side
    entry = side - 1 + upper
    other_entry = side - upper
    lines, width = arrived.shape[1:]
    rows = z.shape[0]
    per = rows // n
    group = 2 * n_row
    chunk = group * per
    half = rows // 2
    count = docs_v.shape[0]
    length = docs_v.shape[1]
    scale = width ** (-0.5)
    blocks = column_blocks(width)
    barrier = pltpu.get_barrier_semaphore()

    loads = [
        pltpu.make_async_copy(one_hbm, one_v, load_sem.at[0]),
        pltpu.make_async_copy(two_hbm, two_v, load_sem.at[1]),
        pltpu.make_async_copy(docs_hbm, docs_v, load_sem.at[2]),
        pltpu.make_async_copy(moment_one_hbm, moment_one, load_sem.at[3]),
        pltpu.make_async_copy(moment_two_hbm, moment_two, load_sem.at[4]),
    ]
    for copy in loads:
        copy.start()

    def greet(k, carry):
        to = (me + k) % n
        pl.semaphore_signal(
            barrier, inc=1, device_id={"row": to // n_col, "col": to % n_col}, device_id_type=MESH
        )
        return carry

    lax.fori_loop(1, n, greet, 0)
    loads[0].wait()
    whole_one[col] = one_v[...].astype(bf16)
    loads[1].wait()
    whole_two[row] = two_v[...].astype(bf16)

    target = route_ref[...]
    named = jnp.broadcast_to(target.astype(f32), (count, count))
    earlier = lax.broadcasted_iota(jnp.int32, (count, count), 0) < lax.broadcasted_iota(
        jnp.int32, (count, count), 1
    )
    rank = jnp.sum(jnp.where((named.T == named) & earlier, 1.0, 0.0), axis=0, keepdims=True)
    slot = target * cap + rank.astype(jnp.int32)
    slots = lax.broadcasted_iota(jnp.int32, (n * cap, count), 0)
    dispatch = jnp.where(slots == slot, 1.0, 0.0).astype(bf16)
    path = lax.broadcasted_iota(jnp.int32, (n, 1, count), 0)
    mine = jnp.where(jnp.broadcast_to(target[None], (n, 1, count)) == path, 1.0, 0.0)
    cnt_ref[...] = jnp.broadcast_to(jnp.sum(mine, axis=-1, keepdims=True), cnt_ref.shape)

    pl.semaphore_wait(barrier, n - 1)

    def own_copy(to):
        return pltpu.make_async_remote_copy(
            src_ref=whole_one.at[col],
            dst_ref=whole_one.at[col],
            send_sem=own_send.at[to],
            recv_sem=one_recv.at[col],
            device_id={"row": row, "col": 2 * to + core},
            device_id_type=MESH,
        )

    def relay(source, to):
        block = 2 * source + core
        return pltpu.make_async_remote_copy(
            src_ref=whole_one.at[block],
            dst_ref=whole_one.at[block],
            send_sem=relay_send.at[source, to],
            recv_sem=one_recv.at[block],
            device_id={"row": row, "col": 2 * to + core},
            device_id_type=MESH,
        )

    def sibling(j):
        return base + (place - base + j) % side

    def beyond(i):
        return (1 - upper) * (side + i) + upper * (side - 1 - i)

    def across(block):
        return pltpu.make_async_remote_copy(
            src_ref=whole_one.at[block],
            dst_ref=whole_one.at[block],
            send_sem=pair_send.at[block],
            recv_sem=pair_recv.at[block],
            device_id={"row": row, "col": partner},
            device_id_type=MESH,
        )

    def two_copy(k):
        return pltpu.make_async_remote_copy(
            src_ref=whole_two.at[row],
            dst_ref=whole_two.at[row],
            send_sem=two_send.at[k],
            recv_sem=two_recv.at[k],
            device_id={"row": (row + k) % n_row, "col": col},
            device_id_type=MESH,
        )

    def two_wait(k):
        from_row = (row - k + n_row) % n_row
        return pltpu.make_async_remote_copy(
            src_ref=whole_two.at[row],
            dst_ref=whole_two.at[from_row],
            send_sem=two_send.at[k],
            recv_sem=two_recv.at[k],
            device_id={"row": (row + k) % n_row, "col": col},
            device_id_type=MESH,
        )

    own_copy(other_entry).start()
    for j in range(1, side):
        own_copy(sibling(j)).start()
    across(col).start()
    for k in range(1, n_row):
        two_copy(k).start()

    loads[2].wait()
    docs = jnp.swapaxes(docs_v[...], 0, 1)
    for step in range(length):
        sent = jnp.dot(dispatch, docs[step], preferred_element_type=f32)
        out_ref[:, step * cap : (step + 1) * cap, :] = sent.reshape(n, cap, width).astype(bf16)

    def pair_of(u):
        to_row = (row + u % n_row) % n_row
        to_col = (place + u // group) % chips * 2 + (core + u // n_row) % 2
        to = to_row * n_col + to_col
        peer = {"row": to_row, "col": to_col}
        return (
            pltpu.make_async_remote_copy(
                src_ref=out_ref.at[to],
                dst_ref=arrived.at[u],
                send_sem=doc_send.at[u],
                recv_sem=doc_recv.at[u],
                device_id=peer,
                device_id_type=MESH,
            ),
            pltpu.make_async_remote_copy(
                src_ref=cnt_ref.at[to],
                dst_ref=counts.at[u],
                send_sem=cnt_send.at[u],
                recv_sem=cnt_recv.at[u],
                device_id=peer,
                device_id_type=MESH,
            ),
        )

    def apart(k, flip):
        near = k * 2 % chips + k // (chips // 2)
        return (near + flip * (chips - 2 * near)) % chips

    def send_docs(first, last):
        def body(u, carry):
            for copy in pair_of(u):
                copy.start()
            return carry

        lax.fori_loop(first, last, body, 0)

    arrived[0] = out_ref[me]
    counts[0] = cnt_ref[me]
    send_docs(1, group)

    def send_group(k):
        at = apart(k, upper) * group
        send_docs(at, at + group)

    for k in range(1, chips - 1):
        send_group(k)

    @pl.when(place == entry)
    def _():
        for i in range(side):
            source = beyond(i)
            relay(source, place).wait_recv()
            across(2 * source + core).start()
            for j in range(1, side):
                relay(source, sibling(j)).start()

    send_group(chips - 1)
    for j in range(1, side):
        relay(sibling(j), place).wait_recv()
        across(2 * sibling(j) + core).start()

    @pl.when(place != entry)
    def _():
        for i in range(side):
            relay(beyond(i), place).wait_recv()
            across(2 * beyond(i) + core).start()

    for q in range(chips):
        across(2 * q + 1 - core).wait_recv()
    for k in range(1, n_row):
        two_wait(k).wait_recv()

    def arrive(first, last):
        def body(u, carry):
            for copy in pair_of(u):
                copy.wait_recv()
            return carry

        lax.fori_loop(first, last, body, 0)

    def unpack(k, at):
        block = arrived[pl.ds(apart(k, 1 - place % 2) * group, group)].astype(f32)
        if per == kept:
            first, last = block[:, :kept], block[:, lines - kept :]
        else:
            live = lax.broadcasted_iota(jnp.int32, block.shape, 1) < kept
            first = jnp.where(live, block, 0.0)[:, :per]
            last = jnp.where(live, pltpu.roll(block, kept, 1), 0.0)[:, :per]
        first = first.reshape(chunk, width)
        xb[at, :] = first.astype(bf16)
        t[at, :] = last.reshape(chunk, width).astype(bf16)
        size = jnp.sum(fold(first * first), axis=-1, keepdims=True) * (1.0 / width)
        rx[at, :] = jnp.broadcast_to(lax.rsqrt(size + 1e-06), (chunk, 128))

    def hidden(at, start):
        size = jnp.zeros((at.size, 128), f32)
        for n0, nn in blocks:
            cols = pl.ds(n0, nn)
            zz = start(cols, nn)
            z[at, cols] = zz
            gate = 1.0 / (1.0 + jnp.exp(-zz))
            act = zz * gate
            hh = xb[at, cols].astype(f32) + act
            h[at, cols] = hh
            hb[at, cols] = hh.astype(bf16)
            g[at, cols] = gate + act * (1.0 - gate)
            size = size + fold(hh * hh)
        size = jnp.sum(size, axis=-1, keepdims=True) * (1.0 / width)
        rr[at, :] = jnp.broadcast_to(lax.rsqrt(size + 1e-06), (at.size, 128))

    def errors(at, weights):
        r = rr[at, :]
        both = jnp.zeros((at.size, 128), f32)
        for n0, nn in blocks:
            cols = pl.ds(n0, nn)
            pp = product(hb[at, :], weights(cols), 1, 0)
            rw = spread(r, nn)
            ee = h[at, cols] + scale * rw * pp - t[at, cols].astype(f32)
            er = ee * rw
            e[at, cols] = ee
            eb[at, cols] = er.astype(bf16)
            both = both + fold(er * pp)
        both = jnp.sum(both, axis=-1, keepdims=True) * (1.0 / width)
        rr[at, :] = jnp.broadcast_to(both, (at.size, 128)) * r * r

    def slopes(at, weights, turn):
        m, rw = rr[at, :], rx[at, :]
        for n0, nn in blocks:
            cols = pl.ds(n0, nn)
            qq = product(eb[at, :], weights(cols), 1, 1)
            dd = (e[at, cols] + scale * (qq - h[at, cols] * spread(m, nn))) * g[at, cols]
            dd = dd * spread(rw, nn)
            if turn is None:
                ds[at, cols] = dd
                db[at, cols] = dd.astype(bf16)
            else:
                total = ds[at, cols] + dd
                ds[at, cols] = total
                db[at, cols] = jnp.where(turn == STEPS - 1, total, dd).astype(bf16)


    def two_cols(cols):
        return whole_two[:, :, cols].reshape(width, cols.size)

    def two_rows(cols):
        return whole_two[...].reshape(width, width)[cols.start : cols.start + cols.size]

    arrive(1, group)
    low, high = pl.ds(0, half), pl.ds(half, half)

    def first_turn(k, carry):
        at = pl.ds(pl.multiple_of(k * chunk, chunk), chunk)
        unpack(k, at)

        def start(cols, nn):
            zz = product(xb[at, :], whole_one[:, :, cols].reshape(width, nn), 1, 0)
            return scale * spread(rx[at, :], nn) * zz

        hidden(at, start)
        errors(at, two_cols)
        slopes(at, two_rows, None)

        @pl.when(k == chips // 2 - 1)
        def _():
            gram[low, low] = product(xb[low, :], xb[low, :], 1, 1).astype(bf16)
            for n0, nn in blocks:
                cols = pl.ds(n0, nn)
                dw[:, cols] = product(hb[low, :], eb[low, cols], 0, 0)

        @pl.when(k < chips - 1)
        def _():
            first = apart(k + 1, 1 - place % 2) * group
            arrive(first, first + group)

        return carry

    lax.fori_loop(0, chips, first_turn, 0)
    gram[high, :] = product(xb[high, :], xb[...], 1, 1).astype(bf16)
    gram[low, high] = product(xb[low, :], xb[high, :], 1, 1).astype(bf16)

    filled = jnp.sum(counts[...].reshape(n, 128), axis=0, keepdims=True)[:, :1]
    rate = inner_rate * scale / (filled * (length - 1))

    for n0, nn in blocks:
        cols = pl.ds(n0, nn)
        change = dw[:, cols] + product(hb[high, :], eb[high, cols], 0, 0)
        dw[:, cols] = change
        w2[1, :, cols] = (two_cols(cols).astype(f32) - rate * change).astype(bf16)

    everything = pl.ds(0, rows)

    def stwo_copy(k):
        to = (row + k) % n_row
        return pltpu.make_async_remote_copy(
            src_ref=two_out.at[to],
            dst_ref=two_buf.at[k],
            send_sem=stwo_send.at[k],
            recv_sem=stwo_recv.at[k],
            device_id={"row": to, "col": col},
            device_id_type=MESH,
        )

    def later_turn(turn, carry):
        now, later = turn % 2, (turn + 1) % 2

        def start(cols, nn):
            step = product(gram[...], db[:, cols], 1, 0)
            return z[:, cols] - (rate * scale) * spread(rx[...], nn) * step

        hidden(everything, start)
        errors(everything, lambda cols: w2[now, :, cols])
        for n0, nn in blocks:
            cols = pl.ds(n0, nn)
            change = dw[:, cols] + product(hb[...], eb[:, cols], 0, 0)
            dw[:, cols] = change
            change = rate * change
            w2[later, :, cols] = (two_cols(cols).astype(f32) - change).astype(bf16)
            two_out[:, :, cols] = change.astype(bf16).reshape(n_row, width // n_row, nn)

        @pl.when(turn == STEPS - 1)
        def _():
            for k in range(1, n_row):
                stwo_copy(k).start()

        slopes(everything, lambda cols: w2[now, cols, :], turn)
        return carry

    lax.fori_loop(1, STEPS, later_turn, 0)

    for n0, nn in blocks:
        cols = pl.ds(n0, nn)
        change = rate * product(xb[...], db[:, cols], 0, 0)
        one_out[:, :, cols] = change.astype(bf16).reshape(n_col, width // n_col, nn)

    def spair_copy(q):
        return pltpu.make_async_remote_copy(
            src_ref=one_out.at[2 * q + 1 - core],
            dst_ref=pair_buf.at[q],
            send_sem=spair_send.at[q],
            recv_sem=spair_recv.at[q],
            device_id={"row": row, "col": partner},
            device_id_type=MESH,
        )

    def sone_copy(k):
        return pltpu.make_async_remote_copy(
            src_ref=one_out.at[2 * ((place + k) % chips) + core],
            dst_ref=one_buf.at[k],
            send_sem=sone_send.at[k],
            recv_sem=sone_recv.at[k],
            device_id={"row": row, "col": (col + 2 * k) % n_col},
            device_id_type=MESH,
        )

    for k in range(1, chips):
        spair_copy((place + k) % chips).start()
    spair_copy(place).start()
    for k in range(1, chips):
        q = (place + k) % chips
        spair_copy(q).wait_recv()
        one_out[2 * q + core] = (
            one_out[2 * q + core].astype(f32) + pair_buf[q].astype(f32)
        ).astype(bf16)
        sone_copy(k).start()
    loads[3].wait()
    loads[4].wait()
    spair_copy(place).wait_recv()

    def finish(share, level, moment, new, following):
        following[...] = momentum_decay * moment[...] + share
        new[...] = level[...] - outer_rate * (share + momentum_decay * following[...])

    share = two_out[row].astype(f32)
    for k in range(1, n_row):
        stwo_copy(k).wait_recv()
        share = share + two_buf[k].astype(f32)
    finish(share / n_row, two_v, moment_two, new_two, next_two)
    share = one_out[col].astype(f32) + pair_buf[place].astype(f32)
    for k in range(1, chips):
        sone_copy(k).wait_recv()
        share = share + one_buf[k].astype(f32)
    finish(share / n_col, one_v, moment_one, new_one, next_one)

    def sent(u, carry):
        for copy in pair_of(u):
            copy.wait_send()
        return carry

    lax.fori_loop(1, n, sent, 0)
    own_copy(other_entry).wait_send()
    for j in range(1, side):
        own_copy(sibling(j)).wait_send()

    @pl.when(place == entry)
    def _():
        for i in range(side):
            for j in range(1, side):
                relay(beyond(i), sibling(j)).wait_send()

    for q in range(chips):
        across(2 * q + core).wait_send()
        spair_copy(q).wait_send()
    for k in range(1, n_row):
        two_copy(k).wait_send()
        stwo_copy(k).wait_send()
    for k in range(1, chips):
        sone_copy(k).wait_send()


def shards(docs, routes, level_one, level_two, moment_one, moment_two):
    n_row = lax.axis_size("row")
    n_col = lax.axis_size("col")
    paths = n_row * n_col
    count, length, width = docs.shape
    cap = max(2, (2 * count + paths - 1) // paths)
    lines = length * cap
    kept = (length - 1) * cap
    per = (kept + 7) // 8 * 8
    rows = paths * per
    chips = n_col // 2
    one_rows, two_rows = width // n_col, width // n_row
    vmem = pl.BlockSpec(memory_space=pltpu.VMEM)
    hbm = pl.BlockSpec(memory_space=pl.ANY)
    dma = pltpu.SemaphoreType.DMA
    full = pltpu.VMEM((rows, width), f32)
    thin = pltpu.VMEM((rows, width), bf16)
    side = pltpu.VMEM((rows, 128), f32)
    wide_one = jax.ShapeDtypeStruct((one_rows, width), f32)
    wide_two = jax.ShapeDtypeStruct((two_rows, width), f32)
    results = pl.pallas_call(
        functools.partial(round_kernel, n_row, n_col, cap, kept),
        out_shape=(wide_one, wide_two, wide_one, wide_two),
        in_specs=[vmem, hbm, hbm, hbm, hbm, hbm],
        out_specs=(vmem,) * 4,
        scratch_shapes=[
            pltpu.VMEM((count, length, width), bf16),
            pltpu.VMEM((one_rows, width), f32),
            pltpu.VMEM((two_rows, width), f32),
            pltpu.VMEM((one_rows, width), f32),
            pltpu.VMEM((two_rows, width), f32),
            pltpu.VMEM((paths, lines, width), bf16),
            pltpu.VMEM((paths, 1, 128), f32),
            pltpu.VMEM((paths, lines, width), bf16),
            pltpu.VMEM((paths, 1, 128), f32),
            pltpu.VMEM((n_col, one_rows, width), bf16),
            pltpu.VMEM((n_row, two_rows, width), bf16),
            full, full, full, full, full, thin, thin, thin, thin, thin,
            pltpu.VMEM((rows, rows), bf16),
            pltpu.VMEM((2, width, width), bf16),
            pltpu.VMEM((width, width), f32),
            side, side,
            pltpu.VMEM((n_col, one_rows, width), bf16),
            pltpu.VMEM((n_row, two_rows, width), bf16),
            pltpu.VMEM((chips, one_rows, width), bf16),
            pltpu.VMEM((chips, one_rows, width), bf16),
            pltpu.VMEM((n_row, two_rows, width), bf16),
            dma((5,)), dma((paths,)), dma((paths,)), dma((paths,)), dma((paths,)),
            dma((chips,)), dma((chips, chips)), dma((n_col,)), dma((n_col,)), dma((n_col,)),
            dma((n_row,)), dma((n_row,)),
            dma((chips,)), dma((chips,)), dma((chips,)), dma((chips,)),
            dma((n_row,)), dma((n_row,)),
        ],
        compiler_params=pltpu.CompilerParams(
            collective_id=0, has_side_effects=True, vmem_limit_bytes=67043328
        ),
    )(
        routes.reshape(1, count), docs, level_one[0], level_two[0], moment_one[0], moment_two[0]
    )
    return tuple(result[None] for result in results)


def solution(mesh):
    placed = (
        P(("row", "col"), None, None),
        P(("row", "col"), None),
        P("row", "col", None),
        P("col", "row", None),
        P("row", "col", None),
        P("col", "row", None),
    )
    return jax.shard_map(
        shards,
        mesh=mesh,
        in_specs=placed,
        out_specs=(
            P("row", "col", None),
            P("col", "row", None),
            P("row", "col", None),
            P("col", "row", None),
        ),
        check_vma=False,
    )
```

```python
import functools
import math

import jax
import jax.numpy as jnp
from jax import lax
from jax.experimental import pallas as pl
from jax.experimental.pallas import tpu as pltpu
from jax.sharding import PartitionSpec as P

STEPS = 3
BLOCK_COLS = 256

inner_rate = 64.0
outer_rate = 0.7
momentum_decay = 0.9

MESH = pl.DeviceIdType.MESH
f32 = jnp.float32
bf16 = jnp.bfloat16


def product(a, b, i, j):
    return lax.dot_general(a, b, (((i,), (j,)), ((), ())), preferred_element_type=f32)


def column_blocks(width):
    return [(at, min(BLOCK_COLS, width - at)) for at in range(0, width, BLOCK_COLS)]


def fold(values):
    return sum(values[:, at : at + 128] for at in range(0, values.shape[1], 128))


def spread(values, width):
    return jnp.concatenate([values] * (width // 128), axis=1) if width > 128 else values


def round_kernel(
    n_row, n_col, cap, kept,
    route_ref, docs_hbm, one_hbm, two_hbm, moment_one_hbm, moment_two_hbm,
    new_one, new_two, next_one, next_two,
    docs_v, one_v, two_v, moment_one, moment_two, out_ref, cnt_ref, arrived, counts, whole_one, whole_two,
    z, h, g, e, ds, t, xb, hb, eb, db, gram, w2, dw, rx, rr,
    one_out, two_out, pair_buf, pre_buf, one_buf, two_buf,
    load_sem, doc_send, doc_recv, cnt_send, cnt_recv,
    own_send, relay_send, one_recv, pair_send, pair_recv, two_send, two_recv,
    spair_send, spair_recv, pre_send, pre_recv, sone_send, sone_recv, stwo_send, stwo_recv, out_sem,
):
    row, col = lax.axis_index("row"), lax.axis_index("col")
    n = n_row * n_col
    me = row * n_col + col
    chips = n_col // 2
    place, core = col // 2, col % 2
    partner = place * 2 + 1 - core
    side = chips // 2
    upper = place // side
    base = upper * side
    entry = side - 1 + upper
    other_entry = side - upper
    lines, width = arrived.shape[1:]
    rows = z.shape[0]
    per = rows // n
    group = 2 * n_row
    chunk = group * per
    early = rows * (chips - 1) // chips // 256 * 256
    count = docs_v.shape[0]
    length = docs_v.shape[1]
    scale = width ** (-0.5)
    blocks = column_blocks(width)
    barrier = pltpu.get_barrier_semaphore()

    loads = [
        pltpu.make_async_copy(one_hbm, one_v, load_sem.at[0]),
        pltpu.make_async_copy(two_hbm, two_v, load_sem.at[1]),
        pltpu.make_async_copy(docs_hbm, docs_v, load_sem.at[2]),
        pltpu.make_async_copy(moment_one_hbm, moment_one, load_sem.at[3]),
        pltpu.make_async_copy(moment_two_hbm, moment_two, load_sem.at[4]),
    ]
    for copy in loads:
        copy.start()

    def greet(k, carry):
        to = (me + k) % n
        pl.semaphore_signal(
            barrier, inc=1, device_id={"row": to // n_col, "col": to % n_col}, device_id_type=MESH
        )
        return carry

    lax.fori_loop(1, n, greet, 0)
    loads[0].wait()
    whole_one[col] = one_v[...].astype(bf16)
    loads[1].wait()
    whole_two[row] = two_v[...].astype(bf16)

    pl.semaphore_wait(barrier, n - 1)

    def own_copy(to):
        return pltpu.make_async_remote_copy(
            src_ref=whole_one.at[col],
            dst_ref=whole_one.at[col],
            send_sem=own_send.at[to],
            recv_sem=one_recv.at[col],
            device_id={"row": row, "col": 2 * to + core},
            device_id_type=MESH,
        )

    def relay(source, to):
        block = 2 * source + core
        return pltpu.make_async_remote_copy(
            src_ref=whole_one.at[block],
            dst_ref=whole_one.at[block],
            send_sem=relay_send.at[source, to],
            recv_sem=one_recv.at[block],
            device_id={"row": row, "col": 2 * to + core},
            device_id_type=MESH,
        )

    def sibling(j):
        return base + (place - base + j) % side

    def beyond(i):
        return (1 - upper) * (side + i) + upper * (side - 1 - i)

    def across(block):
        return pltpu.make_async_remote_copy(
            src_ref=whole_one.at[block],
            dst_ref=whole_one.at[block],
            send_sem=pair_send.at[block],
            recv_sem=pair_recv.at[block],
            device_id={"row": row, "col": partner},
            device_id_type=MESH,
        )

    def two_copy(k):
        return pltpu.make_async_remote_copy(
            src_ref=whole_two.at[row],
            dst_ref=whole_two.at[row],
            send_sem=two_send.at[k],
            recv_sem=two_recv.at[k],
            device_id={"row": (row + k) % n_row, "col": col},
            device_id_type=MESH,
        )

    def two_wait(k):
        from_row = (row - k + n_row) % n_row
        return pltpu.make_async_remote_copy(
            src_ref=whole_two.at[row],
            dst_ref=whole_two.at[from_row],
            send_sem=two_send.at[k],
            recv_sem=two_recv.at[k],
            device_id={"row": (row + k) % n_row, "col": col},
            device_id_type=MESH,
        )

    own_copy(other_entry).start()
    for j in range(1, side):
        own_copy(sibling(j)).start()
    across(col).start()
    for k in range(1, n_row):
        two_copy(k).start()

    target = route_ref[...]
    named = jnp.broadcast_to(target.astype(f32), (count, count))
    earlier = lax.broadcasted_iota(jnp.int32, (count, count), 0) < lax.broadcasted_iota(
        jnp.int32, (count, count), 1
    )
    rank = jnp.sum(jnp.where((named.T == named) & earlier, 1.0, 0.0), axis=0, keepdims=True)
    slot = target * cap + rank.astype(jnp.int32)
    slots = lax.broadcasted_iota(jnp.int32, (n * cap, count), 0)
    dispatch = jnp.where(slots == slot, 1.0, 0.0).astype(bf16)
    path = lax.broadcasted_iota(jnp.int32, (n, 1, count), 0)
    mine = jnp.where(jnp.broadcast_to(target[None], (n, 1, count)) == path, 1.0, 0.0)
    cnt_ref[...] = jnp.broadcast_to(jnp.sum(mine, axis=-1, keepdims=True), cnt_ref.shape)

    loads[2].wait()
    docs = jnp.swapaxes(docs_v[...], 0, 1)
    for step in range(length):
        sent = jnp.dot(dispatch, docs[step], preferred_element_type=f32)
        out_ref[:, step * cap : (step + 1) * cap, :] = sent.reshape(n, cap, width).astype(bf16)

    def pair_of(u):
        to_row = (row + u % n_row) % n_row
        to_col = (place + u // group) % chips * 2 + (core + u // n_row) % 2
        to = to_row * n_col + to_col
        peer = {"row": to_row, "col": to_col}
        return (
            pltpu.make_async_remote_copy(
                src_ref=out_ref.at[to],
                dst_ref=arrived.at[u],
                send_sem=doc_send.at[u],
                recv_sem=doc_recv.at[u],
                device_id=peer,
                device_id_type=MESH,
            ),
            pltpu.make_async_remote_copy(
                src_ref=cnt_ref.at[to],
                dst_ref=counts.at[u],
                send_sem=cnt_send.at[u],
                recv_sem=cnt_recv.at[u],
                device_id=peer,
                device_id_type=MESH,
            ),
        )

    def apart(k, flip):
        near = k * 2 % chips + k // (chips // 2)
        return (near + flip * (chips - 2 * near)) % chips

    def send_docs(first, last):
        def body(u, carry):
            for copy in pair_of(u):
                copy.start()
            return carry

        lax.fori_loop(first, last, body, 0)

    arrived[0] = out_ref[me]
    counts[0] = cnt_ref[me]
    send_docs(1, group)

    def send_group(k):
        at = apart(k, upper) * group
        send_docs(at, at + group)

    for k in range(1, chips - 1):
        send_group(k)

    @pl.when(place == entry)
    def _():
        for i in range(side):
            source = beyond(i)
            relay(source, place).wait_recv()
            across(2 * source + core).start()
            for j in range(1, side):
                relay(source, sibling(j)).start()

    send_group(chips - 1)
    for j in range(1, side):
        relay(sibling(j), place).wait_recv()
        across(2 * sibling(j) + core).start()

    @pl.when(place != entry)
    def _():
        for i in range(side):
            relay(beyond(i), place).wait_recv()
            across(2 * beyond(i) + core).start()

    for q in range(chips):
        across(2 * q + 1 - core).wait_recv()
    for k in range(1, n_row):
        two_wait(k).wait_recv()

    def arrive(first, last):
        def body(u, carry):
            for copy in pair_of(u):
                copy.wait_recv()
            return carry

        lax.fori_loop(first, last, body, 0)

    def unpack(k, at):
        block = arrived[pl.ds(apart(k, 1 - place % 2) * group, group)].astype(f32)
        if per == kept:
            first, last = block[:, :kept], block[:, lines - kept :]
        else:
            live = lax.broadcasted_iota(jnp.int32, block.shape, 1) < kept
            first = jnp.where(live, block, 0.0)[:, :per]
            last = jnp.where(live, pltpu.roll(block, kept, 1), 0.0)[:, :per]
        first = first.reshape(chunk, width)
        xb[at, :] = first.astype(bf16)
        t[at, :] = last.reshape(chunk, width).astype(bf16)
        size = jnp.sum(fold(first * first), axis=-1, keepdims=True) * (1.0 / width)
        rx[at, :] = jnp.broadcast_to(lax.rsqrt(size + 1e-06), (chunk, 128))

    def hidden(at, start):
        size = jnp.zeros((at.size, 128), f32)
        for n0, nn in blocks:
            cols = pl.ds(n0, nn)
            zz = start(cols, nn)
            z[at, cols] = zz
            gate = 1.0 / (1.0 + jnp.exp(-zz))
            act = zz * gate
            hh = xb[at, cols].astype(f32) + act
            h[at, cols] = hh
            hb[at, cols] = hh.astype(bf16)
            g[at, cols] = gate + act * (1.0 - gate)
            size = size + fold(hh * hh)
        size = jnp.sum(size, axis=-1, keepdims=True) * (1.0 / width)
        rr[at, :] = jnp.broadcast_to(lax.rsqrt(size + 1e-06), (at.size, 128))

    def errors(at, weights):
        r = rr[at, :]
        both = jnp.zeros((at.size, 128), f32)
        for n0, nn in blocks:
            cols = pl.ds(n0, nn)
            pp = product(hb[at, :], weights(cols), 1, 0)
            rw = spread(r, nn)
            ee = h[at, cols] + scale * rw * pp - t[at, cols].astype(f32)
            er = ee * rw
            e[at, cols] = ee
            eb[at, cols] = er.astype(bf16)
            both = both + fold(er * pp)
        both = jnp.sum(both, axis=-1, keepdims=True) * (1.0 / width)
        rr[at, :] = jnp.broadcast_to(both, (at.size, 128)) * r * r

    def slopes(at, weights, turn):
        m, rw = rr[at, :], rx[at, :]
        for n0, nn in blocks:
            cols = pl.ds(n0, nn)
            qq = product(eb[at, :], weights(cols), 1, 1)
            dd = (e[at, cols] + scale * (qq - h[at, cols] * spread(m, nn))) * g[at, cols]
            dd = dd * spread(rw, nn)
            if turn is None:
                ds[at, cols] = dd
                db[at, cols] = dd.astype(bf16)
            else:
                total = ds[at, cols] + dd
                ds[at, cols] = total
                db[at, cols] = jnp.where(turn == STEPS - 1, total, dd).astype(bf16)


    def two_cols(cols):
        return whole_two[:, :, cols].reshape(width, cols.size)

    def two_rows(cols):
        return whole_two[...].reshape(width, width)[cols.start : cols.start + cols.size]

    arrive(1, group)
    low, high = pl.ds(0, early), pl.ds(early, rows - early)

    def first_turn(k, carry):
        at = pl.ds(pl.multiple_of(k * chunk, chunk), chunk)
        unpack(k, at)

        def start(cols, nn):
            zz = product(xb[at, :], whole_one[:, :, cols].reshape(width, nn), 1, 0)
            return scale * spread(rx[at, :], nn) * zz

        hidden(at, start)
        errors(at, two_cols)
        slopes(at, two_rows, None)

        @pl.when(k == chips - 2)
        def _():
            gram[low, low] = product(xb[low, :], xb[low, :], 1, 1).astype(bf16)
            for n0, nn in blocks:
                cols = pl.ds(n0, nn)
                dw[:, cols] = product(hb[low, :], eb[low, cols], 0, 0)

        @pl.when(k < chips - 1)
        def _():
            first = apart(k + 1, 1 - place % 2) * group
            arrive(first, first + group)

        return carry

    lax.fori_loop(0, chips, first_turn, 0)
    gram[high, :] = product(xb[high, :], xb[...], 1, 1).astype(bf16)
    gram[low, high] = product(xb[low, :], xb[high, :], 1, 1).astype(bf16)

    filled = jnp.sum(counts[...].reshape(n, 128), axis=0, keepdims=True)[:, :1]
    rate = inner_rate * scale / (filled * (length - 1))

    for n0, nn in blocks:
        cols = pl.ds(n0, nn)
        change = dw[:, cols] + product(hb[high, :], eb[high, cols], 0, 0)
        dw[:, cols] = change
        w2[1, :, cols] = (two_cols(cols).astype(f32) - rate * change).astype(bf16)

    everything = pl.ds(0, rows)

    def stwo_copy(k):
        to = (row + k) % n_row
        return pltpu.make_async_remote_copy(
            src_ref=two_out.at[to],
            dst_ref=two_buf.at[k],
            send_sem=stwo_send.at[k],
            recv_sem=stwo_recv.at[k],
            device_id={"row": to, "col": col},
            device_id_type=MESH,
        )

    def later_turn(turn, carry):
        now, later = turn % 2, (turn + 1) % 2

        def start(cols, nn):
            step = product(gram[...], db[:, cols], 1, 0)
            return z[:, cols] - (rate * scale) * spread(rx[...], nn) * step

        hidden(everything, start)
        errors(everything, lambda cols: w2[now, :, cols])
        for n0, nn in blocks:
            cols = pl.ds(n0, nn)
            change = dw[:, cols] + product(hb[...], eb[:, cols], 0, 0)
            dw[:, cols] = change
            change = rate * change
            w2[later, :, cols] = (two_cols(cols).astype(f32) - change).astype(bf16)
            two_out[:, :, cols] = change.astype(bf16).reshape(n_row, width // n_row, nn)

        @pl.when(turn == STEPS - 1)
        def _():
            for k in range(1, n_row):
                stwo_copy(k).start()

        slopes(everything, lambda cols: w2[now, cols, :], turn)
        return carry

    lax.fori_loop(1, STEPS, later_turn, 0)

    for n0, nn in blocks:
        cols = pl.ds(n0, nn)
        change = rate * product(xb[...], db[:, cols], 0, 0)
        one_out[:, :, cols] = change.astype(bf16).reshape(n_col, width // n_col, nn)

    def spair_copy(q):
        return pltpu.make_async_remote_copy(
            src_ref=one_out.at[2 * q + 1 - core],
            dst_ref=pair_buf.at[q],
            send_sem=spair_send.at[q],
            recv_sem=spair_recv.at[q],
            device_id={"row": row, "col": partner},
            device_id_type=MESH,
        )

    inner = (place == entry).astype(jnp.int32)
    other = side - base

    def far(i):
        return other + (other_entry - other + i + inner) % side

    def sone_copy(to):
        return pltpu.make_async_remote_copy(
            src_ref=one_out.at[2 * to + core],
            dst_ref=one_buf.at[place],
            send_sem=sone_send.at[to],
            recv_sem=sone_recv.at[place],
            device_id={"row": row, "col": 2 * to + core},
            device_id_type=MESH,
        )

    def sone_from(source):
        return pltpu.make_async_remote_copy(
            src_ref=one_out.at[2 * source + core],
            dst_ref=one_buf.at[source],
            send_sem=sone_send.at[source],
            recv_sem=sone_recv.at[source],
            device_id={"row": row, "col": 2 * source + core},
            device_id_type=MESH,
        )

    def pre_copy(source):
        return pltpu.make_async_remote_copy(
            src_ref=one_out.at[2 * other_entry + core],
            dst_ref=pre_buf.at[source - base],
            send_sem=pre_send.at[0],
            recv_sem=pre_recv.at[source - base],
            device_id={"row": row, "col": 2 * entry + core},
            device_id_type=MESH,
        )

    wanted = [far(i) for i in range(side)] + [sibling(j) for j in range(1, side)]
    for q in wanted:
        spair_copy(q).start()
    spair_copy(place).start()
    for i, q in enumerate(wanted):
        spair_copy(q).wait_recv()
        one_out[2 * q + core] = (
            one_out[2 * q + core].astype(f32) + pair_buf[q].astype(f32)
        ).astype(bf16)
        if i in (0, side - 1):
            first = 1 if i == 0 else 0

            @pl.when(inner == first)
            def _():
                sone_copy(q).start()

            if i == 0:

                @pl.when(inner == 0)
                def _():
                    pre_copy(place).start()

        else:
            sone_copy(q).start()

    @pl.when(inner == 1)
    def _():
        share = one_out[2 * other_entry + core].astype(f32)
        for j in range(1, side):
            pre_copy(sibling(j)).wait_recv()
            share = share + pre_buf[sibling(j) - base].astype(f32)
        one_out[2 * other_entry + core] = share.astype(bf16)
        sone_copy(other_entry).start()

    loads[3].wait()
    loads[4].wait()

    def finish(share, level, moment):
        following = momentum_decay * moment[...] + share
        moment[...] = following
        level[...] = level[...] - outer_rate * (share + momentum_decay * following)

    stores = [
        pltpu.make_async_copy(one_v, new_one, out_sem.at[0]),
        pltpu.make_async_copy(two_v, new_two, out_sem.at[1]),
        pltpu.make_async_copy(moment_one, next_one, out_sem.at[2]),
        pltpu.make_async_copy(moment_two, next_two, out_sem.at[3]),
    ]
    share = two_out[row].astype(f32)
    for k in range(1, n_row):
        stwo_copy(k).wait_recv()
        share = share + two_buf[k].astype(f32)
    finish(share / n_row, two_v, moment_two)
    stores[1].start()
    stores[3].start()
    spair_copy(place).wait_recv()
    total = ds.at[pl.ds(0, width // n_col), :]
    total[...] = one_out[col].astype(f32) + pair_buf[place].astype(f32)
    for j in range(1, side):
        sone_from(sibling(j)).wait_recv()
        total[...] += one_buf[sibling(j)].astype(f32)

    @pl.when(inner == 1)
    def _():
        sone_from(other_entry).wait_recv()
        total[...] += one_buf[other_entry].astype(f32)

    @pl.when(inner == 0)
    def _():
        for i in range(side):
            sone_from(far(i)).wait_recv()
            total[...] += one_buf[far(i)].astype(f32)

    finish(total[...] / n_col, one_v, moment_one)
    stores[0].start()
    stores[2].start()

    def sent(u, carry):
        for copy in pair_of(u):
            copy.wait_send()
        return carry

    lax.fori_loop(1, n, sent, 0)
    own_copy(other_entry).wait_send()
    for j in range(1, side):
        own_copy(sibling(j)).wait_send()

    @pl.when(place == entry)
    def _():
        for i in range(side):
            for j in range(1, side):
                relay(beyond(i), sibling(j)).wait_send()

    for q in range(chips):
        across(2 * q + core).wait_send()
        spair_copy(q).wait_send()
    for k in range(1, n_row):
        two_copy(k).wait_send()
        stwo_copy(k).wait_send()
    for j in range(1, side):
        sone_copy(sibling(j)).wait_send()
    for i in range(1, side - 1):
        sone_copy(far(i)).wait_send()

    @pl.when(inner == 1)
    def _():
        for i in sorted({0, side - 1}):
            sone_copy(far(i)).wait_send()

    @pl.when(inner == 0)
    def _():
        sone_copy(far(side - 1)).wait_send()
        pre_copy(place).wait_send()

    for store in stores:
        store.wait()


def pass_kernel(*refs):
    sources, results, held = refs[:4], refs[4:8], refs[8:12]
    in_sem, out_sem = refs[12:]
    arriving = [pltpu.make_async_copy(sources[i], held[i], in_sem.at[i]) for i in range(4)]
    leaving = [pltpu.make_async_copy(held[i], results[i], out_sem.at[i]) for i in range(4)]
    for copy in arriving:
        copy.start()
    for i in range(4):
        arriving[i].wait()
        leaving[i].start()
    for copy in leaving:
        copy.wait()


def shards(docs, routes, level_one, level_two, moment_one, moment_two):
    n_row = lax.axis_size("row")
    n_col = lax.axis_size("col")
    paths = n_row * n_col
    count, length, width = docs.shape
    cap = max(2, (2 * count + paths - 1) // paths)
    lines = length * cap
    kept = (length - 1) * cap
    per = (kept + 7) // 8 * 8
    rows = paths * per
    chips = n_col // 2
    one_rows, two_rows = width // n_col, width // n_row
    vmem = pl.BlockSpec(memory_space=pltpu.VMEM)
    hbm = pl.BlockSpec(memory_space=pl.ANY)
    dma = pltpu.SemaphoreType.DMA
    full = pltpu.VMEM((rows, width), f32)
    thin = pltpu.VMEM((rows, width), bf16)
    side = pltpu.VMEM((rows, 128), f32)
    scratch = [
        pltpu.VMEM((count, length, width), bf16),
        pltpu.VMEM((one_rows, width), f32),
        pltpu.VMEM((two_rows, width), f32),
        pltpu.VMEM((one_rows, width), f32),
        pltpu.VMEM((two_rows, width), f32),
        pltpu.VMEM((paths, lines, width), bf16),
        pltpu.VMEM((paths, 1, 128), f32),
        pltpu.VMEM((paths, lines, width), bf16),
        pltpu.VMEM((paths, 1, 128), f32),
        pltpu.VMEM((n_col, one_rows, width), bf16),
        pltpu.VMEM((n_row, two_rows, width), bf16),
        full, full, full, full, full, thin, thin, thin, thin, thin,
        pltpu.VMEM((rows, rows), bf16),
        pltpu.VMEM((2, width, width), bf16),
        pltpu.VMEM((width, width), f32),
        side, side,
        pltpu.VMEM((n_col, one_rows, width), bf16),
        pltpu.VMEM((n_row, two_rows, width), bf16),
        pltpu.VMEM((chips, one_rows, width), bf16),
        pltpu.VMEM((chips // 2, one_rows, width), bf16),
        pltpu.VMEM((chips, one_rows, width), bf16),
        pltpu.VMEM((n_row, two_rows, width), bf16),
        dma((5,)), dma((paths,)), dma((paths,)), dma((paths,)), dma((paths,)),
        dma((chips,)), dma((chips, chips)), dma((n_col,)), dma((n_col,)), dma((n_col,)),
        dma((n_row,)), dma((n_row,)),
        dma((chips,)), dma((chips,)), dma((1,)), dma((chips // 2,)), dma((chips,)), dma((chips,)),
        dma((n_row,)), dma((n_row,)), dma((4,)),
    ]
    held = sum(
        math.prod(piece.shape) * piece.dtype.itemsize
        for piece in scratch
        if piece.memory_space == pltpu.VMEM
    )
    limit = min(67043328, held + (12 << 20))
    wide_one = jax.ShapeDtypeStruct((one_rows, width), f32)
    wide_two = jax.ShapeDtypeStruct((two_rows, width), f32)
    results = pl.pallas_call(
        functools.partial(round_kernel, n_row, n_col, cap, kept),
        out_shape=(wide_one, wide_two, wide_one, wide_two),
        in_specs=[vmem, hbm, hbm, hbm, hbm, hbm],
        out_specs=(hbm,) * 4,
        scratch_shapes=scratch,
        compiler_params=pltpu.CompilerParams(
            collective_id=0, has_side_effects=True, vmem_limit_bytes=limit
        ),
    )(
        routes.reshape(1, count), docs, level_one[0], level_two[0], moment_one[0], moment_two[0]
    )
    results = pl.pallas_call(
        pass_kernel,
        out_shape=(wide_one, wide_two, wide_one, wide_two),
        in_specs=[hbm] * 4,
        out_specs=(hbm,) * 4,
        scratch_shapes=[
            pltpu.VMEM(piece.shape, piece.dtype) for piece in (wide_one, wide_two, wide_one, wide_two)
        ]
        + [dma((4,)), dma((4,))],
    )(*results)
    return tuple(result[None] for result in results)


def solution(mesh):
    placed = (
        P(("row", "col"), None, None),
        P(("row", "col"), None),
        P("row", "col", None),
        P("col", "row", None),
        P("row", "col", None),
        P("col", "row", None),
    )
    return jax.shard_map(
        shards,
        mesh=mesh,
        in_specs=placed,
        out_specs=(
            P("row", "col", None),
            P("col", "row", None),
            P("row", "col", None),
            P("col", "row", None),
        ),
        check_vma=False,
    )
```

```python
import functools
import math

import jax
import jax.numpy as jnp
from jax import lax
from jax.experimental import pallas as pl
from jax.experimental.pallas import tpu as pltpu
from jax.sharding import PartitionSpec as P

STEPS = 3
BLOCK_COLS = 256

inner_rate = 64.0
outer_rate = 0.7
momentum_decay = 0.9

MESH = pl.DeviceIdType.MESH
f32 = jnp.float32
bf16 = jnp.bfloat16


def product(a, b, i, j):
    return lax.dot_general(a, b, (((i,), (j,)), ((), ())), preferred_element_type=f32)


def column_blocks(width):
    return [(at, min(BLOCK_COLS, width - at)) for at in range(0, width, BLOCK_COLS)]


def fold(values):
    return sum(values[:, at : at + 128] for at in range(0, values.shape[1], 128))


def spread(values, width):
    return jnp.concatenate([values] * (width // 128), axis=1) if width > 128 else values


def round_kernel(
    n_row, n_col, cap, kept,
    route_ref, docs_hbm, one_hbm, two_hbm, moment_one_hbm, moment_two_hbm,
    new_one, new_two, next_one, next_two,
    docs_v, one_v, two_v, moment_one, moment_two, out_ref, cnt_ref, arrived, counts, whole_one, whole_two,
    z, h, g, e, ds, t, xb, hb, eb, db, gram, w2, dw, rx, rr,
    one_out, two_out, pair_buf, pre_buf, one_buf, two_buf,
    load_sem, doc_send, doc_recv, cnt_send, cnt_recv,
    own_send, relay_send, one_recv, pair_send, pair_recv, two_send, two_recv,
    spair_send, spair_recv, pre_send, pre_recv, sone_send, sone_recv, stwo_send, stwo_recv, out_sem,
):
    row, col = lax.axis_index("row"), lax.axis_index("col")
    n = n_row * n_col
    me = row * n_col + col
    chips = n_col // 2
    place, core = col // 2, col % 2
    partner = place * 2 + 1 - core
    side = chips // 2
    upper = place // side
    base = upper * side
    entry = side - 1 + upper
    inner = (place == entry).astype(jnp.int32)
    outer = 1 - inner
    other_entry = side - upper
    lines, width = arrived.shape[1:]
    rows = z.shape[0]
    per = rows // n
    group = 2 * n_row
    half_group = group // 2
    chunk = half_group * per
    chunks = 2 * chips
    early = rows * (chips - 1) // chips // 256 * 256
    count = docs_v.shape[0]
    length = docs_v.shape[1]
    scale = width ** (-0.5)
    blocks = column_blocks(width)
    barrier = pltpu.get_barrier_semaphore()

    loads = [
        pltpu.make_async_copy(one_hbm, one_v, load_sem.at[0]),
        pltpu.make_async_copy(two_hbm, two_v, load_sem.at[1]),
        pltpu.make_async_copy(docs_hbm, docs_v, load_sem.at[2]),
        pltpu.make_async_copy(moment_one_hbm, moment_one, load_sem.at[3]),
        pltpu.make_async_copy(moment_two_hbm, moment_two, load_sem.at[4]),
    ]
    for copy in loads:
        copy.start()

    def greet(k, carry):
        to = (me + k) % n
        pl.semaphore_signal(
            barrier, inc=1, device_id={"row": to // n_col, "col": to % n_col}, device_id_type=MESH
        )
        return carry

    lax.fori_loop(1, n, greet, 0)
    loads[0].wait()
    whole_one[col] = one_v[...].astype(bf16)
    loads[1].wait()
    whole_two[row] = two_v[...].astype(bf16)

    pl.semaphore_wait(barrier, n - 1)

    def own_copy(to):
        return pltpu.make_async_remote_copy(
            src_ref=whole_one.at[col],
            dst_ref=whole_one.at[col],
            send_sem=own_send.at[to],
            recv_sem=one_recv.at[col],
            device_id={"row": row, "col": 2 * to + core},
            device_id_type=MESH,
        )

    def relay(source, to):
        block = 2 * source + core
        return pltpu.make_async_remote_copy(
            src_ref=whole_one.at[block],
            dst_ref=whole_one.at[block],
            send_sem=relay_send.at[source, to],
            recv_sem=one_recv.at[block],
            device_id={"row": row, "col": 2 * to + core},
            device_id_type=MESH,
        )

    def sibling(j):
        return base + (place - base + j) % side

    def beyond(i):
        return (1 - upper) * (side + i) + upper * (side - 1 - i)

    def across(block):
        return pltpu.make_async_remote_copy(
            src_ref=whole_one.at[block],
            dst_ref=whole_one.at[block],
            send_sem=pair_send.at[block],
            recv_sem=pair_recv.at[block],
            device_id={"row": row, "col": partner},
            device_id_type=MESH,
        )

    def two_copy(k):
        return pltpu.make_async_remote_copy(
            src_ref=whole_two.at[row],
            dst_ref=whole_two.at[row],
            send_sem=two_send.at[k],
            recv_sem=two_recv.at[k],
            device_id={"row": (row + k) % n_row, "col": col},
            device_id_type=MESH,
        )

    def two_wait(k):
        from_row = (row - k + n_row) % n_row
        return pltpu.make_async_remote_copy(
            src_ref=whole_two.at[row],
            dst_ref=whole_two.at[from_row],
            send_sem=two_send.at[k],
            recv_sem=two_recv.at[k],
            device_id={"row": (row + k) % n_row, "col": col},
            device_id_type=MESH,
        )

    own_copy(other_entry).start()
    for j in range(1, side):
        own_copy(sibling(j)).start()
    across(col).start()
    for k in range(1, n_row):
        two_copy(k).start()

    target = route_ref[...]
    named = jnp.broadcast_to(target.astype(f32), (count, count))
    earlier = lax.broadcasted_iota(jnp.int32, (count, count), 0) < lax.broadcasted_iota(
        jnp.int32, (count, count), 1
    )
    rank = jnp.sum(jnp.where((named.T == named) & earlier, 1.0, 0.0), axis=0, keepdims=True)
    slot = target * cap + rank.astype(jnp.int32)
    slots = lax.broadcasted_iota(jnp.int32, (n * cap, count), 0)
    dispatch = jnp.where(slots == slot, 1.0, 0.0).astype(bf16)
    path = lax.broadcasted_iota(jnp.int32, (n, 1, count), 0)
    mine = jnp.where(jnp.broadcast_to(target[None], (n, 1, count)) == path, 1.0, 0.0)
    cnt_ref[...] = jnp.broadcast_to(jnp.sum(mine, axis=-1, keepdims=True), cnt_ref.shape)

    loads[2].wait()
    docs = jnp.swapaxes(docs_v[...], 0, 1)
    for step in range(length):
        sent = jnp.dot(dispatch, docs[step], preferred_element_type=f32)
        out_ref[:, step * cap : (step + 1) * cap, :] = sent.reshape(n, cap, width).astype(bf16)

    def pair_of(u):
        to_row = (row + u % n_row) % n_row
        to_col = (place + u // group) % chips * 2 + (core + u // n_row) % 2
        to = to_row * n_col + to_col
        peer = {"row": to_row, "col": to_col}
        return (
            pltpu.make_async_remote_copy(
                src_ref=out_ref.at[to],
                dst_ref=arrived.at[u],
                send_sem=doc_send.at[u],
                recv_sem=doc_recv.at[u],
                device_id=peer,
                device_id_type=MESH,
            ),
            pltpu.make_async_remote_copy(
                src_ref=cnt_ref.at[to],
                dst_ref=counts.at[u],
                send_sem=cnt_send.at[u],
                recv_sem=cnt_recv.at[u],
                device_id=peer,
                device_id_type=MESH,
            ),
        )

    def apart(k, mixed, flip):
        near = k + mixed * (k * 2 % chips + k // (chips // 2) - k)
        return (near + flip * (chips - 2 * near)) % chips

    def send_docs(first, last):
        def body(u, carry):
            for copy in pair_of(u):
                copy.start()
            return carry

        lax.fori_loop(first, last, body, 0)

    arrived[0] = out_ref[me]
    counts[0] = cnt_ref[me]
    send_docs(1, group)

    def send_group(k):
        at = apart(k, inner, upper) * group
        send_docs(at, at + group)

    for k in range(1, chips - 1):
        send_group(k)

    @pl.when(place == entry)
    def _():
        for i in range(side):
            source = beyond(i)
            relay(source, place).wait_recv()
            across(2 * source + core).start()
            for j in range(1, side):
                relay(source, sibling(j)).start()

    send_group(chips - 1)
    for j in range(1, side):
        relay(sibling(j), place).wait_recv()
        across(2 * sibling(j) + core).start()

    @pl.when(place != entry)
    def _():
        for i in range(side):
            relay(beyond(i), place).wait_recv()
            across(2 * beyond(i) + core).start()

    for q in range(chips):
        across(2 * q + 1 - core).wait_recv()
    for k in range(1, n_row):
        two_wait(k).wait_recv()

    def place_of(k):
        flip = upper * inner + (1 - upper) * outer
        return apart(k // 2, outer, flip) * group + k % 2 * half_group

    def arrive(first, last):
        def body(u, carry):
            for copy in pair_of(u):
                copy.wait_recv()
            return carry

        lax.fori_loop(first, last, body, 0)

    def unpack(k, at):
        block = arrived[pl.ds(place_of(k), half_group)].astype(f32)
        if per == kept:
            first, last = block[:, :kept], block[:, lines - kept :]
        else:
            live = lax.broadcasted_iota(jnp.int32, block.shape, 1) < kept
            first = jnp.where(live, block, 0.0)[:, :per]
            last = jnp.where(live, pltpu.roll(block, kept, 1), 0.0)[:, :per]
        first = first.reshape(chunk, width)
        xb[at, :] = first.astype(bf16)
        t[at, :] = last.reshape(chunk, width).astype(bf16)
        size = jnp.sum(fold(first * first), axis=-1, keepdims=True) * (1.0 / width)
        rx[at, :] = jnp.broadcast_to(lax.rsqrt(size + 1e-06), (chunk, 128))

    def hidden(at, start):
        size = jnp.zeros((at.size, 128), f32)
        for n0, nn in blocks:
            cols = pl.ds(n0, nn)
            zz = start(cols, nn)
            z[at, cols] = zz
            gate = 1.0 / (1.0 + jnp.exp(-zz))
            act = zz * gate
            hh = xb[at, cols].astype(f32) + act
            h[at, cols] = hh
            hb[at, cols] = hh.astype(bf16)
            g[at, cols] = gate + act * (1.0 - gate)
            size = size + fold(hh * hh)
        size = jnp.sum(size, axis=-1, keepdims=True) * (1.0 / width)
        rr[at, :] = jnp.broadcast_to(lax.rsqrt(size + 1e-06), (at.size, 128))

    def errors(at, weights):
        r = rr[at, :]
        both = jnp.zeros((at.size, 128), f32)
        for n0, nn in blocks:
            cols = pl.ds(n0, nn)
            pp = product(hb[at, :], weights(cols), 1, 0)
            rw = spread(r, nn)
            ee = h[at, cols] + scale * rw * pp - t[at, cols].astype(f32)
            er = ee * rw
            e[at, cols] = ee
            eb[at, cols] = er.astype(bf16)
            both = both + fold(er * pp)
        both = jnp.sum(both, axis=-1, keepdims=True) * (1.0 / width)
        rr[at, :] = jnp.broadcast_to(both, (at.size, 128)) * r * r

    def slopes(at, weights, turn):
        m, rw = rr[at, :], rx[at, :]
        for n0, nn in blocks:
            cols = pl.ds(n0, nn)
            qq = product(eb[at, :], weights(cols), 1, 1)
            dd = (e[at, cols] + scale * (qq - h[at, cols] * spread(m, nn))) * g[at, cols]
            dd = dd * spread(rw, nn)
            if turn is None:
                ds[at, cols] = dd
                db[at, cols] = dd.astype(bf16)
            else:
                total = ds[at, cols] + dd
                ds[at, cols] = total
                db[at, cols] = jnp.where(turn == STEPS - 1, total, dd).astype(bf16)


    def two_cols(cols):
        return whole_two[:, :, cols].reshape(width, cols.size)

    def two_rows(cols):
        return whole_two[...].reshape(width, width)[cols.start : cols.start + cols.size]

    arrive(1, half_group)
    low, high = pl.ds(0, early), pl.ds(early, rows - early)

    def first_turn(k, carry):
        at = pl.ds(pl.multiple_of(k * chunk, chunk), chunk)
        unpack(k, at)

        def start(cols, nn):
            zz = product(xb[at, :], whole_one[:, :, cols].reshape(width, nn), 1, 0)
            return scale * spread(rx[at, :], nn) * zz

        hidden(at, start)
        errors(at, two_cols)
        slopes(at, two_rows, None)

        @pl.when(k == chunks - 3)
        def _():
            gram[low, low] = product(xb[low, :], xb[low, :], 1, 1).astype(bf16)
            for n0, nn in blocks:
                cols = pl.ds(n0, nn)
                dw[:, cols] = product(hb[low, :], eb[low, cols], 0, 0)

        @pl.when(k < chunks - 1)
        def _():
            first = place_of(k + 1)
            arrive(first, first + half_group)

        return carry

    lax.fori_loop(0, chunks, first_turn, 0)
    gram[high, :] = product(xb[high, :], xb[...], 1, 1).astype(bf16)
    gram[low, high] = product(xb[low, :], xb[high, :], 1, 1).astype(bf16)

    filled = jnp.sum(counts[...].reshape(n, 128), axis=0, keepdims=True)[:, :1]
    rate = inner_rate * scale / (filled * (length - 1))

    for n0, nn in blocks:
        cols = pl.ds(n0, nn)
        change = dw[:, cols] + product(hb[high, :], eb[high, cols], 0, 0)
        dw[:, cols] = change
        w2[1, :, cols] = (two_cols(cols).astype(f32) - rate * change).astype(bf16)

    everything = pl.ds(0, rows)

    def stwo_copy(k):
        to = (row + k) % n_row
        return pltpu.make_async_remote_copy(
            src_ref=two_out.at[to],
            dst_ref=two_buf.at[k],
            send_sem=stwo_send.at[k],
            recv_sem=stwo_recv.at[k],
            device_id={"row": to, "col": col},
            device_id_type=MESH,
        )

    def later_turn(turn, carry):
        now, later = turn % 2, (turn + 1) % 2

        def start(cols, nn):
            step = product(gram[...], db[:, cols], 1, 0)
            return z[:, cols] - (rate * scale) * spread(rx[...], nn) * step

        hidden(everything, start)
        errors(everything, lambda cols: w2[now, :, cols])
        for n0, nn in blocks:
            cols = pl.ds(n0, nn)
            change = dw[:, cols] + product(hb[...], eb[:, cols], 0, 0)
            dw[:, cols] = change
            change = rate * change
            w2[later, :, cols] = (two_cols(cols).astype(f32) - change).astype(bf16)
            two_out[:, :, cols] = change.astype(bf16).reshape(n_row, width // n_row, nn)

        @pl.when(turn == STEPS - 1)
        def _():
            for k in range(1, n_row):
                stwo_copy(k).start()

        slopes(everything, lambda cols: w2[now, cols, :], turn)
        return carry

    lax.fori_loop(1, STEPS, later_turn, 0)

    for n0, nn in blocks:
        cols = pl.ds(n0, nn)
        change = rate * product(xb[...], db[:, cols], 0, 0)
        one_out[:, :, cols] = change.astype(bf16).reshape(n_col, width // n_col, nn)

    def spair_copy(q):
        return pltpu.make_async_remote_copy(
            src_ref=one_out.at[2 * q + 1 - core],
            dst_ref=pair_buf.at[q],
            send_sem=spair_send.at[q],
            recv_sem=spair_recv.at[q],
            device_id={"row": row, "col": partner},
            device_id_type=MESH,
        )

    other = side - base

    def far(i):
        return other + (other_entry - other + i + inner) % side

    def sone_copy(to):
        return pltpu.make_async_remote_copy(
            src_ref=one_out.at[2 * to + core],
            dst_ref=one_buf.at[place],
            send_sem=sone_send.at[to],
            recv_sem=sone_recv.at[place],
            device_id={"row": row, "col": 2 * to + core},
            device_id_type=MESH,
        )

    def sone_from(source):
        return pltpu.make_async_remote_copy(
            src_ref=one_out.at[2 * source + core],
            dst_ref=one_buf.at[source],
            send_sem=sone_send.at[source],
            recv_sem=sone_recv.at[source],
            device_id={"row": row, "col": 2 * source + core},
            device_id_type=MESH,
        )

    def pre_copy(source):
        return pltpu.make_async_remote_copy(
            src_ref=one_out.at[2 * other_entry + core],
            dst_ref=pre_buf.at[source - base],
            send_sem=pre_send.at[0],
            recv_sem=pre_recv.at[source - base],
            device_id={"row": row, "col": 2 * entry + core},
            device_id_type=MESH,
        )

    wanted = [far(i) for i in range(side)] + [sibling(j) for j in range(1, side)]
    for q in wanted:
        spair_copy(q).start()
    spair_copy(place).start()
    for i, q in enumerate(wanted):
        spair_copy(q).wait_recv()
        one_out[2 * q + core] = (
            one_out[2 * q + core].astype(f32) + pair_buf[q].astype(f32)
        ).astype(bf16)
        if i in (0, side - 1):
            first = 1 if i == 0 else 0

            @pl.when(inner == first)
            def _():
                sone_copy(q).start()

            if i == 0:

                @pl.when(inner == 0)
                def _():
                    pre_copy(place).start()

        else:
            sone_copy(q).start()

    @pl.when(inner == 1)
    def _():
        share = one_out[2 * other_entry + core].astype(f32)
        for j in range(1, side):
            pre_copy(sibling(j)).wait_recv()
            share = share + pre_buf[sibling(j) - base].astype(f32)
        one_out[2 * other_entry + core] = share.astype(bf16)
        sone_copy(other_entry).start()

    loads[3].wait()
    loads[4].wait()

    def finish(share, level, moment):
        following = momentum_decay * moment[...] + share
        moment[...] = following
        level[...] = level[...] - outer_rate * (share + momentum_decay * following)

    stores = [
        pltpu.make_async_copy(one_v, new_one, out_sem.at[0]),
        pltpu.make_async_copy(two_v, new_two, out_sem.at[1]),
        pltpu.make_async_copy(moment_one, next_one, out_sem.at[2]),
        pltpu.make_async_copy(moment_two, next_two, out_sem.at[3]),
    ]
    share = two_out[row].astype(f32)
    for k in range(1, n_row):
        stwo_copy(k).wait_recv()
        share = share + two_buf[k].astype(f32)
    finish(share / n_row, two_v, moment_two)
    stores[1].start()
    stores[3].start()
    spair_copy(place).wait_recv()
    total = ds.at[pl.ds(0, width // n_col), :]
    total[...] = one_out[col].astype(f32) + pair_buf[place].astype(f32)
    for j in range(1, side):
        sone_from(sibling(j)).wait_recv()
        total[...] += one_buf[sibling(j)].astype(f32)

    @pl.when(inner == 1)
    def _():
        sone_from(other_entry).wait_recv()
        total[...] += one_buf[other_entry].astype(f32)

    @pl.when(inner == 0)
    def _():
        for i in range(side):
            sone_from(far(i)).wait_recv()
            total[...] += one_buf[far(i)].astype(f32)

    finish(total[...] / n_col, one_v, moment_one)
    stores[0].start()
    stores[2].start()

    def sent(u, carry):
        for copy in pair_of(u):
            copy.wait_send()
        return carry

    lax.fori_loop(1, n, sent, 0)
    own_copy(other_entry).wait_send()
    for j in range(1, side):
        own_copy(sibling(j)).wait_send()

    @pl.when(place == entry)
    def _():
        for i in range(side):
            for j in range(1, side):
                relay(beyond(i), sibling(j)).wait_send()

    for q in range(chips):
        across(2 * q + core).wait_send()
        spair_copy(q).wait_send()
    for k in range(1, n_row):
        two_copy(k).wait_send()
        stwo_copy(k).wait_send()
    for j in range(1, side):
        sone_copy(sibling(j)).wait_send()
    for i in range(1, side - 1):
        sone_copy(far(i)).wait_send()

    @pl.when(inner == 1)
    def _():
        for i in sorted({0, side - 1}):
            sone_copy(far(i)).wait_send()

    @pl.when(inner == 0)
    def _():
        sone_copy(far(side - 1)).wait_send()
        pre_copy(place).wait_send()

    for store in stores:
        store.wait()


def pass_kernel(*refs):
    sources, results, held = refs[:4], refs[4:8], refs[8:12]
    in_sem, out_sem = refs[12:]
    arriving = [pltpu.make_async_copy(sources[i], held[i], in_sem.at[i]) for i in range(4)]
    leaving = [pltpu.make_async_copy(held[i], results[i], out_sem.at[i]) for i in range(4)]
    for copy in arriving:
        copy.start()
    for i in range(4):
        arriving[i].wait()
        leaving[i].start()
    for copy in leaving:
        copy.wait()


def shards(docs, routes, level_one, level_two, moment_one, moment_two):
    n_row = lax.axis_size("row")
    n_col = lax.axis_size("col")
    paths = n_row * n_col
    count, length, width = docs.shape
    cap = max(2, (2 * count + paths - 1) // paths)
    lines = length * cap
    kept = (length - 1) * cap
    per = (kept + 7) // 8 * 8
    rows = paths * per
    chips = n_col // 2
    one_rows, two_rows = width // n_col, width // n_row
    vmem = pl.BlockSpec(memory_space=pltpu.VMEM)
    hbm = pl.BlockSpec(memory_space=pl.ANY)
    dma = pltpu.SemaphoreType.DMA
    full = pltpu.VMEM((rows, width), f32)
    thin = pltpu.VMEM((rows, width), bf16)
    side = pltpu.VMEM((rows, 128), f32)
    scratch = [
        pltpu.VMEM((count, length, width), bf16),
        pltpu.VMEM((one_rows, width), f32),
        pltpu.VMEM((two_rows, width), f32),
        pltpu.VMEM((one_rows, width), f32),
        pltpu.VMEM((two_rows, width), f32),
        pltpu.VMEM((paths, lines, width), bf16),
        pltpu.VMEM((paths, 1, 128), f32),
        pltpu.VMEM((paths, lines, width), bf16),
        pltpu.VMEM((paths, 1, 128), f32),
        pltpu.VMEM((n_col, one_rows, width), bf16),
        pltpu.VMEM((n_row, two_rows, width), bf16),
        full, full, full, full, full, thin, thin, thin, thin, thin,
        pltpu.VMEM((rows, rows), bf16),
        pltpu.VMEM((2, width, width), bf16),
        pltpu.VMEM((width, width), f32),
        side, side,
        pltpu.VMEM((n_col, one_rows, width), bf16),
        pltpu.VMEM((n_row, two_rows, width), bf16),
        pltpu.VMEM((chips, one_rows, width), bf16),
        pltpu.VMEM((chips // 2, one_rows, width), bf16),
        pltpu.VMEM((chips, one_rows, width), bf16),
        pltpu.VMEM((n_row, two_rows, width), bf16),
        dma((5,)), dma((paths,)), dma((paths,)), dma((paths,)), dma((paths,)),
        dma((chips,)), dma((chips, chips)), dma((n_col,)), dma((n_col,)), dma((n_col,)),
        dma((n_row,)), dma((n_row,)),
        dma((chips,)), dma((chips,)), dma((1,)), dma((chips // 2,)), dma((chips,)), dma((chips,)),
        dma((n_row,)), dma((n_row,)), dma((4,)),
    ]
    held = sum(
        math.prod(piece.shape) * piece.dtype.itemsize
        for piece in scratch
        if piece.memory_space == pltpu.VMEM
    )
    limit = min(67043328, held + (12 << 20))
    wide_one = jax.ShapeDtypeStruct((one_rows, width), f32)
    wide_two = jax.ShapeDtypeStruct((two_rows, width), f32)
    results = pl.pallas_call(
        functools.partial(round_kernel, n_row, n_col, cap, kept),
        out_shape=(wide_one, wide_two, wide_one, wide_two),
        in_specs=[vmem, hbm, hbm, hbm, hbm, hbm],
        out_specs=(hbm,) * 4,
        scratch_shapes=scratch,
        compiler_params=pltpu.CompilerParams(
            collective_id=0, has_side_effects=True, vmem_limit_bytes=limit
        ),
    )(
        routes.reshape(1, count), docs, level_one[0], level_two[0], moment_one[0], moment_two[0]
    )
    results = pl.pallas_call(
        pass_kernel,
        out_shape=(wide_one, wide_two, wide_one, wide_two),
        in_specs=[hbm] * 4,
        out_specs=(hbm,) * 4,
        scratch_shapes=[
            pltpu.VMEM(piece.shape, piece.dtype) for piece in (wide_one, wide_two, wide_one, wide_two)
        ]
        + [dma((4,)), dma((4,))],
    )(*results)
    return tuple(result[None] for result in results)


def solution(mesh):
    placed = (
        P(("row", "col"), None, None),
        P(("row", "col"), None),
        P("row", "col", None),
        P("col", "row", None),
        P("row", "col", None),
        P("col", "row", None),
    )
    return jax.shard_map(
        shards,
        mesh=mesh,
        in_specs=placed,
        out_specs=(
            P("row", "col", None),
            P("col", "row", None),
            P("row", "col", None),
            P("col", "row", None),
        ),
        check_vma=False,
    )
```

```python
import functools
import math

import jax
import jax.numpy as jnp
from jax import lax
from jax.experimental import pallas as pl
from jax.experimental.pallas import tpu as pltpu
from jax.sharding import PartitionSpec as P

STEPS = 3
BLOCK_COLS = 256

inner_rate = 64.0
outer_rate = 0.7
momentum_decay = 0.9

MESH = pl.DeviceIdType.MESH
f32 = jnp.float32
bf16 = jnp.bfloat16


def product(a, b, i, j):
    return lax.dot_general(a, b, (((i,), (j,)), ((), ())), preferred_element_type=f32)


def column_blocks(width):
    return [(at, min(BLOCK_COLS, width - at)) for at in range(0, width, BLOCK_COLS)]


def fold(values):
    return sum(values[:, at : at + 128] for at in range(0, values.shape[1], 128))


def spread(values, width):
    return jnp.concatenate([values] * (width // 128), axis=1) if width > 128 else values


def round_kernel(
    n_row, n_col, cap, kept,
    route_ref, docs_hbm, one_hbm, two_hbm, moment_one_hbm, moment_two_hbm,
    new_one, new_two, next_one, next_two,
    docs_v, out_ref, cnt_ref, arrived, counts, whole_one, whole_two,
    z, h, g, e, ds, t, xb, hb, eb, db, gram, w2, dw, rx, rr,
    one_out, two_out, pair_buf, pre_buf, one_buf, two_buf,
    load_sem, doc_send, doc_recv, cnt_send, cnt_recv,
    own_send, relay_send, one_recv, pair_send, pair_recv, two_send, two_recv,
    spair_send, spair_recv, pre_send, pre_recv, sone_send, sone_recv, stwo_send, stwo_recv,
):
    row, col = lax.axis_index("row"), lax.axis_index("col")
    n = n_row * n_col
    me = row * n_col + col
    chips = n_col // 2
    place, core = col // 2, col % 2
    partner = place * 2 + 1 - core
    side = chips // 2
    upper = place // side
    base = upper * side
    entry = side - 1 + upper
    inner = (place == entry).astype(jnp.int32)
    outer = 1 - inner
    other_entry = side - upper
    lines, width = arrived.shape[1:]
    rows = z.shape[0]
    per = rows // n
    group = 2 * n_row
    half_group = group // 2
    chunk = half_group * per
    chunks = 2 * chips
    early = rows * (chips - 1) // chips // 256 * 256
    count = docs_v.shape[0]
    length = docs_v.shape[1]
    scale = width ** (-0.5)
    blocks = column_blocks(width)
    barrier = pltpu.get_barrier_semaphore()

    loads = [
        pltpu.make_async_copy(one_hbm, new_one, load_sem.at[0]),
        pltpu.make_async_copy(two_hbm, new_two, load_sem.at[1]),
        pltpu.make_async_copy(docs_hbm, docs_v, load_sem.at[2]),
        pltpu.make_async_copy(moment_one_hbm, next_one, load_sem.at[3]),
        pltpu.make_async_copy(moment_two_hbm, next_two, load_sem.at[4]),
    ]
    for copy in loads:
        copy.start()

    def greet(k, carry):
        to = (me + k) % n
        pl.semaphore_signal(
            barrier, inc=1, device_id={"row": to // n_col, "col": to % n_col}, device_id_type=MESH
        )
        return carry

    lax.fori_loop(1, n, greet, 0)
    loads[0].wait()
    whole_one[col] = new_one[...].astype(bf16)
    loads[1].wait()
    whole_two[row] = new_two[...].astype(bf16)

    pl.semaphore_wait(barrier, n - 1)

    def own_copy(to):
        return pltpu.make_async_remote_copy(
            src_ref=whole_one.at[col],
            dst_ref=whole_one.at[col],
            send_sem=own_send.at[to],
            recv_sem=one_recv.at[col],
            device_id={"row": row, "col": 2 * to + core},
            device_id_type=MESH,
        )

    def relay(source, to):
        block = 2 * source + core
        return pltpu.make_async_remote_copy(
            src_ref=whole_one.at[block],
            dst_ref=whole_one.at[block],
            send_sem=relay_send.at[source, to],
            recv_sem=one_recv.at[block],
            device_id={"row": row, "col": 2 * to + core},
            device_id_type=MESH,
        )

    def sibling(j):
        return base + (place - base + j) % side

    def beyond(i):
        return (1 - upper) * (side + i) + upper * (side - 1 - i)

    def across(block):
        return pltpu.make_async_remote_copy(
            src_ref=whole_one.at[block],
            dst_ref=whole_one.at[block],
            send_sem=pair_send.at[block],
            recv_sem=pair_recv.at[block],
            device_id={"row": row, "col": partner},
            device_id_type=MESH,
        )

    def two_copy(k):
        return pltpu.make_async_remote_copy(
            src_ref=whole_two.at[row],
            dst_ref=whole_two.at[row],
            send_sem=two_send.at[k],
            recv_sem=two_recv.at[k],
            device_id={"row": (row + k) % n_row, "col": col},
            device_id_type=MESH,
        )

    def two_wait(k):
        from_row = (row - k + n_row) % n_row
        return pltpu.make_async_remote_copy(
            src_ref=whole_two.at[row],
            dst_ref=whole_two.at[from_row],
            send_sem=two_send.at[k],
            recv_sem=two_recv.at[k],
            device_id={"row": (row + k) % n_row, "col": col},
            device_id_type=MESH,
        )

    own_copy(other_entry).start()
    for j in range(1, side):
        own_copy(sibling(j)).start()
    across(col).start()
    for k in range(1, n_row):
        two_copy(k).start()

    target = route_ref[...]
    named = jnp.broadcast_to(target.astype(f32), (count, count))
    earlier = lax.broadcasted_iota(jnp.int32, (count, count), 0) < lax.broadcasted_iota(
        jnp.int32, (count, count), 1
    )
    rank = jnp.sum(jnp.where((named.T == named) & earlier, 1.0, 0.0), axis=0, keepdims=True)
    slot = target * cap + rank.astype(jnp.int32)
    slots = lax.broadcasted_iota(jnp.int32, (n * cap, count), 0)
    dispatch = jnp.where(slots == slot, 1.0, 0.0).astype(bf16)
    path = lax.broadcasted_iota(jnp.int32, (n, 1, count), 0)
    mine = jnp.where(jnp.broadcast_to(target[None], (n, 1, count)) == path, 1.0, 0.0)
    cnt_ref[...] = jnp.broadcast_to(jnp.sum(mine, axis=-1, keepdims=True), cnt_ref.shape)

    loads[2].wait()
    docs = jnp.swapaxes(docs_v[...], 0, 1)
    for step in range(length):
        sent = jnp.dot(dispatch, docs[step], preferred_element_type=f32)
        out_ref[:, step * cap : (step + 1) * cap, :] = sent.reshape(n, cap, width).astype(bf16)

    def pair_of(u):
        to_row = (row + u % n_row) % n_row
        to_col = (place + u // group) % chips * 2 + (core + u // n_row) % 2
        to = to_row * n_col + to_col
        peer = {"row": to_row, "col": to_col}
        return (
            pltpu.make_async_remote_copy(
                src_ref=out_ref.at[to],
                dst_ref=arrived.at[u],
                send_sem=doc_send.at[u],
                recv_sem=doc_recv.at[u],
                device_id=peer,
                device_id_type=MESH,
            ),
            pltpu.make_async_remote_copy(
                src_ref=cnt_ref.at[to],
                dst_ref=counts.at[u],
                send_sem=cnt_send.at[u],
                recv_sem=cnt_recv.at[u],
                device_id=peer,
                device_id_type=MESH,
            ),
        )

    def apart(k, flip):
        return (k + flip * (chips - 2 * k)) % chips

    def send_docs(first, last):
        def body(u, carry):
            for copy in pair_of(u):
                copy.start()
            return carry

        lax.fori_loop(first, last, body, 0)

    arrived[0] = out_ref[me]
    counts[0] = cnt_ref[me]
    send_docs(1, group)

    for k in range(1, chips - 1):
        at = apart(k, upper) * group
        send_docs(at, at + group)
    at = apart(chips - 1, upper) * group
    send_docs(at, at + half_group)

    @pl.when(place == entry)
    def _():
        for i in range(side):
            source = beyond(i)
            relay(source, place).wait_recv()
            across(2 * source + core).start()
            for j in range(1, side):
                relay(source, sibling(j)).start()

    send_docs(at + half_group, at + group)
    for j in range(1, side):
        relay(sibling(j), place).wait_recv()
        across(2 * sibling(j) + core).start()

    @pl.when(place != entry)
    def _():
        for i in range(side):
            relay(beyond(i), place).wait_recv()
            across(2 * beyond(i) + core).start()

    for q in range(chips):
        across(2 * q + 1 - core).wait_recv()
    for k in range(1, n_row):
        two_wait(k).wait_recv()

    def place_of(k):
        flip = upper * inner + (1 - upper) * outer
        return apart(k // 2, flip) * group + k % 2 * half_group

    def arrive(first, last):
        def body(u, carry):
            for copy in pair_of(u):
                copy.wait_recv()
            return carry

        lax.fori_loop(first, last, body, 0)

    def unpack(k, at):
        block = arrived[pl.ds(place_of(k), half_group)].astype(f32)
        if per == kept:
            first, last = block[:, :kept], block[:, lines - kept :]
        else:
            live = lax.broadcasted_iota(jnp.int32, block.shape, 1) < kept
            first = jnp.where(live, block, 0.0)[:, :per]
            last = jnp.where(live, pltpu.roll(block, kept, 1), 0.0)[:, :per]
        first = first.reshape(chunk, width)
        xb[at, :] = first.astype(bf16)
        t[at, :] = last.reshape(chunk, width).astype(bf16)
        size = jnp.sum(fold(first * first), axis=-1, keepdims=True) * (1.0 / width)
        rx[at, :] = jnp.broadcast_to(lax.rsqrt(size + 1e-06), (chunk, 128))

    def hidden(at, start):
        size = jnp.zeros((at.size, 128), f32)
        for n0, nn in blocks:
            cols = pl.ds(n0, nn)
            zz = start(cols, nn)
            z[at, cols] = zz
            gate = 1.0 / (1.0 + jnp.exp(-zz))
            act = zz * gate
            hh = xb[at, cols].astype(f32) + act
            h[at, cols] = hh
            hb[at, cols] = hh.astype(bf16)
            g[at, cols] = gate + act * (1.0 - gate)
            size = size + fold(hh * hh)
        size = jnp.sum(size, axis=-1, keepdims=True) * (1.0 / width)
        rr[at, :] = jnp.broadcast_to(lax.rsqrt(size + 1e-06), (at.size, 128))

    def errors(at, weights):
        r = rr[at, :]
        both = jnp.zeros((at.size, 128), f32)
        for n0, nn in blocks:
            cols = pl.ds(n0, nn)
            pp = product(hb[at, :], weights(cols), 1, 0)
            rw = spread(r, nn)
            ee = h[at, cols] + scale * rw * pp - t[at, cols].astype(f32)
            er = ee * rw
            e[at, cols] = ee
            eb[at, cols] = er.astype(bf16)
            both = both + fold(er * pp)
        both = jnp.sum(both, axis=-1, keepdims=True) * (1.0 / width)
        rr[at, :] = jnp.broadcast_to(both, (at.size, 128)) * r * r

    def slopes(at, weights, turn):
        m, rw = rr[at, :], rx[at, :]
        for n0, nn in blocks:
            cols = pl.ds(n0, nn)
            qq = product(eb[at, :], weights(cols), 1, 1)
            dd = (e[at, cols] + scale * (qq - h[at, cols] * spread(m, nn))) * g[at, cols]
            dd = dd * spread(rw, nn)
            if turn is None:
                ds[at, cols] = dd
                db[at, cols] = dd.astype(bf16)
            else:
                total = ds[at, cols] + dd
                ds[at, cols] = total
                db[at, cols] = jnp.where(turn == STEPS - 1, total, dd).astype(bf16)


    def two_cols(cols):
        return whole_two[:, :, cols].reshape(width, cols.size)

    def two_rows(cols):
        return whole_two[...].reshape(width, width)[cols.start : cols.start + cols.size]

    arrive(1, half_group)
    low, high = pl.ds(0, early), pl.ds(early, rows - early)

    def first_turn(k, carry):
        at = pl.ds(pl.multiple_of(k * chunk, chunk), chunk)
        unpack(k, at)

        def start(cols, nn):
            zz = product(xb[at, :], whole_one[:, :, cols].reshape(width, nn), 1, 0)
            return scale * spread(rx[at, :], nn) * zz

        hidden(at, start)
        errors(at, two_cols)
        slopes(at, two_rows, None)

        @pl.when(k == chunks - 3)
        def _():
            gram[low, low] = product(xb[low, :], xb[low, :], 1, 1).astype(bf16)
            for n0, nn in blocks:
                cols = pl.ds(n0, nn)
                dw[:, cols] = product(hb[low, :], eb[low, cols], 0, 0)

        @pl.when(k < chunks - 1)
        def _():
            first = place_of(k + 1)
            arrive(first, first + half_group)

        return carry

    lax.fori_loop(0, chunks, first_turn, 0)
    gram[high, :] = product(xb[high, :], xb[...], 1, 1).astype(bf16)
    gram[low, high] = product(xb[low, :], xb[high, :], 1, 1).astype(bf16)

    filled = jnp.sum(counts[...].reshape(n, 128), axis=0, keepdims=True)[:, :1]
    rate = inner_rate * scale / (filled * (length - 1))

    for n0, nn in blocks:
        cols = pl.ds(n0, nn)
        change = dw[:, cols] + product(hb[high, :], eb[high, cols], 0, 0)
        dw[:, cols] = change
        w2[1, :, cols] = (two_cols(cols).astype(f32) - rate * change).astype(bf16)

    everything = pl.ds(0, rows)

    def stwo_copy(k):
        to = (row + k) % n_row
        return pltpu.make_async_remote_copy(
            src_ref=two_out.at[to],
            dst_ref=two_buf.at[k],
            send_sem=stwo_send.at[k],
            recv_sem=stwo_recv.at[k],
            device_id={"row": to, "col": col},
            device_id_type=MESH,
        )

    def later_turn(turn, carry):
        now, later = turn % 2, (turn + 1) % 2

        def start(cols, nn):
            step = product(gram[...], db[:, cols], 1, 0)
            return z[:, cols] - (rate * scale) * spread(rx[...], nn) * step

        hidden(everything, start)
        errors(everything, lambda cols: w2[now, :, cols])
        for n0, nn in blocks:
            cols = pl.ds(n0, nn)
            change = dw[:, cols] + product(hb[...], eb[:, cols], 0, 0)
            dw[:, cols] = change
            change = rate * change
            w2[later, :, cols] = (two_cols(cols).astype(f32) - change).astype(bf16)
            two_out[:, :, cols] = change.astype(bf16).reshape(n_row, width // n_row, nn)

        @pl.when(turn == STEPS - 1)
        def _():
            for k in range(1, n_row):
                stwo_copy(k).start()

        slopes(everything, lambda cols: w2[now, cols, :], turn)
        return carry

    lax.fori_loop(1, STEPS, later_turn, 0)

    for n0, nn in blocks:
        cols = pl.ds(n0, nn)
        change = rate * product(xb[...], db[:, cols], 0, 0)
        one_out[:, :, cols] = change.astype(bf16).reshape(n_col, width // n_col, nn)

    def spair_copy(q):
        return pltpu.make_async_remote_copy(
            src_ref=one_out.at[2 * q + 1 - core],
            dst_ref=pair_buf.at[q],
            send_sem=spair_send.at[q],
            recv_sem=spair_recv.at[q],
            device_id={"row": row, "col": partner},
            device_id_type=MESH,
        )

    other = side - base

    def far(i):
        return other + (other_entry - other + i + inner) % side

    def sone_copy(to):
        return pltpu.make_async_remote_copy(
            src_ref=one_out.at[2 * to + core],
            dst_ref=one_buf.at[place],
            send_sem=sone_send.at[to],
            recv_sem=sone_recv.at[place],
            device_id={"row": row, "col": 2 * to + core},
            device_id_type=MESH,
        )

    def sone_from(source):
        return pltpu.make_async_remote_copy(
            src_ref=one_out.at[2 * source + core],
            dst_ref=one_buf.at[source],
            send_sem=sone_send.at[source],
            recv_sem=sone_recv.at[source],
            device_id={"row": row, "col": 2 * source + core},
            device_id_type=MESH,
        )

    def pre_copy(source):
        return pltpu.make_async_remote_copy(
            src_ref=one_out.at[2 * other_entry + core],
            dst_ref=pre_buf.at[source - base],
            send_sem=pre_send.at[0],
            recv_sem=pre_recv.at[source - base],
            device_id={"row": row, "col": 2 * entry + core},
            device_id_type=MESH,
        )

    wanted = [far(i) for i in range(side)] + [sibling(j) for j in range(1, side)]
    for q in wanted:
        spair_copy(q).start()
    spair_copy(place).start()
    for i, q in enumerate(wanted):
        spair_copy(q).wait_recv()
        one_out[2 * q + core] = (
            one_out[2 * q + core].astype(f32) + pair_buf[q].astype(f32)
        ).astype(bf16)
        if i in (0, side - 1):
            first = 1 if i == 0 else 0

            @pl.when(inner == first)
            def _():
                sone_copy(q).start()

            if i == 0:

                @pl.when(inner == 0)
                def _():
                    pre_copy(place).start()

        else:
            sone_copy(q).start()

    @pl.when(inner == 1)
    def _():
        share = one_out[2 * other_entry + core].astype(f32)
        for j in range(1, side):
            pre_copy(sibling(j)).wait_recv()
            share = share + pre_buf[sibling(j) - base].astype(f32)
        one_out[2 * other_entry + core] = share.astype(bf16)
        sone_copy(other_entry).start()

    loads[3].wait()
    loads[4].wait()

    def finish(share, level, moment):
        following = momentum_decay * moment[...] + share
        moment[...] = following
        level[...] = level[...] - outer_rate * (share + momentum_decay * following)

    share = two_out[row].astype(f32)
    for k in range(1, n_row):
        stwo_copy(k).wait_recv()
        share = share + two_buf[k].astype(f32)
    finish(share / n_row, new_two, next_two)
    spair_copy(place).wait_recv()
    total = ds.at[pl.ds(0, width // n_col), :]
    total[...] = one_out[col].astype(f32) + pair_buf[place].astype(f32)
    for j in range(1, side):
        sone_from(sibling(j)).wait_recv()
        total[...] += one_buf[sibling(j)].astype(f32)

    @pl.when(inner == 1)
    def _():
        sone_from(other_entry).wait_recv()
        total[...] += one_buf[other_entry].astype(f32)

    @pl.when(inner == 0)
    def _():
        for i in range(side):
            sone_from(far(i)).wait_recv()
            total[...] += one_buf[far(i)].astype(f32)

    finish(total[...] / n_col, new_one, next_one)

    def sent(u, carry):
        for copy in pair_of(u):
            copy.wait_send()
        return carry

    lax.fori_loop(1, n, sent, 0)
    own_copy(other_entry).wait_send()
    for j in range(1, side):
        own_copy(sibling(j)).wait_send()

    @pl.when(place == entry)
    def _():
        for i in range(side):
            for j in range(1, side):
                relay(beyond(i), sibling(j)).wait_send()

    for q in range(chips):
        across(2 * q + core).wait_send()
        spair_copy(q).wait_send()
    for k in range(1, n_row):
        two_copy(k).wait_send()
        stwo_copy(k).wait_send()
    for j in range(1, side):
        sone_copy(sibling(j)).wait_send()
    for i in range(1, side - 1):
        sone_copy(far(i)).wait_send()

    @pl.when(inner == 1)
    def _():
        for i in sorted({0, side - 1}):
            sone_copy(far(i)).wait_send()

    @pl.when(inner == 0)
    def _():
        sone_copy(far(side - 1)).wait_send()
        pre_copy(place).wait_send()


def shards(docs, routes, level_one, level_two, moment_one, moment_two):
    n_row = lax.axis_size("row")
    n_col = lax.axis_size("col")
    paths = n_row * n_col
    count, length, width = docs.shape
    cap = max(2, (2 * count + paths - 1) // paths)
    lines = length * cap
    kept = (length - 1) * cap
    per = (kept + 7) // 8 * 8
    rows = paths * per
    chips = n_col // 2
    one_rows, two_rows = width // n_col, width // n_row
    vmem = pl.BlockSpec(memory_space=pltpu.VMEM)
    hbm = pl.BlockSpec(memory_space=pl.ANY)
    dma = pltpu.SemaphoreType.DMA
    full = pltpu.VMEM((rows, width), f32)
    thin = pltpu.VMEM((rows, width), bf16)
    side = pltpu.VMEM((rows, 128), f32)
    scratch = [
        pltpu.VMEM((count, length, width), bf16),
        pltpu.VMEM((paths, lines, width), bf16),
        pltpu.VMEM((paths, 1, 128), f32),
        pltpu.VMEM((paths, lines, width), bf16),
        pltpu.VMEM((paths, 1, 128), f32),
        pltpu.VMEM((n_col, one_rows, width), bf16),
        pltpu.VMEM((n_row, two_rows, width), bf16),
        full, full, full, full, full, thin, thin, thin, thin, thin,
        pltpu.VMEM((rows, rows), bf16),
        pltpu.VMEM((2, width, width), bf16),
        pltpu.VMEM((width, width), f32),
        side, side,
        pltpu.VMEM((n_col, one_rows, width), bf16),
        pltpu.VMEM((n_row, two_rows, width), bf16),
        pltpu.VMEM((chips, one_rows, width), bf16),
        pltpu.VMEM((chips // 2, one_rows, width), bf16),
        pltpu.VMEM((chips, one_rows, width), bf16),
        pltpu.VMEM((n_row, two_rows, width), bf16),
        dma((5,)), dma((paths,)), dma((paths,)), dma((paths,)), dma((paths,)),
        dma((chips,)), dma((chips, chips)), dma((n_col,)), dma((n_col,)), dma((n_col,)),
        dma((n_row,)), dma((n_row,)),
        dma((chips,)), dma((chips,)), dma((1,)), dma((chips // 2,)), dma((chips,)), dma((chips,)),
        dma((n_row,)), dma((n_row,)),
    ]
    held = sum(
        math.prod(piece.shape) * piece.dtype.itemsize
        for piece in scratch
        if piece.memory_space == pltpu.VMEM
    )
    kept_bytes = 8 * (one_rows + two_rows) * width
    limit = min(67043328 - kept_bytes, held + (12 << 20))
    held_one = pltpu.VMEM((one_rows, width), f32)
    held_two = pltpu.VMEM((two_rows, width), f32)
    results = pl.pallas_call(
        functools.partial(round_kernel, n_row, n_col, cap, kept),
        out_shape=(held_one, held_two, held_one, held_two),
        in_specs=[vmem, hbm, hbm, hbm, hbm, hbm],
        out_specs=(vmem,) * 4,
        scratch_shapes=scratch,
        compiler_params=pltpu.CompilerParams(
            collective_id=0, has_side_effects=True, vmem_limit_bytes=limit
        ),
    )(
        routes.reshape(1, count), docs, level_one[0], level_two[0], moment_one[0], moment_two[0]
    )
    return tuple(result[None] for result in results)


def solution(mesh):
    placed = (
        P(("row", "col"), None, None),
        P(("row", "col"), None),
        P("row", "col", None),
        P("col", "row", None),
        P("row", "col", None),
        P("col", "row", None),
    )
    return jax.shard_map(
        shards,
        mesh=mesh,
        in_specs=placed,
        out_specs=(
            P("row", "col", None),
            P("col", "row", None),
            P("row", "col", None),
            P("col", "row", None),
        ),
        check_vma=False,
    )
```

```python
import functools
import math

import jax
import jax.numpy as jnp
from jax import lax
from jax.experimental import pallas as pl
from jax.experimental.pallas import tpu as pltpu
from jax.sharding import PartitionSpec as P

STEPS = 3
BLOCK_COLS = 256

inner_rate = 64.0
outer_rate = 0.7
momentum_decay = 0.9

MESH = pl.DeviceIdType.MESH
f32 = jnp.float32
bf16 = jnp.bfloat16


def product(a, b, i, j):
    return lax.dot_general(a, b, (((i,), (j,)), ((), ())), preferred_element_type=f32)


def column_blocks(width):
    return [(at, min(BLOCK_COLS, width - at)) for at in range(0, width, BLOCK_COLS)]


def fold(values):
    return sum(values[:, at : at + 128] for at in range(0, values.shape[1], 128))


def spread(values, width):
    return jnp.concatenate([values] * (width // 128), axis=1) if width > 128 else values


def round_kernel(
    n_row, n_col, cap, kept,
    route_ref, docs_hbm, one_hbm, two_hbm, moment_one_hbm, moment_two_hbm,
    new_one, new_two, next_one, next_two,
    docs_v, out_ref, cnt_ref, arrived, counts, whole_one, whole_two,
    z, h, g, e, ds, t, xb, hb, eb, db, gram, w2, dw, rx, rr,
    one_out, two_out, pair_buf, pre_buf, one_buf, two_buf,
    load_sem, doc_send, doc_recv, cnt_send, cnt_recv,
    own_send, relay_send, one_recv, pair_send, pair_recv, two_send, two_recv,
    spair_send, spair_recv, pre_send, pre_recv, sone_send, sone_recv, stwo_send, stwo_recv,
):
    row, col = lax.axis_index("row"), lax.axis_index("col")
    n = n_row * n_col
    me = row * n_col + col
    chips = n_col // 2
    place, core = col // 2, col % 2
    partner = place * 2 + 1 - core
    side = chips // 2
    upper = place // side
    base = upper * side
    entry = side - 1 + upper
    inner = (place == entry).astype(jnp.int32)
    outer = 1 - inner
    other_entry = side - upper
    lines, width = arrived.shape[1:]
    rows = z.shape[0]
    per = rows // n
    group = 2 * n_row
    half_group = group // 2
    chunk = half_group * per
    chunks = 2 * chips
    early = rows * (chips - 1) // chips // 256 * 256
    count = docs_v.shape[0]
    length = docs_v.shape[1]
    scale = width ** (-0.5)
    blocks = column_blocks(width)
    barrier = pltpu.get_barrier_semaphore()

    loads = [
        pltpu.make_async_copy(one_hbm, new_one, load_sem.at[0]),
        pltpu.make_async_copy(two_hbm, new_two, load_sem.at[1]),
        pltpu.make_async_copy(docs_hbm, docs_v, load_sem.at[2]),
        pltpu.make_async_copy(moment_one_hbm, next_one, load_sem.at[3]),
        pltpu.make_async_copy(moment_two_hbm, next_two, load_sem.at[4]),
    ]
    for copy in loads:
        copy.start()

    def greet(k, carry):
        to = (me + k) % n
        pl.semaphore_signal(
            barrier, inc=1, device_id={"row": to // n_col, "col": to % n_col}, device_id_type=MESH
        )
        return carry

    lax.fori_loop(1, n, greet, 0)
    loads[0].wait()
    whole_one[col] = new_one[...].astype(bf16)
    loads[1].wait()
    whole_two[row] = new_two[...].astype(bf16)

    pl.semaphore_wait(barrier, n - 1)

    def own_copy(to):
        return pltpu.make_async_remote_copy(
            src_ref=whole_one.at[col],
            dst_ref=whole_one.at[col],
            send_sem=own_send.at[to],
            recv_sem=one_recv.at[col],
            device_id={"row": row, "col": 2 * to + core},
            device_id_type=MESH,
        )

    def relay(source, to):
        block = 2 * source + core
        return pltpu.make_async_remote_copy(
            src_ref=whole_one.at[block],
            dst_ref=whole_one.at[block],
            send_sem=relay_send.at[source, to],
            recv_sem=one_recv.at[block],
            device_id={"row": row, "col": 2 * to + core},
            device_id_type=MESH,
        )

    def sibling(j):
        return base + (place - base + j) % side

    def beyond(i):
        return (1 - upper) * (side + i) + upper * (side - 1 - i)

    def across(block):
        return pltpu.make_async_remote_copy(
            src_ref=whole_one.at[block],
            dst_ref=whole_one.at[block],
            send_sem=pair_send.at[block],
            recv_sem=pair_recv.at[block],
            device_id={"row": row, "col": partner},
            device_id_type=MESH,
        )

    def two_copy(k):
        return pltpu.make_async_remote_copy(
            src_ref=whole_two.at[row],
            dst_ref=whole_two.at[row],
            send_sem=two_send.at[k],
            recv_sem=two_recv.at[k],
            device_id={"row": (row + k) % n_row, "col": col},
            device_id_type=MESH,
        )

    def two_wait(k):
        from_row = (row - k + n_row) % n_row
        return pltpu.make_async_remote_copy(
            src_ref=whole_two.at[row],
            dst_ref=whole_two.at[from_row],
            send_sem=two_send.at[k],
            recv_sem=two_recv.at[k],
            device_id={"row": (row + k) % n_row, "col": col},
            device_id_type=MESH,
        )

    own_copy(other_entry).start()
    for j in range(1, side):
        own_copy(sibling(j)).start()
    across(col).start()
    for k in range(1, n_row):
        two_copy(k).start()

    target = route_ref[...]
    named = jnp.broadcast_to(target.astype(f32), (count, count))
    earlier = lax.broadcasted_iota(jnp.int32, (count, count), 0) < lax.broadcasted_iota(
        jnp.int32, (count, count), 1
    )
    rank = jnp.sum(jnp.where((named.T == named) & earlier, 1.0, 0.0), axis=0, keepdims=True)
    slot = target * cap + rank.astype(jnp.int32)
    slots = lax.broadcasted_iota(jnp.int32, (n * cap, count), 0)
    dispatch = jnp.where(slots == slot, 1.0, 0.0).astype(bf16)
    path = lax.broadcasted_iota(jnp.int32, (n, 1, count), 0)
    mine = jnp.where(jnp.broadcast_to(target[None], (n, 1, count)) == path, 1.0, 0.0)
    cnt_ref[...] = jnp.broadcast_to(jnp.sum(mine, axis=-1, keepdims=True), cnt_ref.shape)

    loads[2].wait()
    docs = jnp.swapaxes(docs_v[...], 0, 1)
    for step in range(length):
        sent = jnp.dot(dispatch, docs[step], preferred_element_type=f32)
        out_ref[:, step * cap : (step + 1) * cap, :] = sent.reshape(n, cap, width).astype(bf16)

    def pair_of(u):
        to_row = (row + u % n_row) % n_row
        to_col = (place + u // group) % chips * 2 + (core + u // n_row) % 2
        to = to_row * n_col + to_col
        peer = {"row": to_row, "col": to_col}
        return (
            pltpu.make_async_remote_copy(
                src_ref=out_ref.at[to],
                dst_ref=arrived.at[u],
                send_sem=doc_send.at[u],
                recv_sem=doc_recv.at[u],
                device_id=peer,
                device_id_type=MESH,
            ),
            pltpu.make_async_remote_copy(
                src_ref=cnt_ref.at[to],
                dst_ref=counts.at[u],
                send_sem=cnt_send.at[u],
                recv_sem=cnt_recv.at[u],
                device_id=peer,
                device_id_type=MESH,
            ),
        )

    def apart(k, other_order):
        near = k + inner * (other_order - k)
        return (near + upper * (chips - 2 * near)) % chips

    def last_first(k):
        return (k + chips - 3) % (chips - 1) + 1

    def backwards(k):
        return (2 * chips - 1 - k) % (chips - 1) + 1

    def send_docs(first, last):
        def body(u, carry):
            for copy in pair_of(u):
                copy.start()
            return carry

        lax.fori_loop(first, last, body, 0)

    arrived[0] = out_ref[me]
    counts[0] = cnt_ref[me]
    send_docs(1, group)

    at = apart(1, last_first(1)) * group
    send_docs(at, at + group)

    @pl.when(place == entry)
    def _():
        for i in range(side):
            source = beyond(i)
            relay(source, place).wait_recv()
            across(2 * source + core).start()
            for j in range(1, side):
                relay(source, sibling(j)).start()

    for k in range(2, chips):
        at = apart(k, last_first(k)) * group
        send_docs(at, at + group)
    for j in range(1, side):
        relay(sibling(j), place).wait_recv()
        across(2 * sibling(j) + core).start()

    @pl.when(place != entry)
    def _():
        for i in range(side):
            relay(beyond(i), place).wait_recv()
            across(2 * beyond(i) + core).start()

    for q in range(chips):
        across(2 * q + 1 - core).wait_recv()
    for k in range(1, n_row):
        two_wait(k).wait_recv()

    def place_of(k):
        q = k // 2
        near = (inner * backwards(q) + outer * last_first(q)) * ((q + chips - 1) // chips)
        far_off = (near + upper * (chips - 2 * near)) % chips
        return far_off * group + k % 2 * half_group

    def arrive(first, last):
        def body(u, carry):
            for copy in pair_of(u):
                copy.wait_recv()
            return carry

        lax.fori_loop(first, last, body, 0)

    def unpack(k, at):
        block = arrived[pl.ds(place_of(k), half_group)].astype(f32)
        if per == kept:
            first, last = block[:, :kept], block[:, lines - kept :]
        else:
            live = lax.broadcasted_iota(jnp.int32, block.shape, 1) < kept
            first = jnp.where(live, block, 0.0)[:, :per]
            last = jnp.where(live, pltpu.roll(block, kept, 1), 0.0)[:, :per]
        first = first.reshape(chunk, width)
        xb[at, :] = first.astype(bf16)
        t[at, :] = last.reshape(chunk, width).astype(bf16)
        size = jnp.sum(fold(first * first), axis=-1, keepdims=True) * (1.0 / width)
        rx[at, :] = jnp.broadcast_to(lax.rsqrt(size + 1e-06), (chunk, 128))

    def hidden(at, start):
        size = jnp.zeros((at.size, 128), f32)
        for n0, nn in blocks:
            cols = pl.ds(n0, nn)
            zz = start(cols, nn)
            z[at, cols] = zz
            gate = 1.0 / (1.0 + jnp.exp(-zz))
            act = zz * gate
            hh = xb[at, cols].astype(f32) + act
            h[at, cols] = hh
            hb[at, cols] = hh.astype(bf16)
            g[at, cols] = gate + act * (1.0 - gate)
            size = size + fold(hh * hh)
        size = jnp.sum(size, axis=-1, keepdims=True) * (1.0 / width)
        rr[at, :] = jnp.broadcast_to(lax.rsqrt(size + 1e-06), (at.size, 128))

    def errors(at, weights):
        r = rr[at, :]
        both = jnp.zeros((at.size, 128), f32)
        for n0, nn in blocks:
            cols = pl.ds(n0, nn)
            pp = product(hb[at, :], weights(cols), 1, 0)
            rw = spread(r, nn)
            ee = h[at, cols] + scale * rw * pp - t[at, cols].astype(f32)
            er = ee * rw
            e[at, cols] = ee
            eb[at, cols] = er.astype(bf16)
            both = both + fold(er * pp)
        both = jnp.sum(both, axis=-1, keepdims=True) * (1.0 / width)
        rr[at, :] = jnp.broadcast_to(both, (at.size, 128)) * r * r

    def slopes(at, weights, turn):
        m, rw = rr[at, :], rx[at, :]
        for n0, nn in blocks:
            cols = pl.ds(n0, nn)
            qq = product(eb[at, :], weights(cols), 1, 1)
            dd = (e[at, cols] + scale * (qq - h[at, cols] * spread(m, nn))) * g[at, cols]
            dd = dd * spread(rw, nn)
            if turn is None:
                ds[at, cols] = dd
                db[at, cols] = dd.astype(bf16)
            else:
                total = ds[at, cols] + dd
                ds[at, cols] = total
                db[at, cols] = jnp.where(turn == STEPS - 1, total, dd).astype(bf16)


    def two_cols(cols):
        return whole_two[:, :, cols].reshape(width, cols.size)

    def two_rows(cols):
        return whole_two[...].reshape(width, width)[cols.start : cols.start + cols.size]

    arrive(1, half_group)
    low, high = pl.ds(0, early), pl.ds(early, rows - early)

    def first_turn(k, carry):
        at = pl.ds(pl.multiple_of(k * chunk, chunk), chunk)
        unpack(k, at)

        def start(cols, nn):
            zz = product(xb[at, :], whole_one[:, :, cols].reshape(width, nn), 1, 0)
            return scale * spread(rx[at, :], nn) * zz

        hidden(at, start)
        errors(at, two_cols)
        slopes(at, two_rows, None)

        @pl.when(k == chunks - 3)
        def _():
            gram[low, low] = product(xb[low, :], xb[low, :], 1, 1).astype(bf16)
            for n0, nn in blocks:
                cols = pl.ds(n0, nn)
                dw[:, cols] = product(hb[low, :], eb[low, cols], 0, 0)

        @pl.when(k < chunks - 1)
        def _():
            first = place_of(k + 1)
            arrive(first, first + half_group)

        return carry

    lax.fori_loop(0, chunks, first_turn, 0)
    gram[high, :] = product(xb[high, :], xb[...], 1, 1).astype(bf16)
    gram[low, high] = product(xb[low, :], xb[high, :], 1, 1).astype(bf16)

    filled = jnp.sum(counts[...].reshape(n, 128), axis=0, keepdims=True)[:, :1]
    rate = inner_rate * scale / (filled * (length - 1))

    for n0, nn in blocks:
        cols = pl.ds(n0, nn)
        change = dw[:, cols] + product(hb[high, :], eb[high, cols], 0, 0)
        dw[:, cols] = change
        w2[1, :, cols] = (two_cols(cols).astype(f32) - rate * change).astype(bf16)

    everything = pl.ds(0, rows)

    def stwo_copy(k):
        to = (row + k) % n_row
        return pltpu.make_async_remote_copy(
            src_ref=two_out.at[to],
            dst_ref=two_buf.at[k],
            send_sem=stwo_send.at[k],
            recv_sem=stwo_recv.at[k],
            device_id={"row": to, "col": col},
            device_id_type=MESH,
        )

    def later_turn(turn, carry):
        now, later = turn % 2, (turn + 1) % 2

        def start(cols, nn):
            step = product(gram[...], db[:, cols], 1, 0)
            return z[:, cols] - (rate * scale) * spread(rx[...], nn) * step

        hidden(everything, start)
        errors(everything, lambda cols: w2[now, :, cols])
        for n0, nn in blocks:
            cols = pl.ds(n0, nn)
            change = dw[:, cols] + product(hb[...], eb[:, cols], 0, 0)
            dw[:, cols] = change
            change = rate * change
            w2[later, :, cols] = (two_cols(cols).astype(f32) - change).astype(bf16)
            two_out[:, :, cols] = change.astype(bf16).reshape(n_row, width // n_row, nn)

        @pl.when(turn == STEPS - 1)
        def _():
            for k in range(1, n_row):
                stwo_copy(k).start()

        slopes(everything, lambda cols: w2[now, cols, :], turn)
        return carry

    lax.fori_loop(1, STEPS, later_turn, 0)

    for n0, nn in blocks:
        cols = pl.ds(n0, nn)
        change = rate * product(xb[...], db[:, cols], 0, 0)
        one_out[:, :, cols] = change.astype(bf16).reshape(n_col, width // n_col, nn)

    def spair_copy(q):
        return pltpu.make_async_remote_copy(
            src_ref=one_out.at[2 * q + 1 - core],
            dst_ref=pair_buf.at[q],
            send_sem=spair_send.at[q],
            recv_sem=spair_recv.at[q],
            device_id={"row": row, "col": partner},
            device_id_type=MESH,
        )

    other = side - base

    def far(i):
        return other + (other_entry - other + i + inner) % side

    def sone_copy(to):
        return pltpu.make_async_remote_copy(
            src_ref=one_out.at[2 * to + core],
            dst_ref=one_buf.at[place],
            send_sem=sone_send.at[to],
            recv_sem=sone_recv.at[place],
            device_id={"row": row, "col": 2 * to + core},
            device_id_type=MESH,
        )

    def sone_from(source):
        return pltpu.make_async_remote_copy(
            src_ref=one_out.at[2 * source + core],
            dst_ref=one_buf.at[source],
            send_sem=sone_send.at[source],
            recv_sem=sone_recv.at[source],
            device_id={"row": row, "col": 2 * source + core},
            device_id_type=MESH,
        )

    def pre_copy(source):
        return pltpu.make_async_remote_copy(
            src_ref=one_out.at[2 * other_entry + core],
            dst_ref=pre_buf.at[source - base],
            send_sem=pre_send.at[0],
            recv_sem=pre_recv.at[source - base],
            device_id={"row": row, "col": 2 * entry + core},
            device_id_type=MESH,
        )

    wanted = [far(i) for i in range(side)] + [sibling(j) for j in range(1, side)]
    for q in wanted:
        spair_copy(q).start()
    spair_copy(place).start()
    for i, q in enumerate(wanted):
        spair_copy(q).wait_recv()
        one_out[2 * q + core] = (
            one_out[2 * q + core].astype(f32) + pair_buf[q].astype(f32)
        ).astype(bf16)
        if i in (0, side - 1):
            first = 1 if i == 0 else 0

            @pl.when(inner == first)
            def _():
                sone_copy(q).start()

            if i == 0:

                @pl.when(inner == 0)
                def _():
                    pre_copy(place).start()

        else:
            sone_copy(q).start()

    @pl.when(inner == 1)
    def _():
        share = one_out[2 * other_entry + core].astype(f32)
        for j in range(1, side):
            pre_copy(sibling(j)).wait_recv()
            share = share + pre_buf[sibling(j) - base].astype(f32)
        one_out[2 * other_entry + core] = share.astype(bf16)
        sone_copy(other_entry).start()

    loads[3].wait()
    loads[4].wait()

    def finish(share, level, moment):
        following = momentum_decay * moment[...] + share
        moment[...] = following
        level[...] = level[...] - outer_rate * (share + momentum_decay * following)

    share = two_out[row].astype(f32)
    for k in range(1, n_row):
        stwo_copy(k).wait_recv()
        share = share + two_buf[k].astype(f32)
    finish(share / n_row, new_two, next_two)
    spair_copy(place).wait_recv()
    total = ds.at[pl.ds(0, width // n_col), :]
    total[...] = one_out[col].astype(f32) + pair_buf[place].astype(f32)
    for j in range(1, side):
        sone_from(sibling(j)).wait_recv()
        total[...] += one_buf[sibling(j)].astype(f32)

    @pl.when(inner == 1)
    def _():
        sone_from(other_entry).wait_recv()
        total[...] += one_buf[other_entry].astype(f32)

    @pl.when(inner == 0)
    def _():
        for i in range(side):
            sone_from(far(i)).wait_recv()
            total[...] += one_buf[far(i)].astype(f32)

    finish(total[...] / n_col, new_one, next_one)

    def sent(u, carry):
        for copy in pair_of(u):
            copy.wait_send()
        return carry

    lax.fori_loop(1, n, sent, 0)
    own_copy(other_entry).wait_send()
    for j in range(1, side):
        own_copy(sibling(j)).wait_send()

    @pl.when(place == entry)
    def _():
        for i in range(side):
            for j in range(1, side):
                relay(beyond(i), sibling(j)).wait_send()

    for q in range(chips):
        across(2 * q + core).wait_send()
        spair_copy(q).wait_send()
    for k in range(1, n_row):
        two_copy(k).wait_send()
        stwo_copy(k).wait_send()
    for j in range(1, side):
        sone_copy(sibling(j)).wait_send()
    for i in range(1, side - 1):
        sone_copy(far(i)).wait_send()

    @pl.when(inner == 1)
    def _():
        for i in sorted({0, side - 1}):
            sone_copy(far(i)).wait_send()

    @pl.when(inner == 0)
    def _():
        sone_copy(far(side - 1)).wait_send()
        pre_copy(place).wait_send()


def shards(docs, routes, level_one, level_two, moment_one, moment_two):
    n_row = lax.axis_size("row")
    n_col = lax.axis_size("col")
    paths = n_row * n_col
    count, length, width = docs.shape
    cap = max(2, (2 * count + paths - 1) // paths)
    lines = length * cap
    kept = (length - 1) * cap
    per = (kept + 7) // 8 * 8
    rows = paths * per
    chips = n_col // 2
    one_rows, two_rows = width // n_col, width // n_row
    vmem = pl.BlockSpec(memory_space=pltpu.VMEM)
    hbm = pl.BlockSpec(memory_space=pl.ANY)
    dma = pltpu.SemaphoreType.DMA
    full = pltpu.VMEM((rows, width), f32)
    thin = pltpu.VMEM((rows, width), bf16)
    side = pltpu.VMEM((rows, 128), f32)
    scratch = [
        pltpu.VMEM((count, length, width), bf16),
        pltpu.VMEM((paths, lines, width), bf16),
        pltpu.VMEM((paths, 1, 128), f32),
        pltpu.VMEM((paths, lines, width), bf16),
        pltpu.VMEM((paths, 1, 128), f32),
        pltpu.VMEM((n_col, one_rows, width), bf16),
        pltpu.VMEM((n_row, two_rows, width), bf16),
        full, full, full, full, full, thin, thin, thin, thin, thin,
        pltpu.VMEM((rows, rows), bf16),
        pltpu.VMEM((2, width, width), bf16),
        pltpu.VMEM((width, width), f32),
        side, side,
        pltpu.VMEM((n_col, one_rows, width), bf16),
        pltpu.VMEM((n_row, two_rows, width), bf16),
        pltpu.VMEM((chips, one_rows, width), bf16),
        pltpu.VMEM((chips // 2, one_rows, width), bf16),
        pltpu.VMEM((chips, one_rows, width), bf16),
        pltpu.VMEM((n_row, two_rows, width), bf16),
        dma((5,)), dma((paths,)), dma((paths,)), dma((paths,)), dma((paths,)),
        dma((chips,)), dma((chips, chips)), dma((n_col,)), dma((n_col,)), dma((n_col,)),
        dma((n_row,)), dma((n_row,)),
        dma((chips,)), dma((chips,)), dma((1,)), dma((chips // 2,)), dma((chips,)), dma((chips,)),
        dma((n_row,)), dma((n_row,)),
    ]
    held = sum(
        math.prod(piece.shape) * piece.dtype.itemsize
        for piece in scratch
        if piece.memory_space == pltpu.VMEM
    )
    kept_bytes = 8 * (one_rows + two_rows) * width
    limit = min(67043328 - kept_bytes, held + (12 << 20))
    held_one = pltpu.VMEM((one_rows, width), f32)
    held_two = pltpu.VMEM((two_rows, width), f32)
    results = pl.pallas_call(
        functools.partial(round_kernel, n_row, n_col, cap, kept),
        out_shape=(held_one, held_two, held_one, held_two),
        in_specs=[vmem, hbm, hbm, hbm, hbm, hbm],
        out_specs=(vmem,) * 4,
        scratch_shapes=scratch,
        compiler_params=pltpu.CompilerParams(
            collective_id=0, has_side_effects=True, vmem_limit_bytes=limit
        ),
    )(
        routes.reshape(1, count), docs, level_one[0], level_two[0], moment_one[0], moment_two[0]
    )
    return tuple(result[None] for result in results)


def solution(mesh):
    placed = (
        P(("row", "col"), None, None),
        P(("row", "col"), None),
        P("row", "col", None),
        P("col", "row", None),
        P("row", "col", None),
        P("col", "row", None),
    )
    return jax.shard_map(
        shards,
        mesh=mesh,
        in_specs=placed,
        out_specs=(
            P("row", "col", None),
            P("col", "row", None),
            P("row", "col", None),
            P("col", "row", None),
        ),
        check_vma=False,
    )
```

```python
import functools
import math

import jax
import jax.numpy as jnp
from jax import lax
from jax.experimental import pallas as pl
from jax.experimental.pallas import tpu as pltpu
from jax.sharding import PartitionSpec as P

STEPS = 3
BLOCK_COLS = 256

inner_rate = 64.0
outer_rate = 0.7
momentum_decay = 0.9

MESH = pl.DeviceIdType.MESH
f32 = jnp.float32
bf16 = jnp.bfloat16


def product(a, b, i, j):
    return lax.dot_general(a, b, (((i,), (j,)), ((), ())), preferred_element_type=f32)


def column_blocks(width):
    return [(at, min(BLOCK_COLS, width - at)) for at in range(0, width, BLOCK_COLS)]


def fold(values):
    return sum(values[:, at : at + 128] for at in range(0, values.shape[1], 128))


def spread(values, width):
    return jnp.concatenate([values] * (width // 128), axis=1) if width > 128 else values


def round_kernel(
    n_row, n_col, cap, kept,
    route_ref, docs_hbm, one_hbm, two_hbm, moment_one_hbm, moment_two_hbm,
    new_one, new_two, next_one, next_two,
    docs_v, out_ref, cnt_ref, arrived, counts, whole_one, whole_two,
    z, h, g, e, ds, t, xb, hb, eb, db, gram, w2, dw, rx, rr,
    one_out, two_out, pair_buf, pre_buf, one_buf, two_buf,
    load_sem, doc_send, doc_recv, cnt_send, cnt_recv,
    own_send, relay_send, one_recv, pair_send, pair_recv, two_send, two_recv,
    spair_send, spair_recv, pre_send, pre_recv, sone_send, sone_recv, stwo_send, stwo_recv,
):
    row, col = lax.axis_index("row"), lax.axis_index("col")
    n = n_row * n_col
    me = row * n_col + col
    chips = n_col // 2
    place, core = col // 2, col % 2
    partner = place * 2 + 1 - core
    side = chips // 2
    upper = place // side
    base = upper * side
    entry = side - 1 + upper
    inner = (place == entry).astype(jnp.int32)
    outer = 1 - inner
    other_entry = side - upper
    lines, width = arrived.shape[1:]
    rows = z.shape[0]
    per = rows // n
    group = 2 * n_row
    half_group = group // 2
    chunk = half_group * per
    chunks = 2 * chips
    early = rows * (chips - 1) // chips // 256 * 256
    count = docs_v.shape[0]
    length = docs_v.shape[1]
    scale = width ** (-0.5)
    blocks = column_blocks(width)
    barrier = pltpu.get_barrier_semaphore()

    loads = [
        pltpu.make_async_copy(one_hbm, new_one, load_sem.at[0]),
        pltpu.make_async_copy(two_hbm, new_two, load_sem.at[1]),
        pltpu.make_async_copy(docs_hbm, docs_v, load_sem.at[2]),
        pltpu.make_async_copy(moment_one_hbm, next_one, load_sem.at[3]),
        pltpu.make_async_copy(moment_two_hbm, next_two, load_sem.at[4]),
    ]
    for copy in loads:
        copy.start()

    def greet(k, carry):
        to = (me + k) % n
        pl.semaphore_signal(
            barrier, inc=1, device_id={"row": to // n_col, "col": to % n_col}, device_id_type=MESH
        )
        return carry

    lax.fori_loop(1, n, greet, 0)
    loads[0].wait()
    whole_one[col] = new_one[...].astype(bf16)
    loads[1].wait()
    whole_two[row] = new_two[...].astype(bf16)

    pl.semaphore_wait(barrier, n - 1)

    def own_copy(to):
        return pltpu.make_async_remote_copy(
            src_ref=whole_one.at[col],
            dst_ref=whole_one.at[col],
            send_sem=own_send.at[to],
            recv_sem=one_recv.at[col],
            device_id={"row": row, "col": 2 * to + core},
            device_id_type=MESH,
        )

    def relay(source, to):
        block = 2 * source + core
        return pltpu.make_async_remote_copy(
            src_ref=whole_one.at[block],
            dst_ref=whole_one.at[block],
            send_sem=relay_send.at[source, to],
            recv_sem=one_recv.at[block],
            device_id={"row": row, "col": 2 * to + core},
            device_id_type=MESH,
        )

    def sibling(j):
        return base + (place - base + j) % side

    def beyond(i):
        return (1 - upper) * (side + i) + upper * (side - 1 - i)

    def across(block):
        return pltpu.make_async_remote_copy(
            src_ref=whole_one.at[block],
            dst_ref=whole_one.at[block],
            send_sem=pair_send.at[block],
            recv_sem=pair_recv.at[block],
            device_id={"row": row, "col": partner},
            device_id_type=MESH,
        )

    def two_copy(k):
        return pltpu.make_async_remote_copy(
            src_ref=whole_two.at[row],
            dst_ref=whole_two.at[row],
            send_sem=two_send.at[k],
            recv_sem=two_recv.at[k],
            device_id={"row": (row + k) % n_row, "col": col},
            device_id_type=MESH,
        )

    def two_wait(k):
        from_row = (row - k + n_row) % n_row
        return pltpu.make_async_remote_copy(
            src_ref=whole_two.at[row],
            dst_ref=whole_two.at[from_row],
            send_sem=two_send.at[k],
            recv_sem=two_recv.at[k],
            device_id={"row": (row + k) % n_row, "col": col},
            device_id_type=MESH,
        )

    own_copy(other_entry).start()
    for j in range(1, side):
        own_copy(sibling(j)).start()
    across(col).start()
    for k in range(1, n_row):
        two_copy(k).start()

    target = route_ref[...]
    named = jnp.broadcast_to(target.astype(f32), (count, count))
    earlier = lax.broadcasted_iota(jnp.int32, (count, count), 0) < lax.broadcasted_iota(
        jnp.int32, (count, count), 1
    )
    rank = jnp.sum(jnp.where((named.T == named) & earlier, 1.0, 0.0), axis=0, keepdims=True)
    slot = target * cap + rank.astype(jnp.int32)
    slots = lax.broadcasted_iota(jnp.int32, (n * cap, count), 0)
    dispatch = jnp.where(slots == slot, 1.0, 0.0).astype(bf16)
    path = lax.broadcasted_iota(jnp.int32, (n, 1, count), 0)
    mine = jnp.where(jnp.broadcast_to(target[None], (n, 1, count)) == path, 1.0, 0.0)
    cnt_ref[...] = jnp.broadcast_to(jnp.sum(mine, axis=-1, keepdims=True), cnt_ref.shape)

    loads[2].wait()
    docs = jnp.swapaxes(docs_v[...], 0, 1)
    for step in range(length):
        sent = jnp.dot(dispatch, docs[step], preferred_element_type=f32)
        out_ref[:, step * cap : (step + 1) * cap, :] = sent.reshape(n, cap, width).astype(bf16)

    def pair_of(u):
        to_row = (row + u % n_row) % n_row
        to_col = (place + u // group) % chips * 2 + (core + u // n_row) % 2
        to = to_row * n_col + to_col
        peer = {"row": to_row, "col": to_col}
        return (
            pltpu.make_async_remote_copy(
                src_ref=out_ref.at[to],
                dst_ref=arrived.at[u],
                send_sem=doc_send.at[u],
                recv_sem=doc_recv.at[u],
                device_id=peer,
                device_id_type=MESH,
            ),
            pltpu.make_async_remote_copy(
                src_ref=cnt_ref.at[to],
                dst_ref=counts.at[u],
                send_sem=cnt_send.at[u],
                recv_sem=cnt_recv.at[u],
                device_id=peer,
                device_id_type=MESH,
            ),
        )

    def apart(k):
        near = outer * (k * 2 % chips + k // side) + inner * last_first(k)
        return (near + upper * (chips - 2 * near)) % chips

    def last_first(k):
        return (k + chips - 3) % (chips - 1) + 1

    def send_docs(first, last):
        def body(u, carry):
            for copy in pair_of(u):
                copy.start()
            return carry

        lax.fori_loop(first, last, body, 0)

    arrived[0] = out_ref[me]
    counts[0] = cnt_ref[me]
    send_docs(1, group)

    at = apart(1) * group
    send_docs(at, at + group)

    @pl.when(place == entry)
    def _():
        for i in range(side):
            source = beyond(i)
            relay(source, place).wait_recv()
            across(2 * source + core).start()
            for j in range(1, side):
                relay(source, sibling(j)).start()

    for k in range(2, chips):
        at = apart(k) * group
        send_docs(at, at + group)
    for j in range(1, side):
        relay(sibling(j), place).wait_recv()
        across(2 * sibling(j) + core).start()

    @pl.when(place != entry)
    def _():
        for i in range(side):
            relay(beyond(i), place).wait_recv()
            across(2 * beyond(i) + core).start()

    for q in range(chips):
        across(2 * q + 1 - core).wait_recv()
    for k in range(1, n_row):
        two_wait(k).wait_recv()

    def place_of(k):
        q = k // 2
        near = last_first(q) * ((q + chips - 1) // chips)
        far_off = (near + upper * (chips - 2 * near)) % chips
        return far_off * group + k % 2 * half_group

    def arrive(first, last):
        def body(u, carry):
            for copy in pair_of(u):
                copy.wait_recv()
            return carry

        lax.fori_loop(first, last, body, 0)

    def unpack(k, at):
        block = arrived[pl.ds(place_of(k), half_group)].astype(f32)
        if per == kept:
            first, last = block[:, :kept], block[:, lines - kept :]
        else:
            live = lax.broadcasted_iota(jnp.int32, block.shape, 1) < kept
            first = jnp.where(live, block, 0.0)[:, :per]
            last = jnp.where(live, pltpu.roll(block, kept, 1), 0.0)[:, :per]
        first = first.reshape(chunk, width)
        xb[at, :] = first.astype(bf16)
        t[at, :] = last.reshape(chunk, width).astype(bf16)
        size = jnp.sum(fold(first * first), axis=-1, keepdims=True) * (1.0 / width)
        rx[at, :] = jnp.broadcast_to(lax.rsqrt(size + 1e-06), (chunk, 128))

    def hidden(at, start):
        size = jnp.zeros((at.size, 128), f32)
        for n0, nn in blocks:
            cols = pl.ds(n0, nn)
            zz = start(cols, nn)
            z[at, cols] = zz
            gate = 1.0 / (1.0 + jnp.exp(-zz))
            act = zz * gate
            hh = xb[at, cols].astype(f32) + act
            h[at, cols] = hh
            hb[at, cols] = hh.astype(bf16)
            g[at, cols] = gate + act * (1.0 - gate)
            size = size + fold(hh * hh)
        size = jnp.sum(size, axis=-1, keepdims=True) * (1.0 / width)
        rr[at, :] = jnp.broadcast_to(lax.rsqrt(size + 1e-06), (at.size, 128))

    def errors(at, weights):
        r = rr[at, :]
        both = jnp.zeros((at.size, 128), f32)
        for n0, nn in blocks:
            cols = pl.ds(n0, nn)
            pp = product(hb[at, :], weights(cols), 1, 0)
            rw = spread(r, nn)
            ee = h[at, cols] + scale * rw * pp - t[at, cols].astype(f32)
            er = ee * rw
            e[at, cols] = ee
            eb[at, cols] = er.astype(bf16)
            both = both + fold(er * pp)
        both = jnp.sum(both, axis=-1, keepdims=True) * (1.0 / width)
        rr[at, :] = jnp.broadcast_to(both, (at.size, 128)) * r * r

    def slopes(at, weights, turn):
        m, rw = rr[at, :], rx[at, :]
        for n0, nn in blocks:
            cols = pl.ds(n0, nn)
            qq = product(eb[at, :], weights(cols), 1, 1)
            dd = (e[at, cols] + scale * (qq - h[at, cols] * spread(m, nn))) * g[at, cols]
            dd = dd * spread(rw, nn)
            if turn is None:
                ds[at, cols] = dd
                db[at, cols] = dd.astype(bf16)
            else:
                total = ds[at, cols] + dd
                ds[at, cols] = total
                db[at, cols] = jnp.where(turn == STEPS - 1, total, dd).astype(bf16)


    def two_cols(cols):
        return whole_two[:, :, cols].reshape(width, cols.size)

    def two_rows(cols):
        return whole_two[...].reshape(width, width)[cols.start : cols.start + cols.size]

    arrive(1, half_group)
    low, high = pl.ds(0, early), pl.ds(early, rows - early)

    def first_turn(k, carry):
        at = pl.ds(pl.multiple_of(k * chunk, chunk), chunk)
        unpack(k, at)

        def start(cols, nn):
            zz = product(xb[at, :], whole_one[:, :, cols].reshape(width, nn), 1, 0)
            return scale * spread(rx[at, :], nn) * zz

        hidden(at, start)
        errors(at, two_cols)
        slopes(at, two_rows, None)

        @pl.when(k == chunks - 3)
        def _():
            gram[low, low] = product(xb[low, :], xb[low, :], 1, 1).astype(bf16)
            for n0, nn in blocks:
                cols = pl.ds(n0, nn)
                dw[:, cols] = product(hb[low, :], eb[low, cols], 0, 0)

        @pl.when(k < chunks - 1)
        def _():
            first = place_of(k + 1)
            arrive(first, first + half_group)

        return carry

    lax.fori_loop(0, chunks, first_turn, 0)
    gram[high, :] = product(xb[high, :], xb[...], 1, 1).astype(bf16)
    gram[low, high] = product(xb[low, :], xb[high, :], 1, 1).astype(bf16)

    filled = jnp.sum(counts[...].reshape(n, 128), axis=0, keepdims=True)[:, :1]
    rate = inner_rate * scale / (filled * (length - 1))

    for n0, nn in blocks:
        cols = pl.ds(n0, nn)
        change = dw[:, cols] + product(hb[high, :], eb[high, cols], 0, 0)
        dw[:, cols] = change
        w2[1, :, cols] = (two_cols(cols).astype(f32) - rate * change).astype(bf16)

    everything = pl.ds(0, rows)

    def stwo_copy(k):
        to = (row + k) % n_row
        return pltpu.make_async_remote_copy(
            src_ref=two_out.at[to],
            dst_ref=two_buf.at[k],
            send_sem=stwo_send.at[k],
            recv_sem=stwo_recv.at[k],
            device_id={"row": to, "col": col},
            device_id_type=MESH,
        )

    def later_turn(turn, carry):
        now, later = turn % 2, (turn + 1) % 2

        def start(cols, nn):
            step = product(gram[...], db[:, cols], 1, 0)
            return z[:, cols] - (rate * scale) * spread(rx[...], nn) * step

        hidden(everything, start)
        errors(everything, lambda cols: w2[now, :, cols])
        for n0, nn in blocks:
            cols = pl.ds(n0, nn)
            change = dw[:, cols] + product(hb[...], eb[:, cols], 0, 0)
            dw[:, cols] = change
            change = rate * change
            w2[later, :, cols] = (two_cols(cols).astype(f32) - change).astype(bf16)
            two_out[:, :, cols] = change.astype(bf16).reshape(n_row, width // n_row, nn)

        @pl.when(turn == STEPS - 1)
        def _():
            for k in range(1, n_row):
                stwo_copy(k).start()

        slopes(everything, lambda cols: w2[now, cols, :], turn)
        return carry

    lax.fori_loop(1, STEPS, later_turn, 0)

    for n0, nn in blocks:
        cols = pl.ds(n0, nn)
        change = rate * product(xb[...], db[:, cols], 0, 0)
        one_out[:, :, cols] = change.astype(bf16).reshape(n_col, width // n_col, nn)

    def spair_copy(q):
        return pltpu.make_async_remote_copy(
            src_ref=one_out.at[2 * q + 1 - core],
            dst_ref=pair_buf.at[q],
            send_sem=spair_send.at[q],
            recv_sem=spair_recv.at[q],
            device_id={"row": row, "col": partner},
            device_id_type=MESH,
        )

    other = side - base

    def far(i):
        return other + (other_entry - other + i + inner) % side

    def sone_copy(to):
        return pltpu.make_async_remote_copy(
            src_ref=one_out.at[2 * to + core],
            dst_ref=one_buf.at[place],
            send_sem=sone_send.at[to],
            recv_sem=sone_recv.at[place],
            device_id={"row": row, "col": 2 * to + core},
            device_id_type=MESH,
        )

    def sone_from(source):
        return pltpu.make_async_remote_copy(
            src_ref=one_out.at[2 * source + core],
            dst_ref=one_buf.at[source],
            send_sem=sone_send.at[source],
            recv_sem=sone_recv.at[source],
            device_id={"row": row, "col": 2 * source + core},
            device_id_type=MESH,
        )

    def pre_copy(source):
        return pltpu.make_async_remote_copy(
            src_ref=one_out.at[2 * other_entry + core],
            dst_ref=pre_buf.at[source - base],
            send_sem=pre_send.at[0],
            recv_sem=pre_recv.at[source - base],
            device_id={"row": row, "col": 2 * entry + core},
            device_id_type=MESH,
        )

    wanted = [far(i) for i in range(side)] + [sibling(j) for j in range(1, side)]
    for q in wanted:
        spair_copy(q).start()
    spair_copy(place).start()
    for i, q in enumerate(wanted):
        spair_copy(q).wait_recv()
        one_out[2 * q + core] = (
            one_out[2 * q + core].astype(f32) + pair_buf[q].astype(f32)
        ).astype(bf16)
        if i in (0, side - 1):
            first = 1 if i == 0 else 0

            @pl.when(inner == first)
            def _():
                sone_copy(q).start()

            if i == 0:

                @pl.when(inner == 0)
                def _():
                    pre_copy(place).start()

        else:
            sone_copy(q).start()

    @pl.when(inner == 1)
    def _():
        share = one_out[2 * other_entry + core].astype(f32)
        for j in range(1, side):
            pre_copy(sibling(j)).wait_recv()
            share = share + pre_buf[sibling(j) - base].astype(f32)
        one_out[2 * other_entry + core] = share.astype(bf16)
        sone_copy(other_entry).start()

    loads[3].wait()
    loads[4].wait()

    def finish(share, level, moment):
        following = momentum_decay * moment[...] + share
        moment[...] = following
        level[...] = level[...] - outer_rate * (share + momentum_decay * following)

    share = two_out[row].astype(f32)
    for k in range(1, n_row):
        stwo_copy(k).wait_recv()
        share = share + two_buf[k].astype(f32)
    finish(share / n_row, new_two, next_two)
    spair_copy(place).wait_recv()
    total = ds.at[pl.ds(0, width // n_col), :]
    total[...] = one_out[col].astype(f32) + pair_buf[place].astype(f32)
    for j in range(1, side):
        sone_from(sibling(j)).wait_recv()
        total[...] += one_buf[sibling(j)].astype(f32)

    @pl.when(inner == 1)
    def _():
        sone_from(other_entry).wait_recv()
        total[...] += one_buf[other_entry].astype(f32)

    @pl.when(inner == 0)
    def _():
        for i in range(side):
            sone_from(far(i)).wait_recv()
            total[...] += one_buf[far(i)].astype(f32)

    finish(total[...] / n_col, new_one, next_one)

    def sent(u, carry):
        for copy in pair_of(u):
            copy.wait_send()
        return carry

    lax.fori_loop(1, n, sent, 0)
    own_copy(other_entry).wait_send()
    for j in range(1, side):
        own_copy(sibling(j)).wait_send()

    @pl.when(place == entry)
    def _():
        for i in range(side):
            for j in range(1, side):
                relay(beyond(i), sibling(j)).wait_send()

    for q in range(chips):
        across(2 * q + core).wait_send()
        spair_copy(q).wait_send()
    for k in range(1, n_row):
        two_copy(k).wait_send()
        stwo_copy(k).wait_send()
    for j in range(1, side):
        sone_copy(sibling(j)).wait_send()
    for i in range(1, side - 1):
        sone_copy(far(i)).wait_send()

    @pl.when(inner == 1)
    def _():
        for i in sorted({0, side - 1}):
            sone_copy(far(i)).wait_send()

    @pl.when(inner == 0)
    def _():
        sone_copy(far(side - 1)).wait_send()
        pre_copy(place).wait_send()


def store_kernel(*refs):
    copies = [pltpu.make_async_copy(refs[i], refs[4 + i], refs[8].at[i]) for i in range(4)]
    for copy in copies:
        copy.start()
    for copy in copies:
        copy.wait()


def shards(docs, routes, level_one, level_two, moment_one, moment_two):
    n_row = lax.axis_size("row")
    n_col = lax.axis_size("col")
    paths = n_row * n_col
    count, length, width = docs.shape
    cap = max(2, (2 * count + paths - 1) // paths)
    lines = length * cap
    kept = (length - 1) * cap
    per = (kept + 7) // 8 * 8
    rows = paths * per
    chips = n_col // 2
    one_rows, two_rows = width // n_col, width // n_row
    vmem = pl.BlockSpec(memory_space=pltpu.VMEM)
    hbm = pl.BlockSpec(memory_space=pl.ANY)
    dma = pltpu.SemaphoreType.DMA
    full = pltpu.VMEM((rows, width), f32)
    thin = pltpu.VMEM((rows, width), bf16)
    side = pltpu.VMEM((rows, 128), f32)
    scratch = [
        pltpu.VMEM((count, length, width), bf16),
        pltpu.VMEM((paths, lines, width), bf16),
        pltpu.VMEM((paths, 1, 128), f32),
        pltpu.VMEM((paths, lines, width), bf16),
        pltpu.VMEM((paths, 1, 128), f32),
        pltpu.VMEM((n_col, one_rows, width), bf16),
        pltpu.VMEM((n_row, two_rows, width), bf16),
        full, full, full, full, full, thin, thin, thin, thin, thin,
        pltpu.VMEM((rows, rows), bf16),
        pltpu.VMEM((2, width, width), bf16),
        pltpu.VMEM((width, width), f32),
        side, side,
        pltpu.VMEM((n_col, one_rows, width), bf16),
        pltpu.VMEM((n_row, two_rows, width), bf16),
        pltpu.VMEM((chips, one_rows, width), bf16),
        pltpu.VMEM((chips // 2, one_rows, width), bf16),
        pltpu.VMEM((chips, one_rows, width), bf16),
        pltpu.VMEM((n_row, two_rows, width), bf16),
        dma((5,)), dma((paths,)), dma((paths,)), dma((paths,)), dma((paths,)),
        dma((chips,)), dma((chips, chips)), dma((n_col,)), dma((n_col,)), dma((n_col,)),
        dma((n_row,)), dma((n_row,)),
        dma((chips,)), dma((chips,)), dma((1,)), dma((chips // 2,)), dma((chips,)), dma((chips,)),
        dma((n_row,)), dma((n_row,)),
    ]
    held = sum(
        math.prod(piece.shape) * piece.dtype.itemsize
        for piece in scratch
        if piece.memory_space == pltpu.VMEM
    )
    kept_bytes = 8 * (one_rows + two_rows) * width
    limit = min(67043328 - kept_bytes, held + (12 << 20))
    held_one = pltpu.VMEM((one_rows, width), f32)
    held_two = pltpu.VMEM((two_rows, width), f32)
    results = pl.pallas_call(
        functools.partial(round_kernel, n_row, n_col, cap, kept),
        out_shape=(held_one, held_two, held_one, held_two),
        in_specs=[vmem, hbm, hbm, hbm, hbm, hbm],
        out_specs=(vmem,) * 4,
        scratch_shapes=scratch,
        compiler_params=pltpu.CompilerParams(
            collective_id=0, has_side_effects=True, vmem_limit_bytes=limit
        ),
    )(
        routes.reshape(1, count), docs, level_one[0], level_two[0], moment_one[0], moment_two[0]
    )
    results = pl.pallas_call(
        store_kernel,
        out_shape=tuple(jax.ShapeDtypeStruct(result.shape, f32) for result in results),
        in_specs=[hbm] * 4,
        out_specs=(pl.BlockSpec(memory_space=pltpu.HBM),) * 4,
        scratch_shapes=[dma((4,))],
    )(*(pltpu.with_memory_space_constraint(result, pltpu.VMEM) for result in results))
    return tuple(result[None] for result in results)


def solution(mesh):
    placed = (
        P(("row", "col"), None, None),
        P(("row", "col"), None),
        P("row", "col", None),
        P("col", "row", None),
        P("row", "col", None),
        P("col", "row", None),
    )
    return jax.shard_map(
        shards,
        mesh=mesh,
        in_specs=placed,
        out_specs=(
            P("row", "col", None),
            P("col", "row", None),
            P("row", "col", None),
            P("col", "row", None),
        ),
        check_vma=False,
    )
```

```python
import functools
import math

import jax
import jax.numpy as jnp
from jax import lax
from jax.experimental import pallas as pl
from jax.experimental.pallas import tpu as pltpu
from jax.sharding import PartitionSpec as P

STEPS = 3
BLOCK_COLS = 256

inner_rate = 64.0
outer_rate = 0.7
momentum_decay = 0.9

MESH = pl.DeviceIdType.MESH
f32 = jnp.float32
bf16 = jnp.bfloat16


def product(a, b, i, j):
    return lax.dot_general(a, b, (((i,), (j,)), ((), ())), preferred_element_type=f32)


def column_blocks(width):
    return [(at, min(BLOCK_COLS, width - at)) for at in range(0, width, BLOCK_COLS)]


def fold(values):
    return sum(values[:, at : at + 128] for at in range(0, values.shape[1], 128))


def spread(values, width):
    return jnp.concatenate([values] * (width // 128), axis=1) if width > 128 else values


def round_kernel(
    n_row, n_col, cap, kept,
    route_ref, docs_hbm, one_hbm, two_hbm, moment_one_hbm, moment_two_hbm,
    new_one, new_two, next_one, next_two,
    docs_v, out_ref, cnt_ref, arrived, counts, whole_one, whole_two,
    z, h, g, e, ds, t, xb, hb, eb, db, gram, w2, dw, rx, rr,
    one_out, two_out, pair_buf, pre_buf, one_buf, two_buf,
    load_sem, doc_send, doc_recv, cnt_send, cnt_recv,
    own_send, relay_send, one_recv, pair_send, pair_recv, two_send, two_recv,
    spair_send, spair_recv, pre_send, pre_recv, sone_send, sone_recv, stwo_send, stwo_recv,
):
    row, col = lax.axis_index("row"), lax.axis_index("col")
    n = n_row * n_col
    me = row * n_col + col
    chips = n_col // 2
    place, core = col // 2, col % 2
    partner = place * 2 + 1 - core
    side = chips // 2
    upper = place // side
    base = upper * side
    entry = side - 1 + upper
    inner = (place == entry).astype(jnp.int32)
    outer = 1 - inner
    other_entry = side - upper
    lines, width = arrived.shape[1:]
    rows = z.shape[0]
    per = rows // n
    group = 2 * n_row
    chunk = group * per
    early = rows * (chips - 1) // chips // 256 * 256
    count = docs_v.shape[0]
    length = docs_v.shape[1]
    scale = width ** (-0.5)
    blocks = column_blocks(width)
    barrier = pltpu.get_barrier_semaphore()

    loads = [
        pltpu.make_async_copy(one_hbm, new_one, load_sem.at[0]),
        pltpu.make_async_copy(two_hbm, new_two, load_sem.at[1]),
        pltpu.make_async_copy(docs_hbm, docs_v, load_sem.at[2]),
        pltpu.make_async_copy(moment_one_hbm, next_one, load_sem.at[3]),
        pltpu.make_async_copy(moment_two_hbm, next_two, load_sem.at[4]),
    ]
    for copy in loads:
        copy.start()

    def greet(k, carry):
        to = (me + k) % n
        pl.semaphore_signal(
            barrier, inc=1, device_id={"row": to // n_col, "col": to % n_col}, device_id_type=MESH
        )
        return carry

    lax.fori_loop(1, n, greet, 0)
    loads[0].wait()
    whole_one[col] = new_one[...].astype(bf16)
    loads[1].wait()
    whole_two[row] = new_two[...].astype(bf16)

    pl.semaphore_wait(barrier, n - 1)

    def own_copy(to):
        return pltpu.make_async_remote_copy(
            src_ref=whole_one.at[col],
            dst_ref=whole_one.at[col],
            send_sem=own_send.at[to],
            recv_sem=one_recv.at[col],
            device_id={"row": row, "col": 2 * to + core},
            device_id_type=MESH,
        )

    def relay(source, to):
        block = 2 * source + core
        return pltpu.make_async_remote_copy(
            src_ref=whole_one.at[block],
            dst_ref=whole_one.at[block],
            send_sem=relay_send.at[source, to],
            recv_sem=one_recv.at[block],
            device_id={"row": row, "col": 2 * to + core},
            device_id_type=MESH,
        )

    def sibling(j):
        return base + (place - base + j) % side

    def beyond(i):
        return (1 - upper) * (side + i) + upper * (side - 1 - i)

    def across(block):
        return pltpu.make_async_remote_copy(
            src_ref=whole_one.at[block],
            dst_ref=whole_one.at[block],
            send_sem=pair_send.at[block],
            recv_sem=pair_recv.at[block],
            device_id={"row": row, "col": partner},
            device_id_type=MESH,
        )

    def two_copy(k):
        return pltpu.make_async_remote_copy(
            src_ref=whole_two.at[row],
            dst_ref=whole_two.at[row],
            send_sem=two_send.at[k],
            recv_sem=two_recv.at[k],
            device_id={"row": (row + k) % n_row, "col": col},
            device_id_type=MESH,
        )

    def two_wait(k):
        from_row = (row - k + n_row) % n_row
        return pltpu.make_async_remote_copy(
            src_ref=whole_two.at[row],
            dst_ref=whole_two.at[from_row],
            send_sem=two_send.at[k],
            recv_sem=two_recv.at[k],
            device_id={"row": (row + k) % n_row, "col": col},
            device_id_type=MESH,
        )

    own_copy(other_entry).start()
    for j in range(1, side):
        own_copy(sibling(j)).start()
    across(col).start()
    for k in range(1, n_row):
        two_copy(k).start()

    target = route_ref[...]
    named = jnp.broadcast_to(target.astype(f32), (count, count))
    earlier = lax.broadcasted_iota(jnp.int32, (count, count), 0) < lax.broadcasted_iota(
        jnp.int32, (count, count), 1
    )
    rank = jnp.sum(jnp.where((named.T == named) & earlier, 1.0, 0.0), axis=0, keepdims=True)
    slot = target * cap + rank.astype(jnp.int32)
    slots = lax.broadcasted_iota(jnp.int32, (n * cap, count), 0)
    dispatch = jnp.where(slots == slot, 1.0, 0.0).astype(bf16)
    path = lax.broadcasted_iota(jnp.int32, (n, 1, count), 0)
    mine = jnp.where(jnp.broadcast_to(target[None], (n, 1, count)) == path, 1.0, 0.0)
    cnt_ref[...] = jnp.broadcast_to(jnp.sum(mine, axis=-1, keepdims=True), cnt_ref.shape)

    loads[2].wait()
    docs = jnp.swapaxes(docs_v[...], 0, 1)
    for step in range(length):
        sent = jnp.dot(dispatch, docs[step], preferred_element_type=f32)
        out_ref[:, step * cap : (step + 1) * cap, :] = sent.reshape(n, cap, width).astype(bf16)

    def pair_of(u):
        to_row = (row + u % n_row) % n_row
        to_col = (place + u // group) % chips * 2 + (core + u // n_row) % 2
        to = to_row * n_col + to_col
        peer = {"row": to_row, "col": to_col}
        return (
            pltpu.make_async_remote_copy(
                src_ref=out_ref.at[to],
                dst_ref=arrived.at[u],
                send_sem=doc_send.at[u],
                recv_sem=doc_recv.at[u],
                device_id=peer,
                device_id_type=MESH,
            ),
            pltpu.make_async_remote_copy(
                src_ref=cnt_ref.at[to],
                dst_ref=counts.at[u],
                send_sem=cnt_send.at[u],
                recv_sem=cnt_recv.at[u],
                device_id=peer,
                device_id_type=MESH,
            ),
        )

    def apart(k):
        near = outer * (k * 2 % chips + k // side) + inner * last_first(k)
        return (near + upper * (chips - 2 * near)) % chips

    def last_first(k):
        return (k + chips - 3) % (chips - 1) + 1

    def send_docs(first, last):
        def body(u, carry):
            for copy in pair_of(u):
                copy.start()
            return carry

        lax.fori_loop(first, last, body, 0)

    arrived[0] = out_ref[me]
    counts[0] = cnt_ref[me]
    send_docs(1, group)

    at = apart(1) * group
    send_docs(at, at + group)

    @pl.when(place == entry)
    def _():
        for i in range(side):
            source = beyond(i)
            relay(source, place).wait_recv()
            across(2 * source + core).start()
            for j in range(1, side):
                relay(source, sibling(j)).start()

    for k in range(2, chips):
        at = apart(k) * group
        send_docs(at, at + group)
    for j in range(1, side):
        relay(sibling(j), place).wait_recv()
        across(2 * sibling(j) + core).start()

    @pl.when(place != entry)
    def _():
        for i in range(side):
            relay(beyond(i), place).wait_recv()
            across(2 * beyond(i) + core).start()

    for q in range(chips):
        across(2 * q + 1 - core).wait_recv()
    for k in range(1, n_row):
        two_wait(k).wait_recv()

    def place_of(k):
        near = last_first(k) * ((k + chips - 1) // chips)
        return (near + upper * (chips - 2 * near)) % chips * group

    def arrive(first, last):
        def body(u, carry):
            for copy in pair_of(u):
                copy.wait_recv()
            return carry

        lax.fori_loop(first, last, body, 0)

    def unpack(k, at):
        block = arrived[pl.ds(place_of(k), group)].astype(f32)
        if per == kept:
            first, last = block[:, :kept], block[:, lines - kept :]
        else:
            live = lax.broadcasted_iota(jnp.int32, block.shape, 1) < kept
            first = jnp.where(live, block, 0.0)[:, :per]
            last = jnp.where(live, pltpu.roll(block, kept, 1), 0.0)[:, :per]
        first = first.reshape(chunk, width)
        xb[at, :] = first.astype(bf16)
        t[at, :] = last.reshape(chunk, width).astype(bf16)
        size = jnp.sum(fold(first * first), axis=-1, keepdims=True) * (1.0 / width)
        rx[at, :] = jnp.broadcast_to(lax.rsqrt(size + 1e-06), (chunk, 128))

    def hidden(at, start):
        size = jnp.zeros((at.size, 128), f32)
        for n0, nn in blocks:
            cols = pl.ds(n0, nn)
            zz = start(cols, nn)
            z[at, cols] = zz
            gate = 1.0 / (1.0 + jnp.exp(-zz))
            act = zz * gate
            hh = xb[at, cols].astype(f32) + act
            h[at, cols] = hh
            hb[at, cols] = hh.astype(bf16)
            g[at, cols] = gate + act * (1.0 - gate)
            size = size + fold(hh * hh)
        size = jnp.sum(size, axis=-1, keepdims=True) * (1.0 / width)
        rr[at, :] = jnp.broadcast_to(lax.rsqrt(size + 1e-06), (at.size, 128))

    def errors(at, weights):
        r = rr[at, :]
        both = jnp.zeros((at.size, 128), f32)
        for n0, nn in blocks:
            cols = pl.ds(n0, nn)
            pp = product(hb[at, :], weights(cols), 1, 0)
            rw = spread(r, nn)
            ee = h[at, cols] + scale * rw * pp - t[at, cols].astype(f32)
            er = ee * rw
            e[at, cols] = ee
            eb[at, cols] = er.astype(bf16)
            both = both + fold(er * pp)
        both = jnp.sum(both, axis=-1, keepdims=True) * (1.0 / width)
        rr[at, :] = jnp.broadcast_to(both, (at.size, 128)) * r * r

    def slopes(at, weights, turn):
        m, rw = rr[at, :], rx[at, :]
        for n0, nn in blocks:
            cols = pl.ds(n0, nn)
            qq = product(eb[at, :], weights(cols), 1, 1)
            dd = (e[at, cols] + scale * (qq - h[at, cols] * spread(m, nn))) * g[at, cols]
            dd = dd * spread(rw, nn)
            if turn is None:
                ds[at, cols] = dd
                db[at, cols] = dd.astype(bf16)
            else:
                total = ds[at, cols] + dd
                ds[at, cols] = total
                db[at, cols] = jnp.where(turn == STEPS - 1, total, dd).astype(bf16)


    def two_cols(cols):
        return whole_two[:, :, cols].reshape(width, cols.size)

    def two_rows(cols):
        return whole_two[...].reshape(width, width)[cols.start : cols.start + cols.size]

    arrive(1, group)
    low, high = pl.ds(0, early), pl.ds(early, rows - early)

    def first_turn(k, carry):
        at = pl.ds(pl.multiple_of(k * chunk, chunk), chunk)
        unpack(k, at)

        def start(cols, nn):
            zz = product(xb[at, :], whole_one[:, :, cols].reshape(width, nn), 1, 0)
            return scale * spread(rx[at, :], nn) * zz

        hidden(at, start)
        errors(at, two_cols)
        slopes(at, two_rows, None)

        @pl.when(k == chips - 2)
        def _():
            gram[low, low] = product(xb[low, :], xb[low, :], 1, 1).astype(bf16)
            for n0, nn in blocks:
                cols = pl.ds(n0, nn)
                dw[:, cols] = product(hb[low, :], eb[low, cols], 0, 0)

        @pl.when(k < chips - 1)
        def _():
            first = place_of(k + 1)
            arrive(first, first + group)

        return carry

    lax.fori_loop(0, chips, first_turn, 0)
    gram[high, :] = product(xb[high, :], xb[...], 1, 1).astype(bf16)
    gram[low, high] = product(xb[low, :], xb[high, :], 1, 1).astype(bf16)

    filled = jnp.sum(counts[...].reshape(n, 128), axis=0, keepdims=True)[:, :1]
    rate = inner_rate * scale / (filled * (length - 1))

    for n0, nn in blocks:
        cols = pl.ds(n0, nn)
        change = dw[:, cols] + product(hb[high, :], eb[high, cols], 0, 0)
        dw[:, cols] = change
        w2[1, :, cols] = (two_cols(cols).astype(f32) - rate * change).astype(bf16)

    everything = pl.ds(0, rows)

    def stwo_copy(k):
        to = (row + k) % n_row
        return pltpu.make_async_remote_copy(
            src_ref=two_out.at[to],
            dst_ref=two_buf.at[k],
            send_sem=stwo_send.at[k],
            recv_sem=stwo_recv.at[k],
            device_id={"row": to, "col": col},
            device_id_type=MESH,
        )

    def later_turn(turn, carry):
        now, later = turn % 2, (turn + 1) % 2

        def start(cols, nn):
            step = product(gram[...], db[:, cols], 1, 0)
            return z[:, cols] - (rate * scale) * spread(rx[...], nn) * step

        hidden(everything, start)
        errors(everything, lambda cols: w2[now, :, cols])
        for n0, nn in blocks:
            cols = pl.ds(n0, nn)
            change = dw[:, cols] + product(hb[...], eb[:, cols], 0, 0)
            dw[:, cols] = change
            change = rate * change
            w2[later, :, cols] = (two_cols(cols).astype(f32) - change).astype(bf16)
            two_out[:, :, cols] = change.astype(bf16).reshape(n_row, width // n_row, nn)

        @pl.when(turn == STEPS - 1)
        def _():
            for k in range(1, n_row):
                stwo_copy(k).start()

        slopes(everything, lambda cols: w2[now, cols, :], turn)
        return carry

    lax.fori_loop(1, STEPS, later_turn, 0)

    for n0, nn in blocks:
        cols = pl.ds(n0, nn)
        change = rate * product(xb[...], db[:, cols], 0, 0)
        one_out[:, :, cols] = change.astype(bf16).reshape(n_col, width // n_col, nn)

    def spair_copy(q):
        return pltpu.make_async_remote_copy(
            src_ref=one_out.at[2 * q + 1 - core],
            dst_ref=pair_buf.at[q],
            send_sem=spair_send.at[q],
            recv_sem=spair_recv.at[q],
            device_id={"row": row, "col": partner},
            device_id_type=MESH,
        )

    other = side - base

    def far(i):
        return other + (other_entry - other + i + inner) % side

    def sone_copy(to):
        return pltpu.make_async_remote_copy(
            src_ref=one_out.at[2 * to + core],
            dst_ref=one_buf.at[place],
            send_sem=sone_send.at[to],
            recv_sem=sone_recv.at[place],
            device_id={"row": row, "col": 2 * to + core},
            device_id_type=MESH,
        )

    def sone_from(source):
        return pltpu.make_async_remote_copy(
            src_ref=one_out.at[2 * source + core],
            dst_ref=one_buf.at[source],
            send_sem=sone_send.at[source],
            recv_sem=sone_recv.at[source],
            device_id={"row": row, "col": 2 * source + core},
            device_id_type=MESH,
        )

    def pre_copy(source):
        return pltpu.make_async_remote_copy(
            src_ref=one_out.at[2 * other_entry + core],
            dst_ref=pre_buf.at[source - base],
            send_sem=pre_send.at[0],
            recv_sem=pre_recv.at[source - base],
            device_id={"row": row, "col": 2 * entry + core},
            device_id_type=MESH,
        )

    wanted = [far(i) for i in range(side)] + [sibling(j) for j in range(1, side)]
    for q in wanted:
        spair_copy(q).start()
    spair_copy(place).start()
    for i, q in enumerate(wanted):
        spair_copy(q).wait_recv()
        one_out[2 * q + core] = (
            one_out[2 * q + core].astype(f32) + pair_buf[q].astype(f32)
        ).astype(bf16)
        if i in (0, side - 1):
            first = 1 if i == 0 else 0

            @pl.when(inner == first)
            def _():
                sone_copy(q).start()

            if i == 0:

                @pl.when(inner == 0)
                def _():
                    pre_copy(place).start()

        else:
            sone_copy(q).start()

    @pl.when(inner == 1)
    def _():
        share = one_out[2 * other_entry + core].astype(f32)
        for j in range(1, side):
            pre_copy(sibling(j)).wait_recv()
            share = share + pre_buf[sibling(j) - base].astype(f32)
        one_out[2 * other_entry + core] = share.astype(bf16)
        sone_copy(other_entry).start()

    loads[3].wait()
    loads[4].wait()

    def finish(share, level, moment):
        following = momentum_decay * moment[...] + share
        moment[...] = following
        level[...] = level[...] - outer_rate * (share + momentum_decay * following)

    share = two_out[row].astype(f32)
    for k in range(1, n_row):
        stwo_copy(k).wait_recv()
        share = share + two_buf[k].astype(f32)
    finish(share / n_row, new_two, next_two)
    spair_copy(place).wait_recv()
    total = ds.at[pl.ds(0, width // n_col), :]
    total[...] = one_out[col].astype(f32) + pair_buf[place].astype(f32)
    for j in range(1, side):
        sone_from(sibling(j)).wait_recv()
        total[...] += one_buf[sibling(j)].astype(f32)

    @pl.when(inner == 1)
    def _():
        sone_from(other_entry).wait_recv()
        total[...] += one_buf[other_entry].astype(f32)

    @pl.when(inner == 0)
    def _():
        for i in range(side):
            sone_from(far(i)).wait_recv()
            total[...] += one_buf[far(i)].astype(f32)

    finish(total[...] / n_col, new_one, next_one)

    def sent(u, carry):
        for copy in pair_of(u):
            copy.wait_send()
        return carry

    lax.fori_loop(1, n, sent, 0)
    own_copy(other_entry).wait_send()
    for j in range(1, side):
        own_copy(sibling(j)).wait_send()

    @pl.when(place == entry)
    def _():
        for i in range(side):
            for j in range(1, side):
                relay(beyond(i), sibling(j)).wait_send()

    for q in range(chips):
        across(2 * q + core).wait_send()
        spair_copy(q).wait_send()
    for k in range(1, n_row):
        two_copy(k).wait_send()
        stwo_copy(k).wait_send()
    for j in range(1, side):
        sone_copy(sibling(j)).wait_send()
    for i in range(1, side - 1):
        sone_copy(far(i)).wait_send()

    @pl.when(inner == 1)
    def _():
        for i in sorted({0, side - 1}):
            sone_copy(far(i)).wait_send()

    @pl.when(inner == 0)
    def _():
        sone_copy(far(side - 1)).wait_send()
        pre_copy(place).wait_send()


def store_kernel(*refs):
    copies = [pltpu.make_async_copy(refs[i], refs[4 + i], refs[8].at[i]) for i in range(4)]
    for copy in copies:
        copy.start()
    for copy in copies:
        copy.wait()


def shards(docs, routes, level_one, level_two, moment_one, moment_two):
    n_row = lax.axis_size("row")
    n_col = lax.axis_size("col")
    paths = n_row * n_col
    count, length, width = docs.shape
    cap = max(2, (2 * count + paths - 1) // paths)
    lines = length * cap
    kept = (length - 1) * cap
    per = (kept + 7) // 8 * 8
    rows = paths * per
    chips = n_col // 2
    one_rows, two_rows = width // n_col, width // n_row
    vmem = pl.BlockSpec(memory_space=pltpu.VMEM)
    hbm = pl.BlockSpec(memory_space=pl.ANY)
    dma = pltpu.SemaphoreType.DMA
    full = pltpu.VMEM((rows, width), f32)
    thin = pltpu.VMEM((rows, width), bf16)
    side = pltpu.VMEM((rows, 128), f32)
    scratch = [
        pltpu.VMEM((count, length, width), bf16),
        pltpu.VMEM((paths, lines, width), bf16),
        pltpu.VMEM((paths, 1, 128), f32),
        pltpu.VMEM((paths, lines, width), bf16),
        pltpu.VMEM((paths, 1, 128), f32),
        pltpu.VMEM((n_col, one_rows, width), bf16),
        pltpu.VMEM((n_row, two_rows, width), bf16),
        full, full, full, full, full, thin, thin, thin, thin, thin,
        pltpu.VMEM((rows, rows), bf16),
        pltpu.VMEM((2, width, width), bf16),
        pltpu.VMEM((width, width), f32),
        side, side,
        pltpu.VMEM((n_col, one_rows, width), bf16),
        pltpu.VMEM((n_row, two_rows, width), bf16),
        pltpu.VMEM((chips, one_rows, width), bf16),
        pltpu.VMEM((chips // 2, one_rows, width), bf16),
        pltpu.VMEM((chips, one_rows, width), bf16),
        pltpu.VMEM((n_row, two_rows, width), bf16),
        dma((5,)), dma((paths,)), dma((paths,)), dma((paths,)), dma((paths,)),
        dma((chips,)), dma((chips, chips)), dma((n_col,)), dma((n_col,)), dma((n_col,)),
        dma((n_row,)), dma((n_row,)),
        dma((chips,)), dma((chips,)), dma((1,)), dma((chips // 2,)), dma((chips,)), dma((chips,)),
        dma((n_row,)), dma((n_row,)),
    ]
    held = sum(
        math.prod(piece.shape) * piece.dtype.itemsize
        for piece in scratch
        if piece.memory_space == pltpu.VMEM
    )
    kept_bytes = 8 * (one_rows + two_rows) * width
    limit = min(67043328 - kept_bytes, held + (12 << 20))
    held_one = pltpu.VMEM((one_rows, width), f32)
    held_two = pltpu.VMEM((two_rows, width), f32)
    results = pl.pallas_call(
        functools.partial(round_kernel, n_row, n_col, cap, kept),
        out_shape=(held_one, held_two, held_one, held_two),
        in_specs=[vmem, hbm, hbm, hbm, hbm, hbm],
        out_specs=(vmem,) * 4,
        scratch_shapes=scratch,
        compiler_params=pltpu.CompilerParams(
            collective_id=0, has_side_effects=True, vmem_limit_bytes=limit
        ),
    )(
        routes.reshape(1, count), docs, level_one[0], level_two[0], moment_one[0], moment_two[0]
    )
    results = pl.pallas_call(
        store_kernel,
        out_shape=tuple(jax.ShapeDtypeStruct(result.shape, f32) for result in results),
        in_specs=[hbm] * 4,
        out_specs=(pl.BlockSpec(memory_space=pltpu.HBM),) * 4,
        scratch_shapes=[dma((4,))],
    )(*(pltpu.with_memory_space_constraint(result, pltpu.VMEM) for result in results))
    return tuple(result[None] for result in results)


def solution(mesh):
    placed = (
        P(("row", "col"), None, None),
        P(("row", "col"), None),
        P("row", "col", None),
        P("col", "row", None),
        P("row", "col", None),
        P("col", "row", None),
    )
    return jax.shard_map(
        shards,
        mesh=mesh,
        in_specs=placed,
        out_specs=(
            P("row", "col", None),
            P("col", "row", None),
            P("row", "col", None),
            P("col", "row", None),
        ),
        check_vma=False,
    )
```

```python
import functools
import math

import jax
import jax.numpy as jnp
from jax import lax
from jax.experimental import pallas as pl
from jax.experimental.pallas import tpu as pltpu
from jax.sharding import PartitionSpec as P

STEPS = 3
BLOCK_COLS = 256

inner_rate = 64.0
outer_rate = 0.7
momentum_decay = 0.9

MESH = pl.DeviceIdType.MESH
f32 = jnp.float32
bf16 = jnp.bfloat16


def product(a, b, i, j):
    return lax.dot_general(a, b, (((i,), (j,)), ((), ())), preferred_element_type=f32)


def column_blocks(width):
    return [(at, min(BLOCK_COLS, width - at)) for at in range(0, width, BLOCK_COLS)]


def fold(values):
    return sum(values[:, at : at + 128] for at in range(0, values.shape[1], 128))


def spread(values, width):
    return jnp.concatenate([values] * (width // 128), axis=1) if width > 128 else values


def round_kernel(
    n_row, n_col, cap, kept,
    route_ref, docs_hbm, one_hbm, two_hbm, moment_one_hbm, moment_two_hbm,
    new_one, new_two, next_one, next_two,
    docs_v, out_ref, cnt_ref, arrived, counts, whole_one, whole_two,
    z, h, g, e, ds, t, xb, hb, eb, db, gram, w2, dw, rx, rr,
    one_out, two_out, pair_buf, pre_buf, one_buf, two_buf,
    load_sem, doc_send, doc_recv, cnt_send, cnt_recv,
    own_send, relay_send, one_recv, pair_send, pair_recv, two_send, two_recv,
    spair_send, spair_recv, pre_send, pre_recv, sone_send, sone_recv, stwo_send, stwo_recv,
):
    row, col = lax.axis_index("row"), lax.axis_index("col")
    n = n_row * n_col
    me = row * n_col + col
    chips = n_col // 2
    place, core = col // 2, col % 2
    partner = place * 2 + 1 - core
    side = chips // 2
    upper = place // side
    base = upper * side
    entry = side - 1 + upper
    inner = (place == entry).astype(jnp.int32)
    outer = 1 - inner
    other_entry = side - upper
    lines, width = arrived.shape[1:]
    rows = z.shape[0]
    per = rows // n
    group = 2 * n_row
    half_group = group // 2
    chunk = half_group * per
    chunks = 2 * chips
    early = rows * (chips - 1) // chips // 256 * 256
    count = docs_v.shape[0]
    length = docs_v.shape[1]
    scale = width ** (-0.5)
    blocks = column_blocks(width)
    barrier = pltpu.get_barrier_semaphore()

    loads = [
        pltpu.make_async_copy(one_hbm, new_one, load_sem.at[0]),
        pltpu.make_async_copy(two_hbm, new_two, load_sem.at[1]),
        pltpu.make_async_copy(docs_hbm, docs_v, load_sem.at[2]),
        pltpu.make_async_copy(moment_one_hbm, next_one, load_sem.at[3]),
        pltpu.make_async_copy(moment_two_hbm, next_two, load_sem.at[4]),
    ]
    for copy in loads:
        copy.start()

    def greet(k, carry):
        to = (me + k) % n
        pl.semaphore_signal(
            barrier, inc=1, device_id={"row": to // n_col, "col": to % n_col}, device_id_type=MESH
        )
        return carry

    lax.fori_loop(1, n, greet, 0)
    loads[0].wait()
    whole_one[col] = new_one[...].astype(bf16)

    pl.semaphore_wait(barrier, n - 1)

    def own_copy(to):
        return pltpu.make_async_remote_copy(
            src_ref=whole_one.at[col],
            dst_ref=whole_one.at[col],
            send_sem=own_send.at[to],
            recv_sem=one_recv.at[col],
            device_id={"row": row, "col": 2 * to + core},
            device_id_type=MESH,
        )

    def relay(source, to):
        block = 2 * source + core
        return pltpu.make_async_remote_copy(
            src_ref=whole_one.at[block],
            dst_ref=whole_one.at[block],
            send_sem=relay_send.at[source, to],
            recv_sem=one_recv.at[block],
            device_id={"row": row, "col": 2 * to + core},
            device_id_type=MESH,
        )

    def sibling(j):
        return base + (place - base + j) % side

    def beyond(i):
        return (1 - upper) * (side + i) + upper * (side - 1 - i)

    def across(block):
        return pltpu.make_async_remote_copy(
            src_ref=whole_one.at[block],
            dst_ref=whole_one.at[block],
            send_sem=pair_send.at[block],
            recv_sem=pair_recv.at[block],
            device_id={"row": row, "col": partner},
            device_id_type=MESH,
        )

    def two_copy(k):
        return pltpu.make_async_remote_copy(
            src_ref=whole_two.at[row],
            dst_ref=whole_two.at[row],
            send_sem=two_send.at[k],
            recv_sem=two_recv.at[k],
            device_id={"row": (row + k) % n_row, "col": col},
            device_id_type=MESH,
        )

    def two_wait(k):
        from_row = (row - k + n_row) % n_row
        return pltpu.make_async_remote_copy(
            src_ref=whole_two.at[row],
            dst_ref=whole_two.at[from_row],
            send_sem=two_send.at[k],
            recv_sem=two_recv.at[k],
            device_id={"row": (row + k) % n_row, "col": col},
            device_id_type=MESH,
        )

    own_copy(other_entry).start()
    for j in range(1, side):
        own_copy(sibling(j)).start()
    across(col).start()
    loads[1].wait()
    whole_two[row] = new_two[...].astype(bf16)
    for k in range(1, n_row):
        two_copy(k).start()

    target = route_ref[...]
    named = jnp.broadcast_to(target.astype(f32), (count, count))
    earlier = lax.broadcasted_iota(jnp.int32, (count, count), 0) < lax.broadcasted_iota(
        jnp.int32, (count, count), 1
    )
    rank = jnp.sum(jnp.where((named.T == named) & earlier, 1.0, 0.0), axis=0, keepdims=True)
    slot = target * cap + rank.astype(jnp.int32)
    slots = lax.broadcasted_iota(jnp.int32, (n * cap, count), 0)
    dispatch = jnp.where(slots == slot, 1.0, 0.0).astype(bf16)
    path = lax.broadcasted_iota(jnp.int32, (n, 1, count), 0)
    mine = jnp.where(jnp.broadcast_to(target[None], (n, 1, count)) == path, 1.0, 0.0)
    cnt_ref[...] = jnp.broadcast_to(jnp.sum(mine, axis=-1, keepdims=True), cnt_ref.shape)

    loads[2].wait()
    docs = jnp.swapaxes(docs_v[...], 0, 1)
    for step in range(length):
        sent = jnp.dot(dispatch, docs[step], preferred_element_type=f32)
        out_ref[:, step * cap : (step + 1) * cap, :] = sent.reshape(n, cap, width).astype(bf16)

    def pair_of(u):
        to_row = (row + u % n_row) % n_row
        to_col = (place + u // group) % chips * 2 + (core + u // n_row) % 2
        to = to_row * n_col + to_col
        peer = {"row": to_row, "col": to_col}
        return (
            pltpu.make_async_remote_copy(
                src_ref=out_ref.at[to],
                dst_ref=arrived.at[u],
                send_sem=doc_send.at[u],
                recv_sem=doc_recv.at[u],
                device_id=peer,
                device_id_type=MESH,
            ),
            pltpu.make_async_remote_copy(
                src_ref=cnt_ref.at[to],
                dst_ref=counts.at[u],
                send_sem=cnt_send.at[u],
                recv_sem=cnt_recv.at[u],
                device_id=peer,
                device_id_type=MESH,
            ),
        )

    def apart(k):
        near = outer * (k * 2 % chips + k // side) + inner * last_first(k)
        return (near + upper * (chips - 2 * near)) % chips

    def last_first(k):
        return (k + chips - 3) % (chips - 1) + 1

    def send_docs(first, last):
        def body(u, carry):
            for copy in pair_of(u):
                copy.start()
            return carry

        lax.fori_loop(first, last, body, 0)

    arrived[0] = out_ref[me]
    counts[0] = cnt_ref[me]
    send_docs(1, group)

    at = apart(1) * group
    send_docs(at, at + group)

    @pl.when(place == entry)
    def _():
        for i in range(side):
            source = beyond(i)
            relay(source, place).wait_recv()
            across(2 * source + core).start()
            for j in range(1, side):
                relay(source, sibling(j)).start()

    for k in range(2, chips):
        at = apart(k) * group
        send_docs(at, at + group)
    for j in range(1, side):
        relay(sibling(j), place).wait_recv()
        across(2 * sibling(j) + core).start()

    @pl.when(place != entry)
    def _():
        for i in range(side):
            relay(beyond(i), place).wait_recv()
            across(2 * beyond(i) + core).start()

    for q in range(chips):
        across(2 * q + 1 - core).wait_recv()
    for k in range(1, n_row):
        two_wait(k).wait_recv()

    def place_of(k):
        q = k // 2
        near = last_first(q) * ((q + chips - 1) // chips)
        far_off = (near + upper * (chips - 2 * near)) % chips
        return far_off * group + k % 2 * half_group

    def arrive(first, last):
        def body(u, carry):
            for copy in pair_of(u):
                copy.wait_recv()
            return carry

        lax.fori_loop(first, last, body, 0)

    def unpack(k, at):
        block = arrived[pl.ds(place_of(k), half_group)].astype(f32)
        if per == kept:
            first, last = block[:, :kept], block[:, lines - kept :]
        else:
            live = lax.broadcasted_iota(jnp.int32, block.shape, 1) < kept
            first = jnp.where(live, block, 0.0)[:, :per]
            last = jnp.where(live, pltpu.roll(block, kept, 1), 0.0)[:, :per]
        first = first.reshape(chunk, width)
        xb[at, :] = first.astype(bf16)
        t[at, :] = last.reshape(chunk, width).astype(bf16)
        size = jnp.sum(fold(first * first), axis=-1, keepdims=True) * (1.0 / width)
        rx[at, :] = jnp.broadcast_to(lax.rsqrt(size + 1e-06), (chunk, 128))

    def hidden(at, start):
        size = jnp.zeros((at.size, 128), f32)
        for n0, nn in blocks:
            cols = pl.ds(n0, nn)
            zz = start(cols, nn)
            z[at, cols] = zz
            gate = 1.0 / (1.0 + jnp.exp(-zz))
            act = zz * gate
            hh = xb[at, cols].astype(f32) + act
            h[at, cols] = hh
            hb[at, cols] = hh.astype(bf16)
            g[at, cols] = gate + act * (1.0 - gate)
            size = size + fold(hh * hh)
        size = jnp.sum(size, axis=-1, keepdims=True) * (1.0 / width)
        rr[at, :] = jnp.broadcast_to(lax.rsqrt(size + 1e-06), (at.size, 128))

    def errors(at, weights):
        r = rr[at, :]
        both = jnp.zeros((at.size, 128), f32)
        for n0, nn in blocks:
            cols = pl.ds(n0, nn)
            pp = product(hb[at, :], weights(cols), 1, 0)
            rw = spread(r, nn)
            ee = h[at, cols] + scale * rw * pp - t[at, cols].astype(f32)
            er = ee * rw
            e[at, cols] = ee
            eb[at, cols] = er.astype(bf16)
            both = both + fold(er * pp)
        both = jnp.sum(both, axis=-1, keepdims=True) * (1.0 / width)
        rr[at, :] = jnp.broadcast_to(both, (at.size, 128)) * r * r

    def slopes(at, weights, turn):
        m, rw = rr[at, :], rx[at, :]
        for n0, nn in blocks:
            cols = pl.ds(n0, nn)
            qq = product(eb[at, :], weights(cols), 1, 1)
            dd = (e[at, cols] + scale * (qq - h[at, cols] * spread(m, nn))) * g[at, cols]
            dd = dd * spread(rw, nn)
            if turn is None:
                ds[at, cols] = dd
                db[at, cols] = dd.astype(bf16)
            else:
                total = ds[at, cols] + dd
                ds[at, cols] = total
                db[at, cols] = jnp.where(turn == STEPS - 1, total, dd).astype(bf16)


    def two_cols(cols):
        return whole_two[:, :, cols].reshape(width, cols.size)

    def two_rows(cols):
        return whole_two[...].reshape(width, width)[cols.start : cols.start + cols.size]

    arrive(1, half_group)
    low, high = pl.ds(0, early), pl.ds(early, rows - early)

    def first_turn(k, carry):
        at = pl.ds(pl.multiple_of(k * chunk, chunk), chunk)
        unpack(k, at)

        def start(cols, nn):
            zz = product(xb[at, :], whole_one[:, :, cols].reshape(width, nn), 1, 0)
            return scale * spread(rx[at, :], nn) * zz

        hidden(at, start)
        errors(at, two_cols)
        slopes(at, two_rows, None)

        @pl.when(k == chunks - 3)
        def _():
            gram[low, low] = product(xb[low, :], xb[low, :], 1, 1).astype(bf16)
            for n0, nn in blocks:
                cols = pl.ds(n0, nn)
                dw[:, cols] = product(hb[low, :], eb[low, cols], 0, 0)

        @pl.when(k < chunks - 1)
        def _():
            first = place_of(k + 1)
            arrive(first, first + half_group)

        return carry

    lax.fori_loop(0, chunks, first_turn, 0)
    gram[high, :] = product(xb[high, :], xb[...], 1, 1).astype(bf16)
    gram[low, high] = product(xb[low, :], xb[high, :], 1, 1).astype(bf16)

    filled = jnp.sum(counts[...].reshape(n, 128), axis=0, keepdims=True)[:, :1]
    rate = inner_rate * scale / (filled * (length - 1))

    for n0, nn in blocks:
        cols = pl.ds(n0, nn)
        change = dw[:, cols] + product(hb[high, :], eb[high, cols], 0, 0)
        dw[:, cols] = change
        w2[1, :, cols] = (two_cols(cols).astype(f32) - rate * change).astype(bf16)

    everything = pl.ds(0, rows)

    def stwo_copy(k):
        to = (row + k) % n_row
        return pltpu.make_async_remote_copy(
            src_ref=two_out.at[to],
            dst_ref=two_buf.at[k],
            send_sem=stwo_send.at[k],
            recv_sem=stwo_recv.at[k],
            device_id={"row": to, "col": col},
            device_id_type=MESH,
        )

    def later_turn(turn, carry):
        now, later = turn % 2, (turn + 1) % 2

        def start(cols, nn):
            step = product(gram[...], db[:, cols], 1, 0)
            return z[:, cols] - (rate * scale) * spread(rx[...], nn) * step

        hidden(everything, start)
        errors(everything, lambda cols: w2[now, :, cols])
        for n0, nn in blocks:
            cols = pl.ds(n0, nn)
            change = dw[:, cols] + product(hb[...], eb[:, cols], 0, 0)
            dw[:, cols] = change
            change = rate * change
            w2[later, :, cols] = (two_cols(cols).astype(f32) - change).astype(bf16)
            two_out[:, :, cols] = change.astype(bf16).reshape(n_row, width // n_row, nn)

        @pl.when(turn == STEPS - 1)
        def _():
            for k in range(1, n_row):
                stwo_copy(k).start()

        slopes(everything, lambda cols: w2[now, cols, :], turn)
        return carry

    lax.fori_loop(1, STEPS, later_turn, 0)

    for n0, nn in blocks:
        cols = pl.ds(n0, nn)
        change = rate * product(xb[...], db[:, cols], 0, 0)
        one_out[:, :, cols] = change.astype(bf16).reshape(n_col, width // n_col, nn)

    def spair_copy(q):
        return pltpu.make_async_remote_copy(
            src_ref=one_out.at[2 * q + 1 - core],
            dst_ref=pair_buf.at[q],
            send_sem=spair_send.at[q],
            recv_sem=spair_recv.at[q],
            device_id={"row": row, "col": partner},
            device_id_type=MESH,
        )

    other = side - base

    def far(i):
        return other + (other_entry - other + i + inner) % side

    def sone_copy(to):
        return pltpu.make_async_remote_copy(
            src_ref=one_out.at[2 * to + core],
            dst_ref=one_buf.at[place],
            send_sem=sone_send.at[to],
            recv_sem=sone_recv.at[place],
            device_id={"row": row, "col": 2 * to + core},
            device_id_type=MESH,
        )

    def sone_from(source):
        return pltpu.make_async_remote_copy(
            src_ref=one_out.at[2 * source + core],
            dst_ref=one_buf.at[source],
            send_sem=sone_send.at[source],
            recv_sem=sone_recv.at[source],
            device_id={"row": row, "col": 2 * source + core},
            device_id_type=MESH,
        )

    def pre_copy(source):
        return pltpu.make_async_remote_copy(
            src_ref=one_out.at[2 * other_entry + core],
            dst_ref=pre_buf.at[source - base],
            send_sem=pre_send.at[0],
            recv_sem=pre_recv.at[source - base],
            device_id={"row": row, "col": 2 * entry + core},
            device_id_type=MESH,
        )

    wanted = [far(i) for i in range(side)] + [sibling(j) for j in range(1, side)]
    for q in wanted:
        spair_copy(q).start()
    spair_copy(place).start()
    for i, q in enumerate(wanted):
        spair_copy(q).wait_recv()
        one_out[2 * q + core] = (
            one_out[2 * q + core].astype(f32) + pair_buf[q].astype(f32)
        ).astype(bf16)
        if i in (0, side - 1):
            first = 1 if i == 0 else 0

            @pl.when(inner == first)
            def _():
                sone_copy(q).start()

            if i == 0:

                @pl.when(inner == 0)
                def _():
                    pre_copy(place).start()

        else:
            sone_copy(q).start()

    @pl.when(inner == 1)
    def _():
        share = one_out[2 * other_entry + core].astype(f32)
        for j in range(1, side):
            pre_copy(sibling(j)).wait_recv()
            share = share + pre_buf[sibling(j) - base].astype(f32)
        one_out[2 * other_entry + core] = share.astype(bf16)
        sone_copy(other_entry).start()

    loads[3].wait()
    loads[4].wait()

    def finish(share, level, moment):
        following = momentum_decay * moment[...] + share
        moment[...] = following
        level[...] = level[...] - outer_rate * (share + momentum_decay * following)

    def sent(u, carry):
        for copy in pair_of(u):
            copy.wait_send()
        return carry

    lax.fori_loop(1, n, sent, 0)
    own_copy(other_entry).wait_send()
    for j in range(1, side):
        own_copy(sibling(j)).wait_send()

    @pl.when(place == entry)
    def _():
        for i in range(side):
            for j in range(1, side):
                relay(beyond(i), sibling(j)).wait_send()

    for q in range(chips):
        across(2 * q + core).wait_send()

    share = two_out[row].astype(f32)
    for k in range(1, n_row):
        stwo_copy(k).wait_recv()
        share = share + two_buf[k].astype(f32)
    finish(share / n_row, new_two, next_two)
    spair_copy(place).wait_recv()
    total = ds.at[pl.ds(0, width // n_col), :]
    total[...] = one_out[col].astype(f32) + pair_buf[place].astype(f32)
    for j in range(1, side):
        sone_from(sibling(j)).wait_recv()
        total[...] += one_buf[sibling(j)].astype(f32)

    @pl.when(inner == 1)
    def _():
        sone_from(other_entry).wait_recv()
        total[...] += one_buf[other_entry].astype(f32)

    @pl.when(inner == 0)
    def _():
        for i in range(side):
            sone_from(far(i)).wait_recv()
            total[...] += one_buf[far(i)].astype(f32)

    finish(total[...] / n_col, new_one, next_one)

    for q in range(chips):
        spair_copy(q).wait_send()
    for k in range(1, n_row):
        two_copy(k).wait_send()
        stwo_copy(k).wait_send()
    for j in range(1, side):
        sone_copy(sibling(j)).wait_send()
    for i in range(1, side - 1):
        sone_copy(far(i)).wait_send()

    @pl.when(inner == 1)
    def _():
        for i in sorted({0, side - 1}):
            sone_copy(far(i)).wait_send()

    @pl.when(inner == 0)
    def _():
        sone_copy(far(side - 1)).wait_send()
        pre_copy(place).wait_send()


def store_kernel(*refs):
    copies = [pltpu.make_async_copy(refs[i], refs[4 + i], refs[8].at[i]) for i in range(4)]
    for copy in copies:
        copy.start()
    for copy in copies:
        copy.wait()


def shards(docs, routes, level_one, level_two, moment_one, moment_two):
    n_row = lax.axis_size("row")
    n_col = lax.axis_size("col")
    paths = n_row * n_col
    count, length, width = docs.shape
    cap = max(2, (2 * count + paths - 1) // paths)
    lines = length * cap
    kept = (length - 1) * cap
    per = (kept + 7) // 8 * 8
    rows = paths * per
    chips = n_col // 2
    one_rows, two_rows = width // n_col, width // n_row
    vmem = pl.BlockSpec(memory_space=pltpu.VMEM)
    hbm = pl.BlockSpec(memory_space=pl.ANY)
    dma = pltpu.SemaphoreType.DMA
    full = pltpu.VMEM((rows, width), f32)
    thin = pltpu.VMEM((rows, width), bf16)
    side = pltpu.VMEM((rows, 128), f32)
    scratch = [
        pltpu.VMEM((count, length, width), bf16),
        pltpu.VMEM((paths, lines, width), bf16),
        pltpu.VMEM((paths, 1, 128), f32),
        pltpu.VMEM((paths, lines, width), bf16),
        pltpu.VMEM((paths, 1, 128), f32),
        pltpu.VMEM((n_col, one_rows, width), bf16),
        pltpu.VMEM((n_row, two_rows, width), bf16),
        full, full, full, full, full, thin, thin, thin, thin, thin,
        pltpu.VMEM((rows, rows), bf16),
        pltpu.VMEM((2, width, width), bf16),
        pltpu.VMEM((width, width), f32),
        side, side,
        pltpu.VMEM((n_col, one_rows, width), bf16),
        pltpu.VMEM((n_row, two_rows, width), bf16),
        pltpu.VMEM((chips, one_rows, width), bf16),
        pltpu.VMEM((chips // 2, one_rows, width), bf16),
        pltpu.VMEM((chips, one_rows, width), bf16),
        pltpu.VMEM((n_row, two_rows, width), bf16),
        dma((5,)), dma((paths,)), dma((paths,)), dma((paths,)), dma((paths,)),
        dma((chips,)), dma((chips, chips)), dma((n_col,)), dma((n_col,)), dma((n_col,)),
        dma((n_row,)), dma((n_row,)),
        dma((chips,)), dma((chips,)), dma((1,)), dma((chips // 2,)), dma((chips,)), dma((chips,)),
        dma((n_row,)), dma((n_row,)),
    ]
    held = sum(
        math.prod(piece.shape) * piece.dtype.itemsize
        for piece in scratch
        if piece.memory_space == pltpu.VMEM
    )
    kept_bytes = 8 * (one_rows + two_rows) * width
    limit = min(67043328 - kept_bytes, held + (12 << 20))
    held_one = pltpu.VMEM((one_rows, width), f32)
    held_two = pltpu.VMEM((two_rows, width), f32)
    results = pl.pallas_call(
        functools.partial(round_kernel, n_row, n_col, cap, kept),
        out_shape=(held_one, held_two, held_one, held_two),
        in_specs=[vmem, hbm, hbm, hbm, hbm, hbm],
        out_specs=(vmem,) * 4,
        scratch_shapes=scratch,
        compiler_params=pltpu.CompilerParams(
            collective_id=0, has_side_effects=True, vmem_limit_bytes=limit
        ),
    )(
        routes.reshape(1, count), docs, level_one[0], level_two[0], moment_one[0], moment_two[0]
    )
    results = pl.pallas_call(
        store_kernel,
        out_shape=tuple(jax.ShapeDtypeStruct(result.shape, f32) for result in results),
        in_specs=[hbm] * 4,
        out_specs=(pl.BlockSpec(memory_space=pltpu.HBM),) * 4,
        scratch_shapes=[dma((4,))],
    )(*(pltpu.with_memory_space_constraint(result, pltpu.VMEM) for result in results))
    return tuple(result[None] for result in results)


def solution(mesh):
    placed = (
        P(("row", "col"), None, None),
        P(("row", "col"), None),
        P("row", "col", None),
        P("col", "row", None),
        P("row", "col", None),
        P("col", "row", None),
    )
    return jax.shard_map(
        shards,
        mesh=mesh,
        in_specs=placed,
        out_specs=(
            P("row", "col", None),
            P("col", "row", None),
            P("row", "col", None),
            P("col", "row", None),
        ),
        check_vma=False,
    )
```

```python
import functools
import math

import jax
import jax.numpy as jnp
from jax import lax
from jax.experimental import pallas as pl
from jax.experimental.pallas import tpu as pltpu
from jax.sharding import PartitionSpec as P

STEPS = 3
BLOCK_COLS = 256

inner_rate = 64.0
outer_rate = 0.7
momentum_decay = 0.9

MESH = pl.DeviceIdType.MESH
f32 = jnp.float32
bf16 = jnp.bfloat16


def product(a, b, i, j):
    return lax.dot_general(a, b, (((i,), (j,)), ((), ())), preferred_element_type=f32)


def column_blocks(width):
    return [(at, min(BLOCK_COLS, width - at)) for at in range(0, width, BLOCK_COLS)]


def fold(values):
    return sum(values[:, at : at + 128] for at in range(0, values.shape[1], 128))


def spread(values, width):
    return jnp.concatenate([values] * (width // 128), axis=1) if width > 128 else values


def round_kernel(
    n_row, n_col, cap, kept,
    route_ref, docs_hbm, one_hbm, two_hbm, moment_one_hbm, moment_two_hbm,
    new_one, new_two, next_one, next_two,
    docs_v, out_ref, cnt_ref, arrived, counts, whole_one, whole_two,
    z, h, g, e, ds, t, xb, hb, eb, db, gram, w2, dw, rx, rr,
    one_out, two_out, pair_buf, pre_buf, one_buf, two_buf,
    load_sem, doc_send, doc_recv, cnt_send, cnt_recv,
    own_send, relay_send, one_recv, pair_send, pair_recv, two_send, two_recv,
    spair_send, spair_recv, pre_send, pre_recv, sone_send, sone_recv, stwo_send, stwo_recv,
):
    row, col = lax.axis_index("row"), lax.axis_index("col")
    n = n_row * n_col
    me = row * n_col + col
    chips = n_col // 2
    place, core = col // 2, col % 2
    partner = place * 2 + 1 - core
    side = chips // 2
    upper = place // side
    base = upper * side
    entry = side - 1 + upper
    inner = (place == entry).astype(jnp.int32)
    outer = 1 - inner
    other_entry = side - upper
    lines, width = arrived.shape[1:]
    rows = z.shape[0]
    per = rows // n
    group = 2 * n_row
    half_group = group // 2
    chunk = half_group * per
    chunks = 2 * chips
    early = rows * (chips - 1) // chips // 256 * 256
    count = docs_v.shape[0]
    length = docs_v.shape[1]
    scale = width ** (-0.5)
    blocks = column_blocks(width)
    barrier = pltpu.get_barrier_semaphore()

    loads = [
        pltpu.make_async_copy(one_hbm, new_one, load_sem.at[0]),
        pltpu.make_async_copy(two_hbm, new_two, load_sem.at[1]),
        pltpu.make_async_copy(docs_hbm, docs_v, load_sem.at[2]),
        pltpu.make_async_copy(moment_one_hbm, next_one, load_sem.at[3]),
        pltpu.make_async_copy(moment_two_hbm, next_two, load_sem.at[4]),
    ]
    for copy in loads:
        copy.start()

    def greet(k, carry):
        to = (me + k) % n
        pl.semaphore_signal(
            barrier, inc=1, device_id={"row": to // n_col, "col": to % n_col}, device_id_type=MESH
        )
        return carry

    lax.fori_loop(1, n, greet, 0)
    loads[0].wait()
    whole_one[col] = new_one[...].astype(bf16)

    pl.semaphore_wait(barrier, n - 1)

    def own_copy(to):
        return pltpu.make_async_remote_copy(
            src_ref=whole_one.at[col],
            dst_ref=whole_one.at[col],
            send_sem=own_send.at[to],
            recv_sem=one_recv.at[col],
            device_id={"row": row, "col": 2 * to + core},
            device_id_type=MESH,
        )

    def relay(source, to):
        block = 2 * source + core
        return pltpu.make_async_remote_copy(
            src_ref=whole_one.at[block],
            dst_ref=whole_one.at[block],
            send_sem=relay_send.at[source, to],
            recv_sem=one_recv.at[block],
            device_id={"row": row, "col": 2 * to + core},
            device_id_type=MESH,
        )

    def sibling(j):
        return base + (place - base + j) % side

    def beyond(i):
        return (1 - upper) * (side + i) + upper * (side - 1 - i)

    def across(block):
        return pltpu.make_async_remote_copy(
            src_ref=whole_one.at[block],
            dst_ref=whole_one.at[block],
            send_sem=pair_send.at[block],
            recv_sem=pair_recv.at[block],
            device_id={"row": row, "col": partner},
            device_id_type=MESH,
        )

    def two_copy(k):
        return pltpu.make_async_remote_copy(
            src_ref=whole_two.at[row],
            dst_ref=whole_two.at[row],
            send_sem=two_send.at[k],
            recv_sem=two_recv.at[k],
            device_id={"row": (row + k) % n_row, "col": col},
            device_id_type=MESH,
        )

    def two_wait(k):
        from_row = (row - k + n_row) % n_row
        return pltpu.make_async_remote_copy(
            src_ref=whole_two.at[row],
            dst_ref=whole_two.at[from_row],
            send_sem=two_send.at[k],
            recv_sem=two_recv.at[k],
            device_id={"row": (row + k) % n_row, "col": col},
            device_id_type=MESH,
        )

    own_copy(other_entry).start()
    for j in range(1, side):
        own_copy(sibling(j)).start()
    across(col).start()
    loads[1].wait()
    whole_two[row] = new_two[...].astype(bf16)
    for k in range(1, n_row):
        two_copy(k).start()

    target = route_ref[...]
    named = jnp.broadcast_to(target.astype(f32), (count, count))
    earlier = lax.broadcasted_iota(jnp.int32, (count, count), 0) < lax.broadcasted_iota(
        jnp.int32, (count, count), 1
    )
    rank = jnp.sum(jnp.where((named.T == named) & earlier, 1.0, 0.0), axis=0, keepdims=True)
    slot = target * cap + rank.astype(jnp.int32)
    slots = lax.broadcasted_iota(jnp.int32, (n * cap, count), 0)
    dispatch = jnp.where(slots == slot, 1.0, 0.0).astype(bf16)
    path = lax.broadcasted_iota(jnp.int32, (n, 1, count), 0)
    mine = jnp.where(jnp.broadcast_to(target[None], (n, 1, count)) == path, 1.0, 0.0)
    cnt_ref[...] = jnp.broadcast_to(jnp.sum(mine, axis=-1, keepdims=True), cnt_ref.shape)

    loads[2].wait()
    docs = jnp.swapaxes(docs_v[...], 0, 1)
    for step in range(length):
        sent = jnp.dot(dispatch, docs[step], preferred_element_type=f32)
        out_ref[:, step * cap : (step + 1) * cap, :] = sent.reshape(n, cap, width).astype(bf16)

    def pair_of(u):
        to_row = (row + u % n_row) % n_row
        to_col = (place + u // group) % chips * 2 + (core + u // n_row) % 2
        to = to_row * n_col + to_col
        peer = {"row": to_row, "col": to_col}
        return (
            pltpu.make_async_remote_copy(
                src_ref=out_ref.at[to],
                dst_ref=arrived.at[u],
                send_sem=doc_send.at[u],
                recv_sem=doc_recv.at[u],
                device_id=peer,
                device_id_type=MESH,
            ),
            pltpu.make_async_remote_copy(
                src_ref=cnt_ref.at[to],
                dst_ref=counts.at[u],
                send_sem=cnt_send.at[u],
                recv_sem=cnt_recv.at[u],
                device_id=peer,
                device_id_type=MESH,
            ),
        )

    def apart(k):
        near = outer * (k * 2 % chips + k // side) + inner * last_first(k)
        return (near + upper * (chips - 2 * near)) % chips

    def last_first(k):
        return (k + chips - 3) % (chips - 1) + 1

    def send_docs(first, last):
        def body(u, carry):
            for copy in pair_of(u):
                copy.start()
            return carry

        lax.fori_loop(first, last, body, 0)

    arrived[0] = out_ref[me]
    counts[0] = cnt_ref[me]
    send_docs(1, group)

    at = apart(1) * group
    send_docs(at, at + group)

    @pl.when(place == entry)
    def _():
        for i in range(side):
            source = beyond(i)
            relay(source, place).wait_recv()
            across(2 * source + core).start()
            for j in range(1, side):
                relay(source, sibling(j)).start()

    for k in range(2, chips):
        at = apart(k) * group
        send_docs(at, at + group)
    for j in range(1, side):
        relay(sibling(j), place).wait_recv()
        across(2 * sibling(j) + core).start()

    @pl.when(place != entry)
    def _():
        for i in range(side):
            relay(beyond(i), place).wait_recv()
            across(2 * beyond(i) + core).start()

    for q in range(chips):
        across(2 * q + 1 - core).wait_recv()
    for k in range(1, n_row):
        two_wait(k).wait_recv()

    def place_of(k):
        q = k // 2
        near = last_first(q) * ((q + chips - 1) // chips)
        far_off = (near + upper * (chips - 2 * near)) % chips
        return far_off * group + k % 2 * half_group

    def arrive(first, last):
        def body(u, carry):
            for copy in pair_of(u):
                copy.wait_recv()
            return carry

        lax.fori_loop(first, last, body, 0)

    def unpack(k, at):
        block = arrived[pl.ds(place_of(k), half_group)].astype(f32)
        if per == kept:
            first, last = block[:, :kept], block[:, lines - kept :]
        else:
            live = lax.broadcasted_iota(jnp.int32, block.shape, 1) < kept
            first = jnp.where(live, block, 0.0)[:, :per]
            last = jnp.where(live, pltpu.roll(block, kept, 1), 0.0)[:, :per]
        first = first.reshape(chunk, width)
        xb[at, :] = first.astype(bf16)
        t[at, :] = last.reshape(chunk, width).astype(bf16)
        size = jnp.sum(fold(first * first), axis=-1, keepdims=True) * (1.0 / width)
        rx[at, :] = jnp.broadcast_to(lax.rsqrt(size + 1e-06), (chunk, 128))

    def hidden(at, start):
        size = jnp.zeros((at.size, 128), f32)
        for n0, nn in blocks:
            cols = pl.ds(n0, nn)
            zz = start(cols, nn)
            z[at, cols] = zz
            gate = 1.0 / (1.0 + jnp.exp(-zz))
            act = zz * gate
            hh = xb[at, cols].astype(f32) + act
            h[at, cols] = hh
            hb[at, cols] = hh.astype(bf16)
            g[at, cols] = gate + act * (1.0 - gate)
            size = size + fold(hh * hh)
        size = jnp.sum(size, axis=-1, keepdims=True) * (1.0 / width)
        rr[at, :] = jnp.broadcast_to(lax.rsqrt(size + 1e-06), (at.size, 128))

    def errors(at, weights):
        r = rr[at, :]
        both = jnp.zeros((at.size, 128), f32)
        for n0, nn in blocks:
            cols = pl.ds(n0, nn)
            pp = product(hb[at, :], weights(cols), 1, 0)
            rw = spread(r, nn)
            ee = h[at, cols] + scale * rw * pp - t[at, cols].astype(f32)
            er = ee * rw
            e[at, cols] = ee
            eb[at, cols] = er.astype(bf16)
            both = both + fold(er * pp)
        both = jnp.sum(both, axis=-1, keepdims=True) * (1.0 / width)
        rr[at, :] = jnp.broadcast_to(both, (at.size, 128)) * r * r

    def slopes(at, weights, turn):
        m, rw = rr[at, :], rx[at, :]
        for n0, nn in blocks:
            cols = pl.ds(n0, nn)
            qq = product(eb[at, :], weights(cols), 1, 1)
            dd = (e[at, cols] + scale * (qq - h[at, cols] * spread(m, nn))) * g[at, cols]
            dd = dd * spread(rw, nn)
            if turn is None:
                ds[at, cols] = dd
                db[at, cols] = dd.astype(bf16)
            else:
                total = ds[at, cols] + dd
                ds[at, cols] = total
                db[at, cols] = jnp.where(turn == STEPS - 1, total, dd).astype(bf16)


    def two_cols(cols):
        return whole_two[:, :, cols].reshape(width, cols.size)

    def two_rows(cols):
        return whole_two[...].reshape(width, width)[cols.start : cols.start + cols.size]

    arrive(1, half_group)
    low, high = pl.ds(0, early), pl.ds(early, rows - early)

    def first_turn(k, carry):
        at = pl.ds(pl.multiple_of(k * chunk, chunk), chunk)
        unpack(k, at)

        def start(cols, nn):
            zz = product(xb[at, :], whole_one[:, :, cols].reshape(width, nn), 1, 0)
            return scale * spread(rx[at, :], nn) * zz

        hidden(at, start)
        errors(at, two_cols)
        slopes(at, two_rows, None)

        @pl.when(k == chunks - 3)
        def _():
            gram[low, low] = product(xb[low, :], xb[low, :], 1, 1).astype(bf16)
            for n0, nn in blocks:
                cols = pl.ds(n0, nn)
                dw[:, cols] = product(hb[low, :], eb[low, cols], 0, 0)

        @pl.when(k < chunks - 1)
        def _():
            first = place_of(k + 1)
            arrive(first, first + half_group)

        return carry

    lax.fori_loop(0, chunks, first_turn, 0)
    gram[high, :] = product(xb[high, :], xb[...], 1, 1).astype(bf16)
    gram[low, high] = gram[high, low].T

    filled = jnp.sum(counts[...].reshape(n, 128), axis=0, keepdims=True)[:, :1]
    rate = inner_rate * scale / (filled * (length - 1))

    for n0, nn in blocks:
        cols = pl.ds(n0, nn)
        change = dw[:, cols] + product(hb[high, :], eb[high, cols], 0, 0)
        dw[:, cols] = change
        w2[1, :, cols] = (two_cols(cols).astype(f32) - rate * change).astype(bf16)

    everything = pl.ds(0, rows)

    def stwo_copy(k):
        to = (row + k) % n_row
        return pltpu.make_async_remote_copy(
            src_ref=two_out.at[to],
            dst_ref=two_buf.at[k],
            send_sem=stwo_send.at[k],
            recv_sem=stwo_recv.at[k],
            device_id={"row": to, "col": col},
            device_id_type=MESH,
        )

    def later_turn(turn, carry):
        now, later = turn % 2, (turn + 1) % 2

        def start(cols, nn):
            step = product(gram[...], db[:, cols], 1, 0)
            return z[:, cols] - (rate * scale) * spread(rx[...], nn) * step

        hidden(everything, start)
        errors(everything, lambda cols: w2[now, :, cols])
        for n0, nn in blocks:
            cols = pl.ds(n0, nn)
            change = dw[:, cols] + product(hb[...], eb[:, cols], 0, 0)
            dw[:, cols] = change
            change = rate * change
            w2[later, :, cols] = (two_cols(cols).astype(f32) - change).astype(bf16)
            two_out[:, :, cols] = change.astype(bf16).reshape(n_row, width // n_row, nn)

        @pl.when(turn == STEPS - 1)
        def _():
            for k in range(1, n_row):
                stwo_copy(k).start()

        slopes(everything, lambda cols: w2[now, cols, :], turn)
        return carry

    lax.fori_loop(1, STEPS, later_turn, 0)

    for n0, nn in blocks:
        cols = pl.ds(n0, nn)
        change = rate * product(xb[...], db[:, cols], 0, 0)
        one_out[:, :, cols] = change.astype(bf16).reshape(n_col, width // n_col, nn)

    def spair_copy(q):
        return pltpu.make_async_remote_copy(
            src_ref=one_out.at[2 * q + 1 - core],
            dst_ref=pair_buf.at[q],
            send_sem=spair_send.at[q],
            recv_sem=spair_recv.at[q],
            device_id={"row": row, "col": partner},
            device_id_type=MESH,
        )

    other = side - base

    def far(i):
        return other + (other_entry - other + i + inner) % side

    def sone_copy(to):
        return pltpu.make_async_remote_copy(
            src_ref=one_out.at[2 * to + core],
            dst_ref=one_buf.at[place],
            send_sem=sone_send.at[to],
            recv_sem=sone_recv.at[place],
            device_id={"row": row, "col": 2 * to + core},
            device_id_type=MESH,
        )

    def sone_from(source):
        return pltpu.make_async_remote_copy(
            src_ref=one_out.at[2 * source + core],
            dst_ref=one_buf.at[source],
            send_sem=sone_send.at[source],
            recv_sem=sone_recv.at[source],
            device_id={"row": row, "col": 2 * source + core},
            device_id_type=MESH,
        )

    def pre_copy(source):
        return pltpu.make_async_remote_copy(
            src_ref=one_out.at[2 * other_entry + core],
            dst_ref=pre_buf.at[source - base],
            send_sem=pre_send.at[0],
            recv_sem=pre_recv.at[source - base],
            device_id={"row": row, "col": 2 * entry + core},
            device_id_type=MESH,
        )

    wanted = [far(i) for i in range(side)] + [sibling(j) for j in range(1, side)]
    for q in wanted:
        spair_copy(q).start()
    spair_copy(place).start()
    for i, q in enumerate(wanted):
        spair_copy(q).wait_recv()
        one_out[2 * q + core] = (
            one_out[2 * q + core].astype(f32) + pair_buf[q].astype(f32)
        ).astype(bf16)
        if i in (0, side - 1):
            first = 1 if i == 0 else 0

            @pl.when(inner == first)
            def _():
                sone_copy(q).start()

            if i == 0:

                @pl.when(inner == 0)
                def _():
                    pre_copy(place).start()

        else:
            sone_copy(q).start()

    @pl.when(inner == 1)
    def _():
        share = one_out[2 * other_entry + core].astype(f32)
        for j in range(1, side):
            pre_copy(sibling(j)).wait_recv()
            share = share + pre_buf[sibling(j) - base].astype(f32)
        one_out[2 * other_entry + core] = share.astype(bf16)
        sone_copy(other_entry).start()

    loads[3].wait()
    loads[4].wait()

    def finish(share, level, moment):
        following = momentum_decay * moment[...] + share
        moment[...] = following
        level[...] = level[...] - outer_rate * (share + momentum_decay * following)

    def sent(u, carry):
        for copy in pair_of(u):
            copy.wait_send()
        return carry

    lax.fori_loop(1, n, sent, 0)
    own_copy(other_entry).wait_send()
    for j in range(1, side):
        own_copy(sibling(j)).wait_send()

    @pl.when(place == entry)
    def _():
        for i in range(side):
            for j in range(1, side):
                relay(beyond(i), sibling(j)).wait_send()

    for q in range(chips):
        across(2 * q + core).wait_send()

    share = two_out[row].astype(f32)
    for k in range(1, n_row):
        stwo_copy(k).wait_recv()
        share = share + two_buf[k].astype(f32)
    finish(share / n_row, new_two, next_two)
    spair_copy(place).wait_recv()
    total = ds.at[pl.ds(0, width // n_col), :]
    total[...] = one_out[col].astype(f32) + pair_buf[place].astype(f32)
    for j in range(1, side):
        sone_from(sibling(j)).wait_recv()
        total[...] += one_buf[sibling(j)].astype(f32)

    @pl.when(inner == 1)
    def _():
        sone_from(other_entry).wait_recv()
        total[...] += one_buf[other_entry].astype(f32)

    @pl.when(inner == 0)
    def _():
        for i in range(side):
            sone_from(far(i)).wait_recv()
            total[...] += one_buf[far(i)].astype(f32)

    finish(total[...] / n_col, new_one, next_one)

    for q in range(chips):
        spair_copy(q).wait_send()
    for k in range(1, n_row):
        two_copy(k).wait_send()
        stwo_copy(k).wait_send()
    for j in range(1, side):
        sone_copy(sibling(j)).wait_send()
    for i in range(1, side - 1):
        sone_copy(far(i)).wait_send()

    @pl.when(inner == 1)
    def _():
        for i in sorted({0, side - 1}):
            sone_copy(far(i)).wait_send()

    @pl.when(inner == 0)
    def _():
        sone_copy(far(side - 1)).wait_send()
        pre_copy(place).wait_send()


def store_kernel(*refs):
    copies = [pltpu.make_async_copy(refs[i], refs[4 + i], refs[8].at[i]) for i in range(4)]
    for copy in copies:
        copy.start()
    for copy in copies:
        copy.wait()


def shards(docs, routes, level_one, level_two, moment_one, moment_two):
    n_row = lax.axis_size("row")
    n_col = lax.axis_size("col")
    paths = n_row * n_col
    count, length, width = docs.shape
    cap = max(2, (2 * count + paths - 1) // paths)
    lines = length * cap
    kept = (length - 1) * cap
    per = (kept + 7) // 8 * 8
    rows = paths * per
    chips = n_col // 2
    one_rows, two_rows = width // n_col, width // n_row
    vmem = pl.BlockSpec(memory_space=pltpu.VMEM)
    hbm = pl.BlockSpec(memory_space=pl.ANY)
    dma = pltpu.SemaphoreType.DMA
    full = pltpu.VMEM((rows, width), f32)
    thin = pltpu.VMEM((rows, width), bf16)
    side = pltpu.VMEM((rows, 128), f32)
    scratch = [
        pltpu.VMEM((count, length, width), bf16),
        pltpu.VMEM((paths, lines, width), bf16),
        pltpu.VMEM((paths, 1, 128), f32),
        pltpu.VMEM((paths, lines, width), bf16),
        pltpu.VMEM((paths, 1, 128), f32),
        pltpu.VMEM((n_col, one_rows, width), bf16),
        pltpu.VMEM((n_row, two_rows, width), bf16),
        full, full, full, full, full, thin, thin, thin, thin, thin,
        pltpu.VMEM((rows, rows), bf16),
        pltpu.VMEM((2, width, width), bf16),
        pltpu.VMEM((width, width), f32),
        side, side,
        pltpu.VMEM((n_col, one_rows, width), bf16),
        pltpu.VMEM((n_row, two_rows, width), bf16),
        pltpu.VMEM((chips, one_rows, width), bf16),
        pltpu.VMEM((chips // 2, one_rows, width), bf16),
        pltpu.VMEM((chips, one_rows, width), bf16),
        pltpu.VMEM((n_row, two_rows, width), bf16),
        dma((5,)), dma((paths,)), dma((paths,)), dma((paths,)), dma((paths,)),
        dma((chips,)), dma((chips, chips)), dma((n_col,)), dma((n_col,)), dma((n_col,)),
        dma((n_row,)), dma((n_row,)),
        dma((chips,)), dma((chips,)), dma((1,)), dma((chips // 2,)), dma((chips,)), dma((chips,)),
        dma((n_row,)), dma((n_row,)),
    ]
    held = sum(
        math.prod(piece.shape) * piece.dtype.itemsize
        for piece in scratch
        if piece.memory_space == pltpu.VMEM
    )
    kept_bytes = 8 * (one_rows + two_rows) * width
    limit = min(67043328 - kept_bytes, held + (12 << 20))
    held_one = pltpu.VMEM((one_rows, width), f32)
    held_two = pltpu.VMEM((two_rows, width), f32)
    results = pl.pallas_call(
        functools.partial(round_kernel, n_row, n_col, cap, kept),
        out_shape=(held_one, held_two, held_one, held_two),
        in_specs=[vmem, hbm, hbm, hbm, hbm, hbm],
        out_specs=(vmem,) * 4,
        scratch_shapes=scratch,
        compiler_params=pltpu.CompilerParams(
            collective_id=0, has_side_effects=True, vmem_limit_bytes=limit
        ),
    )(
        routes.reshape(1, count), docs, level_one[0], level_two[0], moment_one[0], moment_two[0]
    )
    results = pl.pallas_call(
        store_kernel,
        out_shape=tuple(jax.ShapeDtypeStruct(result.shape, f32) for result in results),
        in_specs=[hbm] * 4,
        out_specs=(pl.BlockSpec(memory_space=pltpu.HBM),) * 4,
        scratch_shapes=[dma((4,))],
    )(*(pltpu.with_memory_space_constraint(result, pltpu.VMEM) for result in results))
    return tuple(result[None] for result in results)


def solution(mesh):
    placed = (
        P(("row", "col"), None, None),
        P(("row", "col"), None),
        P("row", "col", None),
        P("col", "row", None),
        P("row", "col", None),
        P("col", "row", None),
    )
    return jax.shard_map(
        shards,
        mesh=mesh,
        in_specs=placed,
        out_specs=(
            P("row", "col", None),
            P("col", "row", None),
            P("row", "col", None),
            P("col", "row", None),
        ),
        check_vma=False,
    )
```
